32 devices in a mesh: gx: 4 (over y, x), gy: 4 (over z), ma: 2 (over core).
Axes of the slice: x: 2, y: 2, z: 4, core: 2. Of those that a mesh axis runs over, the one named last changes fastest.
Arguments:
- alpha_fields: bfloat16 [80, 2, 512, 512], P('ma', None, 'gy', 'gx'), may hold values from -6 to 6
- member_perts: bfloat16 [80, 2, 512, 512], P('ma', None, 'gy', 'gx'), may hold values from -0.625 to 0.625
- band_widths: int32 [2], replicated, may hold values from 2 to 8
- lat_index: int32 [1024], P('gy'), may hold values from 0 to 510, as said below
- lat_weight: float32 [1024], P('gy'), may hold values from 0 to 1
- lon_index: int32 [1024], P('gx'), may hold values from 0 to 511, as said below
- lon_weight: float32 [1024], P('gx'), may hold values from 0 to 1
- innovation: float32 [2, 1024, 1024], P(None, 'gy', 'gx'), may hold values from -6 to 6
- obs_weight: float32 [2, 1024, 1024], P(None, 'gy', 'gx'), may hold values from 0.1 to 1
Outputs:
- increment: float32 [2, 1024, 1024], P(None, 'gy', 'gx')
- gradient: float32 [80, 2, 512, 512], P('ma', None, 'gy', 'gx')
The draws below stay inside these ranges and needn't reach their ends.
Inputs may be any that keep to these rules, and one draw needn't show every extreme that they name: lat_index[p] is p // 2 - 1 or p // 2, clamped to 0 .. 510. lon_index[q] is q // 2 - 1 or q // 2, taken modulo 512.
All inputs are finite; a program needn't handle non-finite values.
Results may differ from the reference program's by a relative error of at most 0.0003.
Values may be sent and summed in bfloat16 or wider, within the bound.
A program may use at most 128 MiB of HBM per device.

```python
import math
import jax
import jax.numpy as jnp
from jax import lax

MEM = 80
LEV = 2
HB = 8
NCLAT = 512
NCLON = 512
NFLAT = 1024
NFLON = 1024


def draw_lat_index(key, part):
    position = jnp.arange(NFLAT, dtype=jnp.int32)
    backward = jax.random.randint(key, (NFLAT,), 0, 2, dtype=jnp.int32)
    return jnp.clip(position // 2 - backward, 0, NCLAT - 2).astype(jnp.int32)


def draw_lon_index(key, part):
    position = jnp.arange(NFLON, dtype=jnp.int32)
    backward = jax.random.randint(key, (NFLON,), 0, 2, dtype=jnp.int32)
    return jnp.remainder(position // 2 - backward, NCLON).astype(jnp.int32)


def steps_of(own_key, dims, cuts, smallest, top_value):
    def one(dim, shards_of):
        heights = jax.random.uniform(jax.random.fold_in(jax.random.fold_in(own_key, 6), dim), (shards_of,), jnp.float32, smallest / len(cuts), top_value / len(cuts))
        return jnp.repeat(jnp.exp(heights), dims[dim] // shards_of).reshape((-1,) + (1,) * (len(dims) - dim - 1))

    gain = one(*cuts[0])
    for cut in cuts[1:]:
        gain = gain * one(*cut)
    return gain


def normal_values(rng, extent, width, limit, shards=(), kind=jnp.bfloat16):
    entries = width * jax.random.normal(rng, extent, jnp.float32)
    if shards:
        entries = entries * steps_of(rng, extent, shards, -0.22, 0.18)
    return jnp.clip(entries, -limit, limit).astype(kind)


def setup_inputs(seed: int = 0) -> dict:
    splits = jax.random.split(jax.random.key(seed), 10)
    return {
        "alpha_fields": normal_values(splits[0], (MEM, LEV, NCLAT, NCLON), 1.0, 6.0, ((0, 2), (2, 4), (3, 4))),
        "member_perts": normal_values(splits[1], (MEM, LEV, NCLAT, NCLON), MEM ** -0.5, 0.625, ((0, 2), (2, 4), (3, 4))),
        "band_widths": jax.random.randint(splits[2], (LEV,), 2, HB + 1).astype(jnp.int32),
        "lat_index": draw_lat_index(jax.random.fold_in(splits[9], 71), 0),
        "lat_weight": jnp.clip(1.0 * jax.random.uniform(splits[4], (NFLAT,), jnp.float32) ** steps_of(splits[4], (NFLAT,), ((0, 4),), -0.2, 0.2), 0.0, 1.0),
        "lon_index": draw_lon_index(jax.random.fold_in(splits[9], 71), 0),
        "lon_weight": jnp.clip(1.0 * jax.random.uniform(splits[6], (NFLON,), jnp.float32) ** steps_of(splits[6], (NFLON,), ((0, 4),), -0.2, 0.2), 0.0, 1.0),
        "innovation": normal_values(splits[7], (LEV, NFLAT, NFLON), 1.0, 6.0, ((1, 4), (2, 4)), jnp.float32),
        "obs_weight": jnp.clip(jnp.exp(math.log(1.0) - 2.3025851 * jax.random.uniform(splits[8], (LEV, NFLAT, NFLON), jnp.float32) ** steps_of(splits[8], (LEV, NFLAT, NFLON), ((1, 4), (2, 4)), -0.2, 0.2)), 0.1, 1.0),
    }


def tap_table(band_widths):
    tap_offsets = jnp.arange(-HB, HB + 1).astype(jnp.float32)
    spread = band_widths.astype(jnp.float32)[:, None]
    shapes = jnp.exp(-tap_offsets[None, :] ** 2 / (2.0 * spread * spread))
    return shapes / jnp.sqrt(lax.optimization_barrier(jnp.sum(shapes * shapes, axis=1, keepdims=True)))

def localize(source, filter_taps):
    along_lon = jnp.zeros_like(source)
    for tap_number in range(2 * HB + 1):
        along_lon = along_lon + filter_taps[:, tap_number, None, None] * jnp.roll(source, HB - tap_number, axis=2)
    padded = jnp.pad(along_lon, ((0, 0), (HB, HB), (0, 0)))
    result = jnp.zeros_like(source)
    for tap_number in range(2 * HB + 1):
        result = result + filter_taps[:, tap_number, None, None] * padded[:, tap_number:tap_number + NCLAT, :]
    return result

def reference(alpha_fields, member_perts, band_widths, lat_index, lat_weight, lon_index, lon_weight, innovation, obs_weight):
    filter_taps = tap_table(band_widths)

    def accumulate(running, member_pair):
        localized = localize(member_pair[0].astype(jnp.float32), filter_taps)
        return (running + member_pair[1].astype(jnp.float32) * localized, None)
    coarse_increment, unused = lax.scan(accumulate, jnp.zeros((LEV, NCLAT, NCLON), jnp.float32), (alpha_fields, member_perts))
    lat_next = (lat_index + 1).astype(jnp.int32)
    lon_next = jnp.remainder(lon_index + 1, NCLON).astype(jnp.int32)
    north_weight = lat_weight[None, :, None]
    east_weight = lon_weight[None, None, :]
    by_lat = (1.0 - north_weight) * coarse_increment[:, lat_index, :] + north_weight * coarse_increment[:, lat_next, :]
    increment = (1.0 - east_weight) * by_lat[:, :, lon_index] + east_weight * by_lat[:, :, lon_next]
    misfit = obs_weight * (increment - innovation)
    spread_lon = jnp.zeros((LEV, NFLAT, NCLON), jnp.float32)
    spread_lon = spread_lon.at[:, :, lon_index].add((1.0 - east_weight) * misfit)
    spread_lon = spread_lon.at[:, :, lon_next].add(east_weight * misfit)
    coarse_residual = jnp.zeros((LEV, NCLAT, NCLON), jnp.float32)
    coarse_residual = coarse_residual.at[:, lat_index, :].add((1.0 - north_weight) * spread_lon)
    coarse_residual = coarse_residual.at[:, lat_next, :].add(north_weight * spread_lon)

    def member_gradient(member_pair):
        product = member_pair[1].astype(jnp.float32) * coarse_residual
        return member_pair[0].astype(jnp.float32) + localize(product, filter_taps)
    gradient = lax.map(member_gradient, (alpha_fields, member_perts))
    return (increment, gradient)
```

```python
import jax
import jax.numpy as jnp
from jax import lax
from jax.experimental import pallas as pl
from jax.experimental.pallas import tpu as pltpu
from jax.sharding import PartitionSpec as P

HB = 8
GROUP = 8
FR = 24
FC = 32
CR = 16
STRIP = 24
REACH = HB + 10
MESH = pl.DeviceIdType.MESH
VMEM_LIMIT = 60 * 2**20
F32 = jnp.float32
BF16 = jnp.bfloat16


def iota(shape, dim):
    return lax.broadcasted_iota(jnp.int32, shape, dim)


def dot(a, b):
    return jnp.dot(a, b, preferred_element_type=F32)


def split(value):
    high = value.astype(BF16)
    return high, (value - high.astype(F32)).astype(BF16)


def dot3(a, b):
    return dot(a[0], b[0]) + dot(a[1], b[0]) + dot(a[0], b[1])


def rows_of(*parts):
    return jnp.concatenate(parts, axis=0)


def lanes_of(*parts):
    return jnp.concatenate(parts, axis=1)


def natural(x, rows):
    return rows_of(x[rows : rows + HB], x[:rows], x[rows + HB :])


def place(order, size, width):
    return jnp.where(order < size, order, jnp.where(order < size + width, order - size - width, order - width))


def tap_value(distance, spread, scale):
    d = distance.astype(F32)
    value = jnp.exp(-(d * d) / (2.0 * spread * spread)) * scale
    return jnp.where(jnp.abs(distance) <= HB, value, 0.0)


def tap_scale(spread):
    lane = iota((8, 128), 1)
    d = (lane - HB).astype(F32)
    shape = jnp.where(lane <= 2 * HB, jnp.exp(-(d * d) / (2.0 * spread * spread)), 0.0)
    return (1.0 / jnp.sqrt(jnp.sum(shape * shape, axis=1, keepdims=True)))[:1]


def lat_taps(spread, scale, height, deep, offset, width):
    i, c = iota((height, width), 0), iota((height, width), 1)
    r = jnp.where(c >= 2 * deep, c - 2 * deep, jnp.where(c >= deep, c - deep, c))
    value = tap_value(r - i + offset, spread, scale)
    high = value.astype(BF16).astype(F32)
    return jnp.where((c >= deep) & (c < 2 * deep), value - high, high).astype(BF16)


def side_cell(lane, level, cols):
    west = lane // (GROUP * HB) == level
    return jnp.where(west, lane % HB - HB, cols + lane % HB)


def weigh(cell, index, weight):
    cell = cell.astype(F32)
    return jnp.where(cell == index, 1.0 - weight, 0.0) + jnp.where(cell == index + 1.0, weight, 0.0)


class Link:
    def __init__(self, axis, step, src, dst, send, recv, slot, also=None):
        me, count = lax.axis_index(axis), lax.axis_size(axis)
        target = me + step
        self.sends = self.gets = None
        if axis == "gx":
            target = lax.rem(target + count, count)
        elif axis == "gy":
            self.sends = (target >= 0) & (target < count)
            self.gets = (me - step >= 0) & (me - step < count)
        self.dst = dst
        device = {axis: target} if also is None else {axis: target, "ma": also}
        self.copy = pltpu.make_async_remote_copy(
            src_ref=src,
            dst_ref=dst,
            send_sem=send.at[slot],
            recv_sem=recv.at[slot],
            device_id=device,
            device_id_type=MESH,
        )

    def start(self):
        if self.sends is None:
            self.copy.start()
        else:
            pl.when(self.sends)(self.copy.start)

    def arrive(self):
        if self.gets is None:
            self.copy.wait_recv()
        else:
            pl.when(self.gets)(self.copy.wait_recv)

            @pl.when(jnp.logical_not(self.gets))
            def _():
                self.dst[...] = jnp.zeros_like(self.dst)

    def sent(self):
        if self.sends is None:
            self.copy.wait_send()
        else:
            pl.when(self.sends)(self.copy.wait_send)


def greet():
    barrier = pltpu.get_barrier_semaphore()
    gx, gxn = lax.axis_index("gx"), lax.axis_size("gx")
    gy, gyn = lax.axis_index("gy"), lax.axis_size("gy")
    ma, count = lax.axis_index("ma"), lax.axis_size("ma")
    for step in (1, gxn - 1):
        pl.semaphore_signal(
            barrier, inc=1, device_id={"gx": lax.rem(gx + step, gxn)}, device_id_type=MESH
        )
    for s in range(1, count):
        pl.semaphore_signal(
            barrier, inc=1, device_id={"ma": lax.rem(ma + s, count)}, device_id_type=MESH
        )
    for step, there in ((-1, gy > 0), (1, gy < gyn - 1)):

        @pl.when(there)
        def _(step=step):
            for s in range(count):
                pl.semaphore_signal(
                    barrier,
                    inc=1,
                    device_id={"gy": gy + step, "ma": lax.rem(ma + s, count)},
                    device_id_type=MESH,
                )

    below, above = jnp.minimum(gy, 1), jnp.minimum(gyn - 1 - gy, 1)
    pl.semaphore_wait(barrier, 2 + (count - 1) + (below + above) * count)


def core_kernel(
    widths, lat_i, lat_w, lon_i, lon_w, alpha, perts, innov, weight,
    increment, residual, p_north, p_south, p_west, p_east, lon_taps, lat_back,
    a_tile, p_tile, fine_tile, pick, edge_taps, lat_fore, v_strip, v_side, p_right, p_left,
    f_low, f_high, f_right, f_left, f_west, f_east, fine_wide,
    lat_i_low, lat_i_high, lat_w_low, lat_w_high, lon_i_west, lon_i_east, lon_w_west, lon_w_east,
    up_lon, up_lat, down_lat, down_lon, ext, other, low, high, to_east, to_west, from_west, from_east,
    send, recv, local,
):
    members, levels, rows, cols = alpha.shape
    steps, half, slots = members // GROUP, rows // 2, GROUP * HB
    frows, fcols = innov.shape[1:]
    fhalf = frows // 2
    ma, count = lax.axis_index("ma"), lax.axis_size("ma")
    loads = [
        pltpu.make_async_copy(src, dst, local.at[i])
        for i, (src, dst) in enumerate(
            (
                (perts, p_tile),
                (innov.at[ma], fine_tile.at[0]),
                (weight.at[ma], fine_tile.at[1]),
                (alpha, a_tile),
            )
        )
    ]
    for load in loads:
        load.start()
    counter = iter(range(96))
    pending = []

    def link(axis, step, src, dst, also=None):
        one = Link(axis, step, src, dst, send, recv, next(counter), also)
        pending.append(one)
        return one

    r, c = iota((cols, 2 * cols), 0), iota((cols, 2 * cols), 1)
    base = jnp.where(
        ((c < cols) & (r - (cols - HB) == c % HB)) | ((c >= cols) & (r == c % HB)), 1.0, 0.0
    )
    turned = (c % cols) // slots
    slot = jnp.where(c < cols, turned, 1 - turned) * GROUP + c % slots // HB
    for l in range(levels):
        for k in range(GROUP):
            at = slice(k % 2 * cols, (k % 2 + 1) * cols)
            n = l * GROUP + k
            pick[n // 2, at] = jnp.where(slot == n, base, 0.0).astype(BF16)
    greet()

    f_rows = [
        link("gy", 1, innov.at[ma, pl.ds(frows - FR, FR)], f_low.at[0]),
        link("gy", -1, innov.at[ma, pl.ds(0, FR)], f_high.at[0]),
        link("gy", 1, weight.at[ma, pl.ds(frows - FR, FR)], f_low.at[1]),
        link("gy", -1, weight.at[ma, pl.ds(0, FR)], f_high.at[1]),
    ]
    p_rows = [
        link("gy", 1, perts.at[:, :, pl.ds(rows - HB, HB), :], p_north),
        link("gy", -1, perts.at[:, :, pl.ds(0, HB), :], p_south),
    ]
    small = [
        link("gy", 1, lat_i, lat_i_low),
        link("gy", -1, lat_i, lat_i_high),
        link("gy", 1, lat_w, lat_w_low),
        link("gy", -1, lat_w, lat_w_high),
        link("gx", 1, lon_i, lon_i_west),
        link("gx", -1, lon_i, lon_i_east),
        link("gx", 1, lon_w, lon_w_west),
        link("gx", -1, lon_w, lon_w_east),
    ]
    for one in small + f_rows + p_rows:
        one.start()

    def f_edge(top, bottom, start):
        return lanes_of(*[part[i, :, start : start + FC] for part in (top, bottom) for i in range(2)])

    def f_sides(span):
        pair = [
            link("gx", 1, f_right.at[span], f_west.at[span]),
            link("gx", -1, f_left.at[span], f_east.at[span]),
        ]
        for one in pair:
            one.start()
        return pair

    for load in loads[1:3]:
        load.wait()
    for dst, start in ((f_right, fcols - FC), (f_left, 0)):
        dst[:fhalf] = f_edge(fine_tile.at[:, :fhalf], fine_tile.at[:, fhalf:], start)
    f_arrive = f_sides(pl.ds(0, fhalf))

    def packed(piece):
        total = None
        for l in range(levels):
            for k in range(0, GROUP, 2):
                n = (l * GROUP + k) // 2
                part = dot(lanes_of(piece(l, k), piece(l, k + 1)), pick[n])
                total = part if total is None else total + part
        return total.astype(BF16)

    loads[0].wait()
    p_arrive = []
    for g in range(steps):
        both = packed(lambda l, k: p_tile[g * GROUP + k, l])
        p_right[g, :rows] = both[:, :cols]
        p_left[g, :rows] = both[:, cols:]
        span = pl.ds(0, rows)
        pair = [
            link("gx", 1, p_right.at[g, span], p_west.at[g, span]),
            link("gx", -1, p_left.at[g, span], p_east.at[g, span]),
        ]
        for one in pair:
            one.start()
        p_arrive += pair

    lane = iota((cols, cols), 1)
    deep = half + 2 * HB
    wide_k = lat_fore.shape[3]
    for l in range(levels):
        spread = widths[l].astype(F32)
        scale = tap_scale(spread)
        cell, at = iota((cols, cols), 0), lane
        lon_taps[l, 0], lon_taps[l, 1] = split(tap_value(cell - at, spread, scale))
        lon_taps[l, 2], lon_taps[l, 3] = split(tap_value(side_cell(cell, l, cols) - at, spread, scale))
        edge_taps[l, 0], edge_taps[l, 1] = split(tap_value(side_cell(at, l, cols) - cell, spread, scale))
        lat_back[l] = lat_taps(spread, scale, half, deep, -HB, wide_k)
        lat_fore[l, 0] = lat_taps(spread, scale, deep, deep, HB, wide_k)
        lat_fore[l, 1] = lat_taps(spread, scale, deep, deep, -2 * HB, wide_k)
    loads[3].wait()

    def tall(u, l):
        h, lo = split(u)
        out = []
        for b in range(2):
            at = slice(b * (rows - deep), b * (rows - deep) + deep)
            stack = rows_of(h[at], h[at], lo[at])
            out.append(dot(lat_fore[l, b, :, : 3 * deep], stack)[: half + HB])
        return out

    for l in range(levels):
        ext[l, HB : HB + rows, :cols] = jnp.zeros((rows, cols), F32)

    @pl.loop(0, steps)
    def _(g):
        for l in range(levels):
            taps = rows_of(
                lanes_of(lon_taps[l, 0], edge_taps[l, 0]), lanes_of(lon_taps[l, 1], edge_taps[l, 1])
            )
            side = total = None
            for k in range(0, GROUP, 2):
                cores = []
                for m in (k, k + 1):
                    a = a_tile[g * GROUP + m, l]
                    u = dot(lanes_of(a, a), taps)
                    cores.append(u[:, :cols])
                    mine = lane % slots // HB == m
                    side = u[:, cols:] if side is None else jnp.where(mine, u[:, cols:], side)
                top, bottom = tall(lanes_of(*cores), l)
                for i, m in enumerate((k, k + 1)):
                    at = slice(i * cols, (i + 1) * cols)
                    v = rows_of(top[HB:, at], bottom[:half, at])
                    part = p_tile[g * GROUP + m, l].astype(F32) * v
                    total = part if total is None else total + part
                    v_strip[g * GROUP + m, l] = rows_of(top[:HB, at], bottom[half:, at])
            ext[l, HB : HB + rows, :cols] += total
            v_side[g, l] = rows_of(*tall(side, l))

    for one in p_rows:
        one.arrive()

    both = packed(
        lambda l, k: rows_of(
            *[
                part[g * GROUP + k, l].astype(F32)
                for g in range(steps)
                for part in (p_north, p_south)
            ]
        ).astype(BF16)
    )
    for g in range(steps):
        at = slice(2 * HB * g, 2 * HB * (g + 1))
        p_right[g, rows:] = both[at, :cols]
        p_left[g, rows:] = both[at, cols:]
    span = pl.ds(rows, 2 * HB)
    corners = [
        link("gx", 1, p_right.at[:, span], p_west.at[:, span]),
        link("gx", -1, p_left.at[:, span], p_east.at[:, span]),
    ]
    for one in corners:
        one.start()
    p_arrive += corners
    for one in f_rows:
        one.arrive()
    for dst, start in ((f_right, fcols - FC), (f_left, 0)):
        dst[fhalf:] = f_edge(f_low, f_high, start)
    f_arrive += f_sides(pl.ds(fhalf, FR))

    for one in small:
        one.arrive()
    lat_at = lanes_of(lat_i[...], lat_i_low[:, frows - FR :], lat_i_high[:, :FR]).astype(F32)
    lat_by = lanes_of(lat_w[...], lat_w_low[:, frows - FR :], lat_w_high[:, :FR])
    lat_at = lat_at - (lax.axis_index("gy") * rows).astype(F32)
    lon_at = lanes_of(lon_i[...], lon_i_west[:, fcols - FC :], lon_i_east[:, :FC]).astype(F32)
    lon_by = lanes_of(lon_w[...], lon_w_west[:, fcols - FC :], lon_w_east[:, :FC])
    lon_total = float(cols * lax.axis_size("gx"))
    lon_at = lon_at - (lax.axis_index("gx") * cols).astype(F32)
    lon_at = jnp.where(
        lon_at < -64.0, lon_at + lon_total, jnp.where(lon_at >= lon_total - 64.0, lon_at - lon_total, lon_at)
    )
    f_tall, f_wide = frows + 2 * FR, fcols + 2 * FC

    def upright(at, by):
        size = at.shape[1]
        space = jnp.zeros((1, -size % 128), F32)
        at, by = lanes_of(at, space), lanes_of(by, space)
        shape = (8, at.shape[1])
        both = jnp.where(iota(shape, 0) == 0, jnp.broadcast_to(at, shape), jnp.broadcast_to(by, shape))
        both = both.T[:size]
        return both[:, 0:1], both[:, 1:2]

    lat_at_up, lat_by_up = upright(lat_at, lat_by)
    lon_at_up, lon_by_up = upright(lon_at, lon_by)
    t_rows, e_rows = rows + 2 * CR, rows + 2 * HB
    up_lat[0], up_lat[1] = split(weigh(iota((f_tall, t_rows), 1) - CR, lat_at_up, lat_by_up))
    down_lat[0], down_lat[1] = split(weigh(iota((e_rows, f_tall), 0) - HB, lat_at, lat_by))
    order = iota((2 * cols, f_wide), 0)
    w = order - cols
    wing = jnp.where(
        w < REACH,
        w - (REACH - HB),
        jnp.where(
            (w >= slots - HB) & (w < slots),
            w - slots,
            jnp.where(
                (w >= slots) & (w < slots + REACH),
                w - slots + cols - HB,
                jnp.where(w >= cols - HB, w + HB, -1000),
            ),
        ),
    )
    up_lon[0], up_lon[1] = split(weigh(jnp.where(w < 0, order, wing), lon_at, lon_by))
    order = iota((f_wide, 2 * cols), 1)
    cell = jnp.where(order < cols, order, side_cell(order - cols, ma, cols))
    down_lon[0], down_lon[1] = split(weigh(cell, lon_at_up, lon_by_up))

    for l in range(levels):

        def strips(g, sums):
            north, south = sums
            for k in range(GROUP):
                m = g * GROUP + k
                north = north + p_north[m, l].astype(F32) * v_strip[m, l, :HB]
                south = south + p_south[m, l].astype(F32) * v_strip[m, l, HB:]
            return north, south

        zero = jnp.zeros((HB, cols), F32)
        north, south = lax.fori_loop(0, steps, strips, (zero, zero))
        ext[l, :HB, :cols] = north
        ext[l, HB + rows :, :cols] = south

    for one in f_arrive:
        one.arrive()
    for i in range(2):

        def wing_of(part):
            x, y = FC * i, 2 * FC + FC * i
            return rows_of(
                part[:fhalf, x : x + FC],
                part[:fhalf, y : y + FC],
                part[fhalf:, x : x + FC],
                part[fhalf:, y : y + FC],
            )

        fine_wide[i] = lanes_of(
            rows_of(fine_tile[i], f_low[i], f_high[i]), wing_of(f_west), wing_of(f_east)
        )

    for one in p_arrive:
        one.arrive()
    tall_lane = iota((e_rows, cols), 1)
    for l in range(levels):
        total = None
        for g in range(steps):
            side = jnp.where(
                tall_lane // slots == l, p_west[g].astype(F32), p_east[g].astype(F32)
            )
            part = natural(side, rows) * v_side[g, l]
            total = part if total is None else total + part
        ext[l, :, cols:] = total if l == 0 else pltpu.roll(total, slots, 1)

    swaps, lows, highs = [], [], []
    for s in range(count):
        peer = lax.rem(ma + s, count)
        if s:
            swaps.append(link("ma", peer - ma, ext.at[peer], other.at[s - 1]))
        lows.append(link("gy", 1, ext.at[peer, pl.ds(e_rows - STRIP, STRIP)], low.at[s], peer))
        highs.append(link("gy", -1, ext.at[peer, pl.ds(0, STRIP)], high.at[s], peer))
    for one in lows + highs + swaps:
        one.start()
    for one in swaps + lows + highs:
        one.arrive()
    mine = ext[ma]
    for s in range(count - 1):
        mine = mine + other[s]
    above, below = low[0], high[0]
    for s in range(1, count):
        above, below = above + low[s], below + high[s]
    lap = CR - HB
    edge = STRIP - lap
    mine = rows_of(
        above[:lap],
        mine[:edge] + above[lap:],
        mine[edge : e_rows - edge],
        mine[e_rows - edge :] + below[:edge],
        below[edge:],
    )
    core, side = mine[:, :cols], mine[:, cols:]
    for shift in (HB, 2 * HB, 4 * HB):
        side = side + pltpu.roll(side, shift, 1)

    blocks = (t_rows + STRIP - 1) // STRIP
    t_lane = iota((t_rows, cols), 1)
    thin = iota((STRIP, cols), 1)

    def fold(x, first):
        if blocks * STRIP > t_rows:
            x = rows_of(x, jnp.zeros((blocks * STRIP - t_rows, cols), F32))
        total = None
        for b in range(blocks):
            part = pltpu.roll(x[b * STRIP : (b + 1) * STRIP], (b * REACH - first) % cols, 1)
            total = part if total is None else jnp.where(thin >= b * REACH, part, total)
        return total

    def unfold(x, first):
        parts = [pltpu.roll(x, (first - b * REACH) % cols, 1) for b in range(blocks)]
        return rows_of(*parts)[:t_rows]

    eastward = jnp.where(t_lane >= cols - HB, side, pltpu.roll(core, cols - HB, 1))
    westward = jnp.where(t_lane < slots, side, pltpu.roll(core, slots, 1))
    to_east[...] = fold(eastward, cols - REACH)
    to_west[...] = fold(westward, slots - HB)
    sides = [
        link("gx", 1, to_east, from_west),
        link("gx", -1, to_west, from_east),
    ]
    for one in sides:
        one.start()
    for one in sides:
        one.arrive()
    wings = jnp.where(
        t_lane < REACH,
        unfold(from_west[...], 0),
        jnp.where((t_lane >= slots) & (t_lane < slots + REACH), unfold(from_east[...], slots), side),
    )
    across = dot3(split(lanes_of(core, wings)), (up_lon[0], up_lon[1]))
    fine = dot3((up_lat[0], up_lat[1]), split(across))
    increment[ma] = fine[:frows, :fcols]
    misfit = fine_wide[1] * (fine - fine_wide[0])
    across = dot3((down_lat[0], down_lat[1]), split(misfit))
    residual[ma] = dot3(split(across), (down_lon[0], down_lon[1]))
    ends = []
    for s in range(1, count):
        peer = lax.rem(ma + s, count)
        for whole in (residual, increment):
            ends.append(link("ma", peer - ma, whole.at[ma], whole.at[ma]))
    for one in ends:
        one.start()
    for one in ends:
        one.arrive()
    for one in pending:
        one.sent()


def cost(flops, nbytes):
    return pl.CostEstimate(flops=flops, bytes_accessed=nbytes, transcendentals=0)


def core_step(widths, lat_i, lat_w, lon_i, lon_w, alpha, perts, innov, weight):
    members, levels, rows, cols = alpha.shape
    steps = members // GROUP
    frows, fcols = innov.shape[1:]
    count = lax.axis_size("ma")
    assert levels == 2 and count == levels
    half = rows // 2
    deep = half + 2 * HB
    wide_k = -(-3 * deep // 128) * 128
    e_rows, t_rows = rows + 2 * HB, rows + 2 * CR
    f_tall, f_wide = frows + 2 * FR, fcols + 2 * FC
    strip = ((members, levels, HB, cols), BF16)
    side = ((steps, e_rows, cols), BF16)
    outs = [
        (innov.shape, F32),
        ((levels, e_rows, 2 * cols), F32),
        strip,
        strip,
        side,
        side,
        ((levels, 4, cols, cols), BF16),
        ((levels, half, wide_k), BF16),
    ]
    fine_edge = ((2, FR, fcols), F32)
    fine_side = ((frows // 2 + FR, 4 * FC), F32)
    scratch = [
        (alpha.shape, BF16),
        (alpha.shape, BF16),
        ((2, frows, fcols), F32),
        ((levels * GROUP // 2, 2 * cols, 2 * cols), BF16),
        ((levels, 2, cols, cols), BF16),
        ((levels, 2, deep, wide_k), BF16),
        ((members, levels, 2 * HB, cols), F32),
        ((steps, levels, e_rows, cols), F32),
        side,
        side,
        fine_edge,
        fine_edge,
        fine_side,
        fine_side,
        fine_side,
        fine_side,
        ((2, f_tall, f_wide), F32),
        (lat_i.shape, jnp.int32),
        (lat_i.shape, jnp.int32),
        (lat_w.shape, F32),
        (lat_w.shape, F32),
        (lon_i.shape, jnp.int32),
        (lon_i.shape, jnp.int32),
        (lon_w.shape, F32),
        (lon_w.shape, F32),
        ((2, 2 * cols, f_wide), BF16),
        ((2, f_tall, t_rows), BF16),
        ((2, e_rows, f_tall), BF16),
        ((2, f_wide, 2 * cols), BF16),
        ((levels, e_rows, 2 * cols), F32),
        ((count - 1, e_rows, 2 * cols), F32),
        ((count, STRIP, 2 * cols), F32),
        ((count, STRIP, 2 * cols), F32),
    ] + [((STRIP, cols), F32)] * 4
    vmem = pl.BlockSpec(memory_space=pltpu.VMEM)
    anywhere = pl.BlockSpec(memory_space=pl.ANY)
    return pl.pallas_call(
        core_kernel,
        in_specs=[pl.BlockSpec(memory_space=pltpu.SMEM)] + [vmem] * 4 + [anywhere] * 4,
        out_specs=[vmem] * len(outs),
        out_shape=[jax.ShapeDtypeStruct(shape, kind) for shape, kind in outs],
        scratch_shapes=[pltpu.VMEM(shape, kind) for shape, kind in scratch]
        + [
            pltpu.SemaphoreType.DMA((96,)),
            pltpu.SemaphoreType.DMA((96,)),
            pltpu.SemaphoreType.DMA((4,)),
        ],
        compiler_params=pltpu.CompilerParams(
            collective_id=0, has_side_effects=True, vmem_limit_bytes=VMEM_LIMIT
        ),
        cost_estimate=cost(2**30, 2**24),
    )(widths, lat_i, lat_w, lon_i, lon_w, alpha, perts, innov, weight)


def band(high, low, taps):
    half = taps.shape[0]
    deep = half + 2 * HB
    out = []
    for first in range(0, high.shape[0] - 2 * HB, half):
        h, lo = high[first : first + deep], low[first : first + deep]
        out.append(dot(taps, rows_of(h, h, lo)))
    return rows_of(*out)


def adjoint_kernel(alpha, perts, north, south, west, east, residual, lon, lat, out):
    rows, cols = alpha.shape[2:]
    slots = GROUP * HB
    l = pl.program_id(1)
    res = residual[l]
    wide = iota((rows + 2 * HB, cols), 1)
    side = jnp.where(wide // slots == l, west[0].astype(F32), east[0].astype(F32))
    side = natural(side, rows) * res[:, cols:]
    taps = lat[l, :, : 3 * (rows // 2 + 2 * HB)]
    zero = jnp.zeros((cols, cols), BF16)

    def stack(high, low):
        return rows_of(lanes_of(high, low), lanes_of(high, zero))

    core, wing = stack(lon[l, 0], lon[l, 1]), stack(lon[l, 2], lon[l, 3])
    edge_h, edge_l = split(band(*split(side), taps))
    lane = iota((rows, cols), 1)
    for k in range(0, GROUP, 2):
        pairs = []
        for m in (k, k + 1):
            tall = rows_of(north[m, 0].astype(F32), perts[m, 0].astype(F32), south[m, 0].astype(F32))
            pairs.append(split(tall * res[:, :cols]))
        both = band(lanes_of(pairs[0][0], pairs[1][0]), lanes_of(pairs[0][1], pairs[1][1]), taps)
        for i, m in enumerate((k, k + 1)):
            mine = lane % slots // HB == m
            edges = lanes_of(
                jnp.where(mine, edge_h, jnp.zeros_like(edge_h)),
                jnp.where(mine, edge_l, jnp.zeros_like(edge_l)),
            )
            total = dot(lanes_of(*split(both[:, i * cols : (i + 1) * cols])), core) + dot(edges, wing)
            out[m, 0] = alpha[m, 0].astype(F32) + (total[:, :cols] + total[:, cols:])


def adjoint(alpha, perts, north, south, west, east, residual, lon, lat):
    members, levels, rows, cols = alpha.shape
    block = pl.BlockSpec((GROUP, 1, rows, cols), lambda g, l: (g, l, 0, 0))
    strip = pl.BlockSpec((GROUP, 1, HB, cols), lambda g, l: (g, l, 0, 0))
    side = pl.BlockSpec((1, rows + 2 * HB, cols), lambda g, l: (g, 0, 0))

    def whole(x):
        return pl.BlockSpec(x.shape, lambda g, l: (0,) * x.ndim)

    return pl.pallas_call(
        adjoint_kernel,
        grid=(members // GROUP, levels),
        in_specs=[block, block, strip, strip, side, side, whole(residual), whole(lon), whole(lat)],
        out_specs=block,
        out_shape=jax.ShapeDtypeStruct(alpha.shape, F32),
        cost_estimate=cost(members * levels * 2**25, alpha.size * 8),
    )(alpha, perts, north, south, west, east, residual, lon, lat)


def body(
    alpha_fields,
    member_perts,
    band_widths,
    lat_index,
    lat_weight,
    lon_index,
    lon_weight,
    innovation,
    obs_weight,
):
    tables = [x.reshape(1, -1) for x in (lat_index, lat_weight, lon_index, lon_weight)]
    increment, residual, *halos = core_step(
        band_widths, *tables, alpha_fields, member_perts, innovation, obs_weight
    )
    north, south, west, east, lon, lat = halos
    gradient = adjoint(alpha_fields, member_perts, north, south, west, east, residual, lon, lat)
    return (increment, gradient)


def solution(mesh):
    placed = (
        P("ma", None, "gy", "gx"),
        P("ma", None, "gy", "gx"),
        P(),
        P("gy"),
        P("gy"),
        P("gx"),
        P("gx"),
        P(None, "gy", "gx"),
        P(None, "gy", "gx"),
    )
    return jax.shard_map(
        body,
        mesh=mesh,
        in_specs=placed,
        out_specs=(P(None, "gy", "gx"), P("ma", None, "gy", "gx")),
        check_vma=False,
    )
```

```python
import jax
import jax.numpy as jnp
from jax import lax
from jax.experimental import pallas as pl
from jax.experimental.pallas import tpu as pltpu
from jax.sharding import PartitionSpec as P

HB = 8
GROUP = 8
FR = 24
FC = 20
FOLD = 3
CR = 16
STRIP = 24
REACH = HB + 10
MESH = pl.DeviceIdType.MESH
VMEM_LIMIT = 60 * 2**20
F32 = jnp.float32
BF16 = jnp.bfloat16


def iota(shape, dim):
    return lax.broadcasted_iota(jnp.int32, shape, dim)


def dot(a, b):
    return jnp.dot(a, b, preferred_element_type=F32)


def split(value):
    high = value.astype(BF16)
    return high, (value - high.astype(F32)).astype(BF16)


def dot3(a, b):
    return dot(a[0], b[0]) + dot(a[1], b[0]) + dot(a[0], b[1])


def rows_of(*parts):
    return jnp.concatenate(parts, axis=0)


def lanes_of(*parts):
    return jnp.concatenate(parts, axis=1)


def natural(x, rows):
    return rows_of(x[rows : rows + HB], x[:rows], x[rows + HB :])


def place(order, size, width):
    return jnp.where(order < size, order, jnp.where(order < size + width, order - size - width, order - width))


def tap_value(distance, spread, scale):
    d = distance.astype(F32)
    value = jnp.exp(-(d * d) / (2.0 * spread * spread)) * scale
    return jnp.where(jnp.abs(distance) <= HB, value, 0.0)


def tap_scale(spread):
    lane = iota((8, 128), 1)
    d = (lane - HB).astype(F32)
    shape = jnp.where(lane <= 2 * HB, jnp.exp(-(d * d) / (2.0 * spread * spread)), 0.0)
    return (1.0 / jnp.sqrt(jnp.sum(shape * shape, axis=1, keepdims=True)))[:1]


def lat_taps(spread, scale, height, deep, offset, width):
    i, c = iota((height, width), 0), iota((height, width), 1)
    r = jnp.where(c >= 2 * deep, c - 2 * deep, jnp.where(c >= deep, c - deep, c))
    value = tap_value(r - i + offset, spread, scale)
    high = value.astype(BF16).astype(F32)
    return jnp.where((c >= deep) & (c < 2 * deep), value - high, high).astype(BF16)


def side_cell(lane, level, cols):
    west = lane // (GROUP * HB) == level
    return jnp.where(west, lane % HB - HB, cols + lane % HB)


def weigh(cell, index, weight):
    cell = cell.astype(F32)
    return jnp.where(cell == index, 1.0 - weight, 0.0) + jnp.where(cell == index + 1.0, weight, 0.0)


class Link:
    def __init__(self, axis, step, src, dst, send, recv, slot, also=None):
        me, count = lax.axis_index(axis), lax.axis_size(axis)
        target = me + step
        self.sends = self.gets = None
        if axis == "gx":
            target = lax.rem(target + count, count)
        elif axis == "gy":
            self.sends = (target >= 0) & (target < count)
            self.gets = (me - step >= 0) & (me - step < count)
        self.dst = dst
        device = {axis: target, **(also or {})}
        self.copy = pltpu.make_async_remote_copy(
            src_ref=src,
            dst_ref=dst,
            send_sem=send.at[slot],
            recv_sem=recv.at[slot],
            device_id=device,
            device_id_type=MESH,
        )

    def start(self):
        if self.sends is None:
            self.copy.start()
        else:
            pl.when(self.sends)(self.copy.start)

    def arrive(self):
        if self.gets is None:
            self.copy.wait_recv()
        else:
            pl.when(self.gets)(self.copy.wait_recv)

            @pl.when(jnp.logical_not(self.gets))
            def _():
                self.dst[...] = jnp.zeros_like(self.dst)

    def sent(self):
        if self.sends is None:
            self.copy.wait_send()
        else:
            pl.when(self.sends)(self.copy.wait_send)


def greet():
    barrier = pltpu.get_barrier_semaphore()
    gx, gxn = lax.axis_index("gx"), lax.axis_size("gx")
    gy, gyn = lax.axis_index("gy"), lax.axis_size("gy")
    ma, count = lax.axis_index("ma"), lax.axis_size("ma")
    for step in (1, gxn - 1):
        pl.semaphore_signal(
            barrier, inc=1, device_id={"gx": lax.rem(gx + step, gxn)}, device_id_type=MESH
        )
    for s in range(1, count):
        pl.semaphore_signal(
            barrier, inc=1, device_id={"ma": lax.rem(ma + s, count)}, device_id_type=MESH
        )
    for step, there in ((-1, gy > 0), (1, gy < gyn - 1)):

        @pl.when(there)
        def _(step=step):
            for s in range(count):
                pl.semaphore_signal(
                    barrier,
                    inc=1,
                    device_id={"gy": gy + step, "ma": lax.rem(ma + s, count)},
                    device_id_type=MESH,
                )
            for side in (1, gxn - 1):
                pl.semaphore_signal(
                    barrier,
                    inc=1,
                    device_id={"gx": lax.rem(gx + side, gxn), "gy": gy + step},
                    device_id_type=MESH,
                )

    below, above = jnp.minimum(gy, 1), jnp.minimum(gyn - 1 - gy, 1)
    pl.semaphore_wait(barrier, 2 + (count - 1) + (below + above) * (count + 2))


def core_kernel(
    widths, lat_i, lat_w, lon_i, lon_w, alpha, perts, innov, weight,
    increment, residual, p_north, p_south, p_west, p_east, lon_taps, lat_back,
    a_tile, p_tile, fine_tile, pick, edge_taps, lat_fore, v_strip, v_side, p_right, p_left,
    f_low, f_high, f_right, f_left, f_west, f_east, fine_wide,
    lat_i_low, lat_i_high, lat_w_low, lat_w_high, lon_i_west, lon_i_east, lon_w_west, lon_w_east,
    up_lon, up_lat, down_lat, down_lon, ext, other, low, high, to_east, to_west, from_west, from_east,
    send, recv, local,
):
    members, levels, rows, cols = alpha.shape
    steps, half, slots = members // GROUP, rows // 2, GROUP * HB
    frows, fcols = innov.shape[1:]
    ma, count = lax.axis_index("ma"), lax.axis_size("ma")
    gx, gxn = lax.axis_index("gx"), lax.axis_size("gx")
    f_loads = [
        pltpu.make_async_copy(src.at[ma], fine_tile.at[i], local.at[i])
        for i, src in enumerate((innov, weight))
    ]

    def group_load(src, dst, g, first):
        span = pl.ds(g * GROUP, GROUP)
        return pltpu.make_async_copy(src.at[span], dst.at[span], local.at[first + g])

    p_loads = [group_load(perts, p_tile, g, 2) for g in range(steps)]
    for load in f_loads + p_loads:
        load.start()
    counter = iter(range(96))
    pending = []

    def link(axis, step, src, dst, also=None):
        one = Link(axis, step, src, dst, send, recv, next(counter), also)
        pending.append(one)
        return one

    r, c = iota((cols, 2 * cols), 0), iota((cols, 2 * cols), 1)
    base = jnp.where(
        ((c < cols) & (r - (cols - HB) == c % HB)) | ((c >= cols) & (r == c % HB)), 1.0, 0.0
    )
    turned = (c % cols) // slots
    slot = jnp.where(c < cols, turned, 1 - turned) * GROUP + c % slots // HB
    for l in range(levels):
        for k in range(GROUP):
            at = slice(k % 2 * cols, (k % 2 + 1) * cols)
            n = l * GROUP + k
            pick[n // 2, at] = jnp.where(slot == n, base, 0.0).astype(BF16)
    greet()

    f_rows = [
        link("gy", 1, innov.at[ma, pl.ds(frows - FR, FR)], f_low.at[0]),
        link("gy", -1, innov.at[ma, pl.ds(0, FR)], f_high.at[0]),
        link("gy", 1, weight.at[ma, pl.ds(frows - FR, FR)], f_low.at[1]),
        link("gy", -1, weight.at[ma, pl.ds(0, FR)], f_high.at[1]),
    ]
    p_rows = [
        link("gy", 1, perts.at[:, :, pl.ds(rows - HB, HB), :], p_north),
        link("gy", -1, perts.at[:, :, pl.ds(0, HB), :], p_south),
    ]
    small = [
        link("gy", 1, lat_i, lat_i_low),
        link("gy", -1, lat_i, lat_i_high),
        link("gy", 1, lat_w, lat_w_low),
        link("gy", -1, lat_w, lat_w_high),
        link("gx", 1, lon_i, lon_i_west),
        link("gx", -1, lon_i, lon_i_east),
        link("gx", 1, lon_w, lon_w_west),
        link("gx", -1, lon_w, lon_w_east),
    ]
    for one in small + f_rows + p_rows:
        one.start()

    def tilted(src, dst, side, top, bottom, first):
        pairs = []
        for step, at, to in ((1, bottom, first), (-1, top, first + HB)):
            span, there = pl.ds(at, HB), pl.ds(to, HB)
            index = (slice(None),) * (src.ndim - 2)
            pairs.append(
                link(
                    "gy",
                    step,
                    src.at[(*index, span)],
                    dst.at[(*index, there)],
                    {"gx": lax.rem(gx + side, gxn)},
                )
            )
        return pairs

    f_main = f_west.shape[0] - 2 * HB

    def f_fold(first, count, start):
        deep = -(-count // (FOLD * HB)) * HB
        parts = []
        for b in range(FOLD):
            stop = min(first + (b + 1) * deep, first + count)
            for i in range(2):
                part = fine_tile[i, first + b * deep : stop, start : start + FC]
                short = deep - part.shape[0]
                parts.append(rows_of(part, jnp.zeros((short, FC), F32)) if short else part)
        return lanes_of(*parts, jnp.zeros((deep, cols - 2 * FOLD * FC), F32))

    for load in f_loads:
        load.wait()
    f_arrive = []
    for step, side, src, dst, start in (
        (1, 1, f_right, f_west, fcols - FC),
        (-1, gxn - 1, f_left, f_east, 0),
    ):
        src[:f_main] = f_fold(0, frows, start)
        src[f_main : f_main + HB] = f_fold(0, FR, start)
        src[f_main + HB :] = f_fold(frows - FR, FR, start)
        span = pl.ds(0, f_main)
        f_arrive.append(link("gx", step, src.at[span], dst.at[span]))
        f_arrive += tilted(src, dst, side, f_main, f_main + HB, f_main)
    for one in f_arrive:
        one.start()

    def packed(piece):
        total = None
        for l in range(levels):
            for k in range(0, GROUP, 2):
                n = (l * GROUP + k) // 2
                part = dot(lanes_of(piece(l, k), piece(l, k + 1)), pick[n])
                total = part if total is None else total + part
        return total.astype(BF16)

    a_loads = [group_load(alpha, a_tile, g, 2 + steps) for g in range(steps)]
    p_arrive = []
    for g in range(steps):
        p_loads[g].wait()
        a_loads[g].start()
        both = packed(lambda l, k: p_tile[g * GROUP + k, l])
        p_right[g] = both[:, :cols]
        p_left[g] = both[:, cols:]
        span = pl.ds(0, rows)
        pair = [
            link("gx", 1, p_right.at[g], p_west.at[g, span]),
            link("gx", -1, p_left.at[g], p_east.at[g, span]),
        ]
        for one in pair:
            one.start()
        p_arrive += pair
    corners = tilted(p_right, p_west, 1, 0, rows - HB, rows)
    corners += tilted(p_left, p_east, gxn - 1, 0, rows - HB, rows)
    for one in corners:
        one.start()
    p_arrive += corners

    lane = iota((cols, cols), 1)
    deep = half + 2 * HB
    wide_k = lat_fore.shape[3]
    for l in range(levels):
        spread = widths[l].astype(F32)
        scale = tap_scale(spread)
        cell, at = iota((cols, cols), 0), lane
        lon_taps[l, 0], lon_taps[l, 1] = split(tap_value(cell - at, spread, scale))
        lon_taps[l, 2], lon_taps[l, 3] = split(tap_value(side_cell(cell, l, cols) - at, spread, scale))
        edge_taps[l, 0], edge_taps[l, 1] = split(tap_value(side_cell(at, l, cols) - cell, spread, scale))
        lat_back[l] = lat_taps(spread, scale, half, deep, -HB, wide_k)
        lat_fore[l, 0] = lat_taps(spread, scale, deep, deep, HB, wide_k)
        lat_fore[l, 1] = lat_taps(spread, scale, deep, deep, -2 * HB, wide_k)

    def tall(u, l):
        h, lo = split(u)
        out = []
        for b in range(2):
            at = slice(b * (rows - deep), b * (rows - deep) + deep)
            stack = rows_of(h[at], h[at], lo[at])
            out.append(dot(lat_fore[l, b, :, : 3 * deep], stack)[: half + HB])
        return out

    for l in range(levels):
        ext[l, HB : HB + rows, :cols] = jnp.zeros((rows, cols), F32)

    @pl.loop(0, steps)
    def _(g):
        group_load(alpha, a_tile, g, 2 + steps).wait()
        for l in range(levels):
            taps = rows_of(
                lanes_of(lon_taps[l, 0], edge_taps[l, 0]), lanes_of(lon_taps[l, 1], edge_taps[l, 1])
            )
            side = total = None
            for k in range(0, GROUP, 2):
                cores = []
                for m in (k, k + 1):
                    a = a_tile[g * GROUP + m, l]
                    u = dot(lanes_of(a, a), taps)
                    cores.append(u[:, :cols])
                    mine = lane % slots // HB == m
                    side = u[:, cols:] if side is None else jnp.where(mine, u[:, cols:], side)
                top, bottom = tall(lanes_of(*cores), l)
                for i, m in enumerate((k, k + 1)):
                    at = slice(i * cols, (i + 1) * cols)
                    v = rows_of(top[HB:, at], bottom[:half, at])
                    part = p_tile[g * GROUP + m, l].astype(F32) * v
                    total = part if total is None else total + part
                    v_strip[g * GROUP + m, l] = rows_of(top[:HB, at], bottom[half:, at])
            ext[l, HB : HB + rows, :cols] += total
            v_side[g, l] = rows_of(*tall(side, l))

    for one in p_rows:
        one.arrive()

    for one in f_rows:
        one.arrive()
    for one in small:
        one.arrive()
    lat_at = lanes_of(lat_i[...], lat_i_low[:, frows - FR :], lat_i_high[:, :FR]).astype(F32)
    lat_by = lanes_of(lat_w[...], lat_w_low[:, frows - FR :], lat_w_high[:, :FR])
    lat_at = lat_at - (lax.axis_index("gy") * rows).astype(F32)
    lon_at = lanes_of(lon_i[...], lon_i_west[:, fcols - FC :], lon_i_east[:, :FC]).astype(F32)
    lon_by = lanes_of(lon_w[...], lon_w_west[:, fcols - FC :], lon_w_east[:, :FC])
    lon_total = float(cols * lax.axis_size("gx"))
    lon_at = lon_at - (lax.axis_index("gx") * cols).astype(F32)
    lon_at = jnp.where(
        lon_at < -64.0, lon_at + lon_total, jnp.where(lon_at >= lon_total - 64.0, lon_at - lon_total, lon_at)
    )
    f_tall, f_wide = frows + 2 * FR, fcols + 2 * FC

    def upright(at, by):
        size = at.shape[1]
        space = jnp.zeros((1, -size % 128), F32)
        at, by = lanes_of(at, space), lanes_of(by, space)
        shape = (8, at.shape[1])
        both = jnp.where(iota(shape, 0) == 0, jnp.broadcast_to(at, shape), jnp.broadcast_to(by, shape))
        both = both.T[:size]
        return both[:, 0:1], both[:, 1:2]

    lat_at_up, lat_by_up = upright(lat_at, lat_by)
    lon_at_up, lon_by_up = upright(lon_at, lon_by)
    t_rows, e_rows = rows + 2 * CR, rows + 2 * HB
    up_lat[0], up_lat[1] = split(weigh(iota((f_tall, t_rows), 1) - CR, lat_at_up, lat_by_up))
    down_lat[0], down_lat[1] = split(weigh(iota((e_rows, f_tall), 0) - HB, lat_at, lat_by))
    order = iota((2 * cols, f_wide), 0)
    w = order - cols
    wing = jnp.where(
        w < REACH,
        w - (REACH - HB),
        jnp.where(
            (w >= slots - HB) & (w < slots),
            w - slots,
            jnp.where(
                (w >= slots) & (w < slots + REACH),
                w - slots + cols - HB,
                jnp.where(w >= cols - HB, w + HB, -1000),
            ),
        ),
    )
    up_lon[0], up_lon[1] = split(weigh(jnp.where(w < 0, order, wing), lon_at, lon_by))
    order = iota((f_wide, 2 * cols), 1)
    cell = jnp.where(order < cols, order, side_cell(order - cols, ma, cols))
    down_lon[0], down_lon[1] = split(weigh(cell, lon_at_up, lon_by_up))

    for l in range(levels):

        def strips(g, sums):
            north, south = sums
            for k in range(GROUP):
                m = g * GROUP + k
                north = north + p_north[m, l].astype(F32) * v_strip[m, l, :HB]
                south = south + p_south[m, l].astype(F32) * v_strip[m, l, HB:]
            return north, south

        zero = jnp.zeros((HB, cols), F32)
        north, south = lax.fori_loop(0, steps, strips, (zero, zero))
        ext[l, :HB, :cols] = north
        ext[l, HB + rows :, :cols] = south

    for one in f_arrive:
        one.arrive()
    for i in range(2):

        def wing_of(part):
            def opened(first, last):
                lanes = range(FC * i, 2 * FOLD * FC, 2 * FC)
                return [part[first:last, x : x + FC] for x in lanes]

            low, high = f_main, f_main + HB
            return rows_of(
                rows_of(*opened(0, low))[:frows], *opened(low, high), *opened(high, high + HB)
            )

        fine_wide[i] = lanes_of(
            rows_of(fine_tile[i], f_low[i], f_high[i]), wing_of(f_west), wing_of(f_east)
        )

    for one in p_arrive:
        one.arrive()
    tall_lane = iota((e_rows, cols), 1)
    for l in range(levels):
        total = None
        for g in range(steps):
            side = jnp.where(
                tall_lane // slots == l, p_west[g].astype(F32), p_east[g].astype(F32)
            )
            part = natural(side, rows) * v_side[g, l]
            total = part if total is None else total + part
        ext[l, :, cols:] = total if l == 0 else pltpu.roll(total, slots, 1)

    swaps, lows, highs = [], [], []
    for s in range(count):
        peer = lax.rem(ma + s, count)
        if s:
            swaps.append(link("ma", peer - ma, ext.at[peer], other.at[s - 1]))
        lows.append(link("gy", 1, ext.at[peer, pl.ds(e_rows - STRIP, STRIP)], low.at[s], {"ma": peer}))
        highs.append(link("gy", -1, ext.at[peer, pl.ds(0, STRIP)], high.at[s], {"ma": peer}))
    for one in lows + highs + swaps:
        one.start()
    for one in swaps + lows + highs:
        one.arrive()
    mine = ext[ma]
    for s in range(count - 1):
        mine = mine + other[s]
    above, below = low[0], high[0]
    for s in range(1, count):
        above, below = above + low[s], below + high[s]
    lap = CR - HB
    edge = STRIP - lap
    mine = rows_of(
        above[:lap],
        mine[:edge] + above[lap:],
        mine[edge : e_rows - edge],
        mine[e_rows - edge :] + below[:edge],
        below[edge:],
    )
    core, side = mine[:, :cols], mine[:, cols:]
    for shift in (HB, 2 * HB, 4 * HB):
        side = side + pltpu.roll(side, shift, 1)

    blocks = (t_rows + STRIP - 1) // STRIP
    t_lane = iota((t_rows, cols), 1)
    thin = iota((STRIP, cols), 1)

    def fold(x, first):
        if blocks * STRIP > t_rows:
            x = rows_of(x, jnp.zeros((blocks * STRIP - t_rows, cols), F32))
        total = None
        for b in range(blocks):
            part = pltpu.roll(x[b * STRIP : (b + 1) * STRIP], (b * REACH - first) % cols, 1)
            total = part if total is None else jnp.where(thin >= b * REACH, part, total)
        return total

    def unfold(x, first):
        parts = [pltpu.roll(x, (first - b * REACH) % cols, 1) for b in range(blocks)]
        return rows_of(*parts)[:t_rows]

    eastward = jnp.where(t_lane >= cols - HB, side, pltpu.roll(core, cols - HB, 1))
    westward = jnp.where(t_lane < slots, side, pltpu.roll(core, slots, 1))
    to_east[...] = fold(eastward, cols - REACH)
    to_west[...] = fold(westward, slots - HB)
    sides = [
        link("gx", 1, to_east, from_west),
        link("gx", -1, to_west, from_east),
    ]
    for one in sides:
        one.start()
    for one in sides:
        one.arrive()
    wings = jnp.where(
        t_lane < REACH,
        unfold(from_west[...], 0),
        jnp.where((t_lane >= slots) & (t_lane < slots + REACH), unfold(from_east[...], slots), side),
    )
    across = dot3(split(lanes_of(core, wings)), (up_lon[0], up_lon[1]))
    fine = dot3((up_lat[0], up_lat[1]), split(across))
    increment[ma] = fine[:frows, :fcols]
    ends = []

    def share(whole):
        for s in range(1, count):
            peer = lax.rem(ma + s, count)
            ends.append(link("ma", peer - ma, whole.at[ma], whole.at[ma]))
            ends[-1].start()

    share(increment)
    misfit = fine_wide[1] * (fine - fine_wide[0])
    across = dot3((down_lat[0], down_lat[1]), split(misfit))
    residual[ma] = dot3(split(across), (down_lon[0], down_lon[1]))
    share(residual)
    for one in ends:
        one.arrive()
    for one in pending:
        one.sent()


def cost(flops, nbytes):
    return pl.CostEstimate(flops=flops, bytes_accessed=nbytes, transcendentals=0)


def core_step(widths, lat_i, lat_w, lon_i, lon_w, alpha, perts, innov, weight):
    members, levels, rows, cols = alpha.shape
    steps = members // GROUP
    frows, fcols = innov.shape[1:]
    count = lax.axis_size("ma")
    assert levels == 2 and count == levels
    half = rows // 2
    deep = half + 2 * HB
    wide_k = -(-3 * deep // 128) * 128
    e_rows, t_rows = rows + 2 * HB, rows + 2 * CR
    f_tall, f_wide = frows + 2 * FR, fcols + 2 * FC
    strip = ((members, levels, HB, cols), BF16)
    side = ((steps, e_rows, cols), BF16)
    outs = [
        (innov.shape, F32),
        ((levels, e_rows, 2 * cols), F32),
        strip,
        strip,
        side,
        side,
        ((levels, 4, cols, cols), BF16),
        ((levels, half, wide_k), BF16),
    ]
    fine_edge = ((2, FR, fcols), F32)
    fine_side = ((-(-frows // (FOLD * HB)) * HB + 2 * HB, cols), F32)
    packed = ((steps, rows, cols), BF16)
    scratch = [
        (alpha.shape, BF16),
        (alpha.shape, BF16),
        ((2, frows, fcols), F32),
        ((levels * GROUP // 2, 2 * cols, 2 * cols), BF16),
        ((levels, 2, cols, cols), BF16),
        ((levels, 2, deep, wide_k), BF16),
        ((members, levels, 2 * HB, cols), F32),
        ((steps, levels, e_rows, cols), F32),
        packed,
        packed,
        fine_edge,
        fine_edge,
        fine_side,
        fine_side,
        fine_side,
        fine_side,
        ((2, f_tall, f_wide), F32),
        (lat_i.shape, jnp.int32),
        (lat_i.shape, jnp.int32),
        (lat_w.shape, F32),
        (lat_w.shape, F32),
        (lon_i.shape, jnp.int32),
        (lon_i.shape, jnp.int32),
        (lon_w.shape, F32),
        (lon_w.shape, F32),
        ((2, 2 * cols, f_wide), BF16),
        ((2, f_tall, t_rows), BF16),
        ((2, e_rows, f_tall), BF16),
        ((2, f_wide, 2 * cols), BF16),
        ((levels, e_rows, 2 * cols), F32),
        ((count - 1, e_rows, 2 * cols), F32),
        ((count, STRIP, 2 * cols), F32),
        ((count, STRIP, 2 * cols), F32),
    ] + [((STRIP, cols), F32)] * 4
    vmem = pl.BlockSpec(memory_space=pltpu.VMEM)
    anywhere = pl.BlockSpec(memory_space=pl.ANY)
    return pl.pallas_call(
        core_kernel,
        in_specs=[pl.BlockSpec(memory_space=pltpu.SMEM)] + [vmem] * 4 + [anywhere] * 4,
        out_specs=[vmem] * len(outs),
        out_shape=[jax.ShapeDtypeStruct(shape, kind) for shape, kind in outs],
        scratch_shapes=[pltpu.VMEM(shape, kind) for shape, kind in scratch]
        + [
            pltpu.SemaphoreType.DMA((96,)),
            pltpu.SemaphoreType.DMA((96,)),
            pltpu.SemaphoreType.DMA((2 + 2 * steps,)),
        ],
        compiler_params=pltpu.CompilerParams(
            collective_id=0, has_side_effects=True, vmem_limit_bytes=VMEM_LIMIT
        ),
        cost_estimate=cost(2**30, 2**24),
    )(widths, lat_i, lat_w, lon_i, lon_w, alpha, perts, innov, weight)


def band(high, low, taps):
    half = taps.shape[0]
    deep = half + 2 * HB
    out = []
    for first in range(0, high.shape[0] - 2 * HB, half):
        h, lo = high[first : first + deep], low[first : first + deep]
        out.append(dot(taps, rows_of(h, h, lo)))
    return rows_of(*out)


def adjoint_kernel(
    alpha, perts, north, south, west, east, residual, lon, lat, fine, out, fine_out, held, sems
):
    rows, cols = alpha.shape[2:]
    slots = GROUP * HB
    g, l = pl.program_id(0), pl.program_id(1)
    take = pltpu.make_async_copy(fine, held, sems.at[0])
    give = pltpu.make_async_copy(held, fine_out, sems.at[1])

    @pl.when((g == 0) & (l == 0))
    def _():
        take.start()

    @pl.when((g == 1) & (l == 0))
    def _():
        take.wait()
        give.start()

    @pl.when((g == pl.num_programs(0) - 1) & (l == pl.num_programs(1) - 1))
    def _():
        give.wait()

    res = residual[l]
    wide = iota((rows + 2 * HB, cols), 1)
    side = jnp.where(wide // slots == l, west[0].astype(F32), east[0].astype(F32))
    side = natural(side, rows) * res[:, cols:]
    taps = lat[l, :, : 3 * (rows // 2 + 2 * HB)]
    zero = jnp.zeros((cols, cols), BF16)

    def stack(high, low):
        return rows_of(lanes_of(high, low), lanes_of(high, zero))

    core, wing = stack(lon[l, 0], lon[l, 1]), stack(lon[l, 2], lon[l, 3])
    edge_h, edge_l = split(band(*split(side), taps))
    lane = iota((rows, cols), 1)
    for k in range(0, GROUP, 2):
        pairs = []
        for m in (k, k + 1):
            tall = rows_of(north[m, 0].astype(F32), perts[m, 0].astype(F32), south[m, 0].astype(F32))
            pairs.append(split(tall * res[:, :cols]))
        both = band(lanes_of(pairs[0][0], pairs[1][0]), lanes_of(pairs[0][1], pairs[1][1]), taps)
        for i, m in enumerate((k, k + 1)):
            mine = lane % slots // HB == m
            edges = lanes_of(
                jnp.where(mine, edge_h, jnp.zeros_like(edge_h)),
                jnp.where(mine, edge_l, jnp.zeros_like(edge_l)),
            )
            total = dot(lanes_of(*split(both[:, i * cols : (i + 1) * cols])), core) + dot(edges, wing)
            out[m, 0] = alpha[m, 0].astype(F32) + (total[:, :cols] + total[:, cols:])


def adjoint(alpha, perts, north, south, west, east, residual, lon, lat, fine):
    members, levels, rows, cols = alpha.shape
    block = pl.BlockSpec((GROUP, 1, rows, cols), lambda g, l: (g, l, 0, 0))
    strip = pl.BlockSpec((GROUP, 1, HB, cols), lambda g, l: (g, l, 0, 0))
    side = pl.BlockSpec((1, rows + 2 * HB, cols), lambda g, l: (g, 0, 0))

    def whole(x):
        return pl.BlockSpec(x.shape, lambda g, l: (0,) * x.ndim)

    return pl.pallas_call(
        adjoint_kernel,
        grid=(members // GROUP, levels),
        in_specs=[block, block, strip, strip, side, side, whole(residual), whole(lon), whole(lat)]
        + [pl.BlockSpec(memory_space=pl.ANY)],
        out_specs=[block, pl.BlockSpec(memory_space=pl.ANY)],
        out_shape=[
            jax.ShapeDtypeStruct(alpha.shape, F32),
            jax.ShapeDtypeStruct(fine.shape, F32),
        ],
        scratch_shapes=[pltpu.VMEM(fine.shape, F32), pltpu.SemaphoreType.DMA((2,))],
        cost_estimate=cost(members * levels * 2**25, alpha.size * 8),
    )(alpha, perts, north, south, west, east, residual, lon, lat, fine)


def body(
    alpha_fields,
    member_perts,
    band_widths,
    lat_index,
    lat_weight,
    lon_index,
    lon_weight,
    innovation,
    obs_weight,
):
    tables = [x.reshape(1, -1) for x in (lat_index, lat_weight, lon_index, lon_weight)]
    increment, residual, *halos = core_step(
        band_widths, *tables, alpha_fields, member_perts, innovation, obs_weight
    )
    north, south, west, east, lon, lat = halos
    gradient, increment = adjoint(
        alpha_fields, member_perts, north, south, west, east, residual, lon, lat, increment
    )
    return (increment, gradient)


def solution(mesh):
    placed = (
        P("ma", None, "gy", "gx"),
        P("ma", None, "gy", "gx"),
        P(),
        P("gy"),
        P("gy"),
        P("gx"),
        P("gx"),
        P(None, "gy", "gx"),
        P(None, "gy", "gx"),
    )
    return jax.shard_map(
        body,
        mesh=mesh,
        in_specs=placed,
        out_specs=(P(None, "gy", "gx"), P("ma", None, "gy", "gx")),
        check_vma=False,
    )
```

```python
import math

import jax
import jax.numpy as jnp
from jax import lax
from jax.experimental import pallas as pl
from jax.experimental.pallas import tpu as pltpu
from jax.sharding import PartitionSpec as P

HB = 8
GROUP = 8
FR = 24
FC = 20
FOLD = 3
CR = 16
STRIP = 24
REACH = HB + 10
MESH = pl.DeviceIdType.MESH
VMEM_BYTES = 67043328
VMEM_SLACK = 2**17
BACK_LIMIT = 32 * 2**20
F32 = jnp.float32
BF16 = jnp.bfloat16


def iota(shape, dim):
    return lax.broadcasted_iota(jnp.int32, shape, dim)


def dot(a, b):
    return jnp.dot(a, b, preferred_element_type=F32)


def split(value):
    high = value.astype(BF16)
    return high, (value - high.astype(F32)).astype(BF16)


def dot3(a, b):
    return dot(a[0], b[0]) + dot(a[1], b[0]) + dot(a[0], b[1])


def rows_of(*parts):
    return jnp.concatenate(parts, axis=0)


def lanes_of(*parts):
    return jnp.concatenate(parts, axis=1)


def natural(x, rows):
    return rows_of(x[rows : rows + HB], x[:rows], x[rows + HB :])


def place(order, size, width):
    return jnp.where(order < size, order, jnp.where(order < size + width, order - size - width, order - width))


def tap_value(distance, spread, scale):
    d = distance.astype(F32)
    value = jnp.exp(-(d * d) / (2.0 * spread * spread)) * scale
    return jnp.where(jnp.abs(distance) <= HB, value, 0.0)


def tap_scale(spread):
    lane = iota((8, 128), 1)
    d = (lane - HB).astype(F32)
    shape = jnp.where(lane <= 2 * HB, jnp.exp(-(d * d) / (2.0 * spread * spread)), 0.0)
    return (1.0 / jnp.sqrt(jnp.sum(shape * shape, axis=1, keepdims=True)))[:1]


def lat_taps(spread, scale, height, deep, offset, width):
    i, c = iota((height, width), 0), iota((height, width), 1)
    r = jnp.where(c >= 2 * deep, c - 2 * deep, jnp.where(c >= deep, c - deep, c))
    value = tap_value(r - i + offset, spread, scale)
    high = value.astype(BF16).astype(F32)
    return jnp.where((c >= deep) & (c < 2 * deep), value - high, high).astype(BF16)


def side_cell(lane, level, cols):
    west = lane // (GROUP * HB) == level
    return jnp.where(west, lane % HB - HB, cols + lane % HB)


def weigh(cell, index, weight):
    cell = cell.astype(F32)
    return jnp.where(cell == index, 1.0 - weight, 0.0) + jnp.where(cell == index + 1.0, weight, 0.0)


class Link:
    def __init__(self, axis, step, src, dst, send, recv, slot, also=None):
        me, count = lax.axis_index(axis), lax.axis_size(axis)
        target = me + step
        self.sends = self.gets = None
        if axis == "gx":
            target = lax.rem(target + count, count)
        elif axis == "gy":
            self.sends = (target >= 0) & (target < count)
            self.gets = (me - step >= 0) & (me - step < count)
        self.dst = dst
        device = {axis: target, **(also or {})}
        self.copy = pltpu.make_async_remote_copy(
            src_ref=src,
            dst_ref=dst,
            send_sem=send.at[slot],
            recv_sem=recv.at[slot],
            device_id=device,
            device_id_type=MESH,
        )

    def start(self):
        if self.sends is None:
            self.copy.start()
        else:
            pl.when(self.sends)(self.copy.start)

    def arrive(self):
        if self.gets is None:
            self.copy.wait_recv()
        else:
            pl.when(self.gets)(self.copy.wait_recv)

            @pl.when(jnp.logical_not(self.gets))
            def _():
                self.dst[...] = jnp.zeros_like(self.dst)

    def sent(self):
        if self.sends is None:
            self.copy.wait_send()
        else:
            pl.when(self.sends)(self.copy.wait_send)


def greet():
    barrier = pltpu.get_barrier_semaphore()
    gx, gxn = lax.axis_index("gx"), lax.axis_size("gx")
    gy, gyn = lax.axis_index("gy"), lax.axis_size("gy")
    ma, count = lax.axis_index("ma"), lax.axis_size("ma")
    for step in (1, gxn - 1):
        pl.semaphore_signal(
            barrier, inc=1, device_id={"gx": lax.rem(gx + step, gxn)}, device_id_type=MESH
        )
    for s in range(1, count):
        pl.semaphore_signal(
            barrier, inc=1, device_id={"ma": lax.rem(ma + s, count)}, device_id_type=MESH
        )
    for step, there in ((-1, gy > 0), (1, gy < gyn - 1)):

        @pl.when(there)
        def _(step=step):
            for s in range(count):
                pl.semaphore_signal(
                    barrier,
                    inc=1,
                    device_id={"gy": gy + step, "ma": lax.rem(ma + s, count)},
                    device_id_type=MESH,
                )
            for side in (1, gxn - 1):
                pl.semaphore_signal(
                    barrier,
                    inc=1,
                    device_id={"gx": lax.rem(gx + side, gxn), "gy": gy + step},
                    device_id_type=MESH,
                )

    below, above = jnp.minimum(gy, 1), jnp.minimum(gyn - 1 - gy, 1)
    return lambda: pl.semaphore_wait(barrier, 2 + (count - 1) + (below + above) * (count + 2))


def core_kernel(
    widths, lat_i, lat_w, lon_i, lon_w, alpha, perts, innov, weight,
    increment, residual, a_tile, p_tile, p_north, p_south, p_west, p_east, lon_taps, lat_back,
    fine_tile, pick, edge_taps, lat_fore, v_strip, v_side, p_right, p_left,
    f_low, f_high, f_right, f_left, f_west, f_east, fine_wide,
    lat_i_low, lat_i_high, lat_w_low, lat_w_high, lon_i_west, lon_i_east, lon_w_west, lon_w_east,
    up_lon, up_lat, down_lat, down_lon, ext, other, low, high, to_east, to_west, from_west, from_east,
    send, recv, local,
):
    members, levels, rows, cols = alpha.shape
    steps, half, slots = members // GROUP, rows // 2, GROUP * HB
    frows, fcols = innov.shape[1:]
    ma, count = lax.axis_index("ma"), lax.axis_size("ma")
    gx, gxn = lax.axis_index("gx"), lax.axis_size("gx")
    met = greet()
    f_loads = [
        pltpu.make_async_copy(src.at[ma], fine_tile.at[i], local.at[i])
        for i, src in enumerate((innov, weight))
    ]

    def group_load(src, dst, g, first):
        span = pl.ds(g * GROUP, GROUP)
        return pltpu.make_async_copy(src.at[span], dst.at[span], local.at[first + g])

    p_loads = [group_load(perts, p_tile, g, 2) for g in range(steps)]
    for load in p_loads + f_loads:
        load.start()
    counter = iter(range(96))
    pending = []

    def link(axis, step, src, dst, also=None):
        one = Link(axis, step, src, dst, send, recv, next(counter), also)
        pending.append(one)
        return one

    r, c = iota((cols, 2 * cols), 0), iota((cols, 2 * cols), 1)
    base = jnp.where(
        ((c < cols) & (r - (cols - HB) == c % HB)) | ((c >= cols) & (r == c % HB)), 1.0, 0.0
    )
    turned = (c % cols) // slots
    slot = jnp.where(c < cols, turned, 1 - turned) * GROUP + c % slots // HB
    for l in range(levels):
        for k in range(GROUP):
            at = slice(k % 2 * cols, (k % 2 + 1) * cols)
            n = l * GROUP + k
            pick[n // 2, at] = jnp.where(slot == n, base, 0.0).astype(BF16)
    f_rows = [
        link("gy", 1, innov.at[ma, pl.ds(frows - FR, FR)], f_low.at[0]),
        link("gy", -1, innov.at[ma, pl.ds(0, FR)], f_high.at[0]),
        link("gy", 1, weight.at[ma, pl.ds(frows - FR, FR)], f_low.at[1]),
        link("gy", -1, weight.at[ma, pl.ds(0, FR)], f_high.at[1]),
    ]
    p_rows = [
        link("gy", 1, perts.at[:, :, pl.ds(rows - HB, HB), :], p_north),
        link("gy", -1, perts.at[:, :, pl.ds(0, HB), :], p_south),
    ]
    small = [
        link("gy", 1, lat_i, lat_i_low),
        link("gy", -1, lat_i, lat_i_high),
        link("gy", 1, lat_w, lat_w_low),
        link("gy", -1, lat_w, lat_w_high),
        link("gx", 1, lon_i, lon_i_west),
        link("gx", -1, lon_i, lon_i_east),
        link("gx", 1, lon_w, lon_w_west),
        link("gx", -1, lon_w, lon_w_east),
    ]
    def tilted(src, dst, side, top, bottom, first):
        pairs = []
        for step, at, to in ((1, bottom, first), (-1, top, first + HB)):
            span, there = pl.ds(at, HB), pl.ds(to, HB)
            index = (slice(None),) * (src.ndim - 2)
            pairs.append(
                link(
                    "gy",
                    step,
                    src.at[(*index, span)],
                    dst.at[(*index, there)],
                    {"gx": lax.rem(gx + side, gxn)},
                )
            )
        return pairs

    def packed(piece):
        total = None
        for l in range(levels):
            for k in range(0, GROUP, 2):
                n = (l * GROUP + k) // 2
                part = dot(lanes_of(piece(l, k), piece(l, k + 1)), pick[n])
                total = part if total is None else total + part
        return total.astype(BF16)

    a_loads = [group_load(alpha, a_tile, g, 2 + steps) for g in range(steps)]
    p_arrive = []
    for g in range(steps):
        p_loads[g].wait()
        a_loads[g].start()
        both = packed(lambda l, k: p_tile[g * GROUP + k, l])
        p_right[g] = both[:, :cols]
        p_left[g] = both[:, cols:]
        if g == 0:
            met()
            for one in small + p_rows:
                one.start()
        span = pl.ds(0, rows)
        pair = [
            link("gx", 1, p_right.at[g], p_west.at[g, span]),
            link("gx", -1, p_left.at[g], p_east.at[g, span]),
        ]
        for one in pair:
            one.start()
        p_arrive += pair
    corners = tilted(p_right, p_west, 1, 0, rows - HB, rows)
    corners += tilted(p_left, p_east, gxn - 1, 0, rows - HB, rows)
    for one in corners + f_rows:
        one.start()
    p_arrive += corners

    f_main = f_west.shape[0] - 2 * HB

    def f_fold(first, count, start):
        deep = -(-count // (FOLD * HB)) * HB
        parts = []
        for b in range(FOLD):
            stop = min(first + (b + 1) * deep, first + count)
            for i in range(2):
                part = fine_tile[i, first + b * deep : stop, start : start + FC]
                short = deep - part.shape[0]
                parts.append(rows_of(part, jnp.zeros((short, FC), F32)) if short else part)
        return lanes_of(*parts, jnp.zeros((deep, cols - 2 * FOLD * FC), F32))

    for load in f_loads:
        load.wait()
    f_arrive = []
    for step, side, src, dst, start in (
        (1, 1, f_right, f_west, fcols - FC),
        (-1, gxn - 1, f_left, f_east, 0),
    ):
        src[:f_main] = f_fold(0, frows, start)
        src[f_main : f_main + HB] = f_fold(0, FR, start)
        src[f_main + HB :] = f_fold(frows - FR, FR, start)
        span = pl.ds(0, f_main)
        f_arrive.append(link("gx", step, src.at[span], dst.at[span]))
        f_arrive += tilted(src, dst, side, f_main, f_main + HB, f_main)
    for one in f_arrive:
        one.start()

    lane = iota((cols, cols), 1)
    deep = half + 2 * HB
    wide_k = lat_fore.shape[3]
    for l in range(levels):
        spread = widths[l].astype(F32)
        scale = tap_scale(spread)
        cell, at = iota((cols, cols), 0), lane
        lon_taps[l, 0], lon_taps[l, 1] = split(tap_value(cell - at, spread, scale))
        shift = at % (2 * HB)
        gap = side_cell(cell, l, cols) - jnp.where(shift < HB, cols - HB + shift, shift - HB)
        own = cell % slots // HB == at // (2 * HB)
        lon_taps[l, 2], lon_taps[l, 3] = split(jnp.where(own, tap_value(gap, spread, scale), 0.0))
        edge_taps[l, 0], edge_taps[l, 1] = split(tap_value(side_cell(at, l, cols) - cell, spread, scale))
        lat_back[l] = lat_taps(spread, scale, half, deep, -HB, wide_k)
        lat_fore[l, 0] = lat_taps(spread, scale, deep, deep, HB, wide_k)
        lat_fore[l, 1] = lat_taps(spread, scale, deep, deep, -2 * HB, wide_k)

    def tall(u, l):
        h, lo = split(u)
        out = []
        for b in range(2):
            at = slice(b * (rows - deep), b * (rows - deep) + deep)
            stack = rows_of(h[at], h[at], lo[at])
            out.append(dot(lat_fore[l, b, :, : 3 * deep], stack)[: half + HB])
        return out

    for l in range(levels):
        ext[l, HB : HB + rows, :cols] = jnp.zeros((rows, cols), F32)

    @pl.loop(0, steps)
    def _(g):
        group_load(alpha, a_tile, g, 2 + steps).wait()
        for l in range(levels):
            taps = rows_of(
                lanes_of(lon_taps[l, 0], edge_taps[l, 0]), lanes_of(lon_taps[l, 1], edge_taps[l, 1])
            )
            side = total = None
            for k in range(0, GROUP, 2):
                cores = []
                for m in (k, k + 1):
                    a = a_tile[g * GROUP + m, l]
                    u = dot(lanes_of(a, a), taps)
                    cores.append(u[:, :cols])
                    mine = lane % slots // HB == m
                    side = u[:, cols:] if side is None else jnp.where(mine, u[:, cols:], side)
                top, bottom = tall(lanes_of(*cores), l)
                for i, m in enumerate((k, k + 1)):
                    at = slice(i * cols, (i + 1) * cols)
                    v = rows_of(top[HB:, at], bottom[:half, at])
                    part = p_tile[g * GROUP + m, l].astype(F32) * v
                    total = part if total is None else total + part
                    v_strip[g * GROUP + m, l] = rows_of(top[:HB, at], bottom[half:, at])
            ext[l, HB : HB + rows, :cols] += total
            v_side[g, l] = rows_of(*tall(side, l))

    for one in p_rows:
        one.arrive()

    for one in f_rows:
        one.arrive()
    for one in small:
        one.arrive()
    lat_at = lanes_of(lat_i[...], lat_i_low[:, frows - FR :], lat_i_high[:, :FR]).astype(F32)
    lat_by = lanes_of(lat_w[...], lat_w_low[:, frows - FR :], lat_w_high[:, :FR])
    lat_at = lat_at - (lax.axis_index("gy") * rows).astype(F32)
    lon_at = lanes_of(lon_i[...], lon_i_west[:, fcols - FC :], lon_i_east[:, :FC]).astype(F32)
    lon_by = lanes_of(lon_w[...], lon_w_west[:, fcols - FC :], lon_w_east[:, :FC])
    lon_total = float(cols * lax.axis_size("gx"))
    lon_at = lon_at - (lax.axis_index("gx") * cols).astype(F32)
    lon_at = jnp.where(
        lon_at < -64.0, lon_at + lon_total, jnp.where(lon_at >= lon_total - 64.0, lon_at - lon_total, lon_at)
    )
    f_tall, f_wide = frows + 2 * FR, fcols + 2 * FC

    def upright(at, by):
        size = at.shape[1]
        space = jnp.zeros((1, -size % 128), F32)
        at, by = lanes_of(at, space), lanes_of(by, space)
        shape = (8, at.shape[1])
        both = jnp.where(iota(shape, 0) == 0, jnp.broadcast_to(at, shape), jnp.broadcast_to(by, shape))
        both = both.T[:size]
        return both[:, 0:1], both[:, 1:2]

    lat_at_up, lat_by_up = upright(lat_at, lat_by)
    lon_at_up, lon_by_up = upright(lon_at, lon_by)
    t_rows, e_rows = rows + 2 * CR, rows + 2 * HB
    up_lat[0], up_lat[1] = split(weigh(iota((f_tall, t_rows), 1) - CR, lat_at_up, lat_by_up))
    down_lat[0], down_lat[1] = split(weigh(iota((e_rows, f_tall), 0) - HB, lat_at, lat_by))
    order = iota((2 * cols, f_wide), 0)
    w = order - cols
    wing = jnp.where(
        w < REACH,
        w - (REACH - HB),
        jnp.where(
            (w >= slots - HB) & (w < slots),
            w - slots,
            jnp.where(
                (w >= slots) & (w < slots + REACH),
                w - slots + cols - HB,
                jnp.where(w >= cols - HB, w + HB, -1000),
            ),
        ),
    )
    up_lon[0], up_lon[1] = split(weigh(jnp.where(w < 0, order, wing), lon_at, lon_by))
    order = iota((f_wide, 2 * cols), 1)
    cell = jnp.where(order < cols, order, side_cell(order - cols, ma, cols))
    down_lon[0], down_lon[1] = split(weigh(cell, lon_at_up, lon_by_up))

    for l in range(levels):

        def strips(g, sums):
            north, south = sums
            for k in range(GROUP):
                m = g * GROUP + k
                north = north + p_north[m, l].astype(F32) * v_strip[m, l, :HB]
                south = south + p_south[m, l].astype(F32) * v_strip[m, l, HB:]
            return north, south

        zero = jnp.zeros((HB, cols), F32)
        north, south = lax.fori_loop(0, steps, strips, (zero, zero))
        ext[l, :HB, :cols] = north
        ext[l, HB + rows :, :cols] = south

    for one in f_arrive:
        one.arrive()
    for i in range(2):

        def wing_of(part):
            def opened(first, last):
                lanes = range(FC * i, 2 * FOLD * FC, 2 * FC)
                return [part[first:last, x : x + FC] for x in lanes]

            low, high = f_main, f_main + HB
            return rows_of(
                rows_of(*opened(0, low))[:frows], *opened(low, high), *opened(high, high + HB)
            )

        fine_wide[i] = lanes_of(
            rows_of(fine_tile[i], f_low[i], f_high[i]), wing_of(f_west), wing_of(f_east)
        )

    for one in p_arrive:
        one.arrive()
    tall_lane = iota((e_rows, cols), 1)
    for l in range(levels):
        total = None
        for g in range(steps):
            side = jnp.where(
                tall_lane // slots == l, p_west[g].astype(F32), p_east[g].astype(F32)
            )
            part = natural(side, rows) * v_side[g, l]
            total = part if total is None else total + part
        ext[l, :, cols:] = total if l == 0 else pltpu.roll(total, slots, 1)

    swaps, lows, highs = [], [], []
    for s in range(count):
        peer = lax.rem(ma + s, count)
        if s:
            swaps.append(link("ma", peer - ma, ext.at[peer], other.at[s - 1]))
        lows.append(link("gy", 1, ext.at[peer, pl.ds(e_rows - STRIP, STRIP)], low.at[s], {"ma": peer}))
        highs.append(link("gy", -1, ext.at[peer, pl.ds(0, STRIP)], high.at[s], {"ma": peer}))
    for one in lows + highs + swaps:
        one.start()
    for one in swaps + lows + highs:
        one.arrive()
    mine = ext[ma]
    for s in range(count - 1):
        mine = mine + other[s]
    above, below = low[0], high[0]
    for s in range(1, count):
        above, below = above + low[s], below + high[s]
    lap = CR - HB
    edge = STRIP - lap
    mine = rows_of(
        above[:lap],
        mine[:edge] + above[lap:],
        mine[edge : e_rows - edge],
        mine[e_rows - edge :] + below[:edge],
        below[edge:],
    )
    core, side = mine[:, :cols], mine[:, cols:]
    for shift in (HB, 2 * HB, 4 * HB):
        side = side + pltpu.roll(side, shift, 1)

    blocks = (t_rows + STRIP - 1) // STRIP
    t_lane = iota((t_rows, cols), 1)
    thin = iota((STRIP, cols), 1)

    def fold(x, first):
        if blocks * STRIP > t_rows:
            x = rows_of(x, jnp.zeros((blocks * STRIP - t_rows, cols), F32))
        total = None
        for b in range(blocks):
            part = pltpu.roll(x[b * STRIP : (b + 1) * STRIP], (b * REACH - first) % cols, 1)
            total = part if total is None else jnp.where(thin >= b * REACH, part, total)
        return total

    def unfold(x, first):
        parts = [pltpu.roll(x, (first - b * REACH) % cols, 1) for b in range(blocks)]
        return rows_of(*parts)[:t_rows]

    eastward = jnp.where(t_lane >= cols - HB, side, pltpu.roll(core, cols - HB, 1))
    westward = jnp.where(t_lane < slots, side, pltpu.roll(core, slots, 1))
    to_east[...] = fold(eastward, cols - REACH)
    to_west[...] = fold(westward, slots - HB)
    sides = [
        link("gx", 1, to_east, from_west),
        link("gx", -1, to_west, from_east),
    ]
    for one in sides:
        one.start()
    for one in sides:
        one.arrive()
    wings = jnp.where(
        t_lane < REACH,
        unfold(from_west[...], 0),
        jnp.where((t_lane >= slots) & (t_lane < slots + REACH), unfold(from_east[...], slots), side),
    )
    across = dot3(split(lanes_of(core, wings)), (up_lon[0], up_lon[1]))
    fine = dot3((up_lat[0], up_lat[1]), split(across))
    increment[ma] = fine[:frows, :fcols]
    ends = []

    def share(whole):
        for s in range(1, count):
            peer = lax.rem(ma + s, count)
            ends.append(link("ma", peer - ma, whole.at[ma], whole.at[ma]))
            ends[-1].start()

    share(increment)
    misfit = fine_wide[1] * (fine - fine_wide[0])
    across = dot3((down_lat[0], down_lat[1]), split(misfit))
    residual[ma] = dot3(split(across), (down_lon[0], down_lon[1]))
    share(residual)
    for one in ends:
        one.arrive()
    for one in pending:
        one.sent()


def cost(flops, nbytes):
    return pl.CostEstimate(flops=flops, bytes_accessed=nbytes, transcendentals=0)


def core_step(widths, lat_i, lat_w, lon_i, lon_w, alpha, perts, innov, weight):
    members, levels, rows, cols = alpha.shape
    steps = members // GROUP
    frows, fcols = innov.shape[1:]
    count = lax.axis_size("ma")
    assert levels == 2 and count == levels
    half = rows // 2
    deep = half + 2 * HB
    wide_k = -(-3 * deep // 128) * 128
    e_rows, t_rows = rows + 2 * HB, rows + 2 * CR
    f_tall, f_wide = frows + 2 * FR, fcols + 2 * FC
    strip = ((members, levels, HB, cols), BF16)
    side = ((steps, e_rows, cols), BF16)
    outs = [
        (innov.shape, F32),
        ((levels, e_rows, 2 * cols), F32),
        (alpha.shape, BF16),
        (alpha.shape, BF16),
        strip,
        strip,
        side,
        side,
        ((levels, 4, cols, cols), BF16),
        ((levels, half, wide_k), BF16),
    ]
    kept = sum(math.prod(shape) * jnp.dtype(kind).itemsize for shape, kind in outs)
    fine_edge = ((2, FR, fcols), F32)
    fine_side = ((-(-frows // (FOLD * HB)) * HB + 2 * HB, cols), F32)
    packed = ((steps, rows, cols), BF16)
    scratch = [
        ((2, frows, fcols), F32),
        ((levels * GROUP // 2, 2 * cols, 2 * cols), BF16),
        ((levels, 2, cols, cols), BF16),
        ((levels, 2, deep, wide_k), BF16),
        ((members, levels, 2 * HB, cols), F32),
        ((steps, levels, e_rows, cols), F32),
        packed,
        packed,
        fine_edge,
        fine_edge,
        fine_side,
        fine_side,
        fine_side,
        fine_side,
        ((2, f_tall, f_wide), F32),
        (lat_i.shape, jnp.int32),
        (lat_i.shape, jnp.int32),
        (lat_w.shape, F32),
        (lat_w.shape, F32),
        (lon_i.shape, jnp.int32),
        (lon_i.shape, jnp.int32),
        (lon_w.shape, F32),
        (lon_w.shape, F32),
        ((2, 2 * cols, f_wide), BF16),
        ((2, f_tall, t_rows), BF16),
        ((2, e_rows, f_tall), BF16),
        ((2, f_wide, 2 * cols), BF16),
        ((levels, e_rows, 2 * cols), F32),
        ((count - 1, e_rows, 2 * cols), F32),
        ((count, STRIP, 2 * cols), F32),
        ((count, STRIP, 2 * cols), F32),
    ] + [((STRIP, cols), F32)] * 4
    vmem = pl.BlockSpec(memory_space=pltpu.VMEM)
    anywhere = pl.BlockSpec(memory_space=pltpu.HBM)
    return pl.pallas_call(
        core_kernel,
        in_specs=[pl.BlockSpec(memory_space=pltpu.SMEM)] + [vmem] * 4 + [anywhere] * 4,
        out_specs=[vmem] * len(outs),
        out_shape=[pltpu.VMEM(shape, kind) for shape, kind in outs],
        scratch_shapes=[pltpu.VMEM(shape, kind) for shape, kind in scratch]
        + [
            pltpu.SemaphoreType.DMA((96,)),
            pltpu.SemaphoreType.DMA((96,)),
            pltpu.SemaphoreType.DMA((2 + 2 * steps,)),
        ],
        compiler_params=pltpu.CompilerParams(
            collective_id=0, has_side_effects=True, vmem_limit_bytes=VMEM_BYTES - VMEM_SLACK - kept
        ),
        cost_estimate=cost(2**30, 2**24),
    )(widths, lat_i, lat_w, lon_i, lon_w, alpha, perts, innov, weight)


def band(high, low, taps):
    half = taps.shape[0]
    deep = half + 2 * HB
    out = []
    for first in range(0, high.shape[0] - 2 * HB, half):
        h, lo = high[first : first + deep], low[first : first + deep]
        out.append(dot(taps, rows_of(h, h, lo)))
    return rows_of(*out)


def adjoint_kernel(
    alpha, perts, north, south, west, east, residual, lon, lat, fine, out, fine_out, sem
):
    rows, cols = alpha.shape[2:]
    slots = GROUP * HB
    g = pl.program_id(0)
    give = pltpu.make_async_copy(fine, fine_out, sem.at[0])

    @pl.when(g == 0)
    def _():
        give.start()

    @pl.when(g == pl.num_programs(0) - 1)
    def _():
        give.wait()

    zero = jnp.zeros((cols, cols), BF16)

    def stack(high, low):
        return rows_of(lanes_of(high, low), lanes_of(high, zero))

    def halves(x):
        return x[:, :cols] + x[:, cols:]

    lane = iota((rows, cols), 1)
    inner = (lane >= HB) & (lane < cols - HB)
    wide = iota((rows + 2 * HB, cols), 1)
    for l in range(alpha.shape[1]):
        res = residual[l]
        taps = lat[l, :, : 3 * (rows // 2 + 2 * HB)]
        side = jnp.where(wide // slots == l, west[g].astype(F32), east[g].astype(F32))
        edge = band(*split(natural(side, rows) * res[:, cols:]), taps)
        edge = halves(dot(lanes_of(*split(edge)), stack(lon[l, 2], lon[l, 3])))
        cores = []
        for k in range(0, GROUP, 2):
            pairs = []
            for m in (k, k + 1):
                n = g * GROUP + m
                tall = rows_of(
                    north[n, l].astype(F32), perts[n, l].astype(F32), south[n, l].astype(F32)
                )
                pairs.append(split(tall * res[:, :cols]))
            both = band(lanes_of(pairs[0][0], pairs[1][0]), lanes_of(pairs[0][1], pairs[1][1]), taps)
            for i in range(2):
                cores.append(lanes_of(*split(both[:, i * cols : (i + 1) * cols])))
        total = dot(rows_of(*cores), stack(lon[l, 0], lon[l, 1]))
        for m in range(GROUP):
            turned = pltpu.roll(edge, (cols - HB - 2 * HB * m) % cols, 1)
            value = halves(total[m * rows : (m + 1) * rows]) + jnp.where(inner, 0.0, turned)
            out[m, l] = alpha[g * GROUP + m, l].astype(F32) + value


def adjoint(alpha, perts, north, south, west, east, residual, lon, lat, fine):
    members, levels, rows, cols = alpha.shape
    return pl.pallas_call(
        adjoint_kernel,
        grid=(members // GROUP,),
        in_specs=[pl.BlockSpec(memory_space=pltpu.VMEM)] * 10,
        out_specs=[
            pl.BlockSpec((GROUP, levels, rows, cols), lambda g: (g, 0, 0, 0)),
            pl.BlockSpec(memory_space=pltpu.HBM),
        ],
        out_shape=[
            jax.ShapeDtypeStruct(alpha.shape, F32),
            jax.ShapeDtypeStruct(fine.shape, F32),
        ],
        scratch_shapes=[pltpu.SemaphoreType.DMA((1,))],
        compiler_params=pltpu.CompilerParams(vmem_limit_bytes=BACK_LIMIT),
        cost_estimate=cost(members * levels * 2**25, alpha.size * 8),
    )(alpha, perts, north, south, west, east, residual, lon, lat, fine)


def body(
    alpha_fields,
    member_perts,
    band_widths,
    lat_index,
    lat_weight,
    lon_index,
    lon_weight,
    innovation,
    obs_weight,
):
    tables = [x.reshape(1, -1) for x in (lat_index, lat_weight, lon_index, lon_weight)]
    increment, residual, alpha, perts, *rest = core_step(
        band_widths, *tables, alpha_fields, member_perts, innovation, obs_weight
    )
    north, south, west, east, lon, lat = rest
    gradient, increment = adjoint(
        alpha, perts, north, south, west, east, residual, lon, lat, increment
    )
    return (increment, gradient)


def solution(mesh):
    placed = (
        P("ma", None, "gy", "gx"),
        P("ma", None, "gy", "gx"),
        P(),
        P("gy"),
        P("gy"),
        P("gx"),
        P("gx"),
        P(None, "gy", "gx"),
        P(None, "gy", "gx"),
    )
    return jax.shard_map(
        body,
        mesh=mesh,
        in_specs=placed,
        out_specs=(P(None, "gy", "gx"), P("ma", None, "gy", "gx")),
        check_vma=False,
    )
```

```python
import math

import jax
import jax.numpy as jnp
from jax import lax
from jax.experimental import pallas as pl
from jax.experimental.pallas import tpu as pltpu
from jax.sharding import PartitionSpec as P

HB = 8
GROUP = 8
FR = 24
FC = 20
FOLD = 3
CR = 16
STRIP = 24
REACH = HB + 10
MESH = pl.DeviceIdType.MESH
VMEM_BYTES = 67043328
VMEM_SLACK = 2**17
BACK_LIMIT = 32 * 2**20
F32 = jnp.float32
BF16 = jnp.bfloat16


def iota(shape, dim):
    return lax.broadcasted_iota(jnp.int32, shape, dim)


def dot(a, b):
    return jnp.dot(a, b, preferred_element_type=F32)


def split(value):
    high = value.astype(BF16)
    return high, (value - high.astype(F32)).astype(BF16)


def dot3(a, b):
    return dot(a[0], b[0]) + dot(a[1], b[0]) + dot(a[0], b[1])


def rows_of(*parts):
    return jnp.concatenate(parts, axis=0)


def lanes_of(*parts):
    return jnp.concatenate(parts, axis=1)


def natural(x, rows):
    return rows_of(x[rows : rows + HB], x[:rows], x[rows + HB :])


def place(order, size, width):
    return jnp.where(order < size, order, jnp.where(order < size + width, order - size - width, order - width))


def tap_value(distance, spread, scale):
    d = distance.astype(F32)
    value = jnp.exp(-(d * d) / (2.0 * spread * spread)) * scale
    return jnp.where(jnp.abs(distance) <= HB, value, 0.0)


def tap_scale(spread):
    lane = iota((8, 128), 1)
    d = (lane - HB).astype(F32)
    shape = jnp.where(lane <= 2 * HB, jnp.exp(-(d * d) / (2.0 * spread * spread)), 0.0)
    return (1.0 / jnp.sqrt(jnp.sum(shape * shape, axis=1, keepdims=True)))[:1]


def lat_taps(spread, scale, height, deep, offset, width):
    i, c = iota((height, width), 0), iota((height, width), 1)
    r = jnp.where(c >= 2 * deep, c - 2 * deep, jnp.where(c >= deep, c - deep, c))
    value = tap_value(r - i + offset, spread, scale)
    high = value.astype(BF16).astype(F32)
    return jnp.where((c >= deep) & (c < 2 * deep), value - high, high).astype(BF16)


def side_cell(lane, level, cols):
    west = lane // (GROUP * HB) == level
    return jnp.where(west, lane % HB - HB, cols + lane % HB)


def weigh(cell, index, weight):
    cell = cell.astype(F32)
    return jnp.where(cell == index, 1.0 - weight, 0.0) + jnp.where(cell == index + 1.0, weight, 0.0)


class Link:
    def __init__(self, axis, step, src, dst, send, recv, slot, also=None):
        me, count = lax.axis_index(axis), lax.axis_size(axis)
        target = me + step
        self.sends = self.gets = None
        if axis == "gx":
            target = lax.rem(target + count, count)
        elif axis == "gy":
            self.sends = (target >= 0) & (target < count)
            self.gets = (me - step >= 0) & (me - step < count)
        self.dst = dst
        device = {axis: target, **(also or {})}
        self.copy = pltpu.make_async_remote_copy(
            src_ref=src,
            dst_ref=dst,
            send_sem=send.at[slot],
            recv_sem=recv.at[slot],
            device_id=device,
            device_id_type=MESH,
        )

    def start(self):
        if self.sends is None:
            self.copy.start()
        else:
            pl.when(self.sends)(self.copy.start)

    def arrive(self):
        if self.gets is None:
            self.copy.wait_recv()
        else:
            pl.when(self.gets)(self.copy.wait_recv)

            @pl.when(jnp.logical_not(self.gets))
            def _():
                self.dst[...] = jnp.zeros_like(self.dst)

    def sent(self):
        if self.sends is None:
            self.copy.wait_send()
        else:
            pl.when(self.sends)(self.copy.wait_send)


def greet():
    barrier = pltpu.get_barrier_semaphore()
    gx, gxn = lax.axis_index("gx"), lax.axis_size("gx")
    gy, gyn = lax.axis_index("gy"), lax.axis_size("gy")
    ma, count = lax.axis_index("ma"), lax.axis_size("ma")

    def hail(device):
        pl.semaphore_signal(barrier, inc=1, device_id=device, device_id_type=MESH)

    for s in range(count):
        peer = lax.rem(ma + s, count)
        if s:
            hail({"ma": peer})
        sides = [lax.rem(gx + step, gxn) for step in (1, gxn - 1)]
        for side in sides:
            hail({"gx": side, "ma": peer})
        for step, there in ((-1, gy > 0), (1, gy < gyn - 1)):

            @pl.when(there)
            def _(step=step, peer=peer, sides=sides):
                for side in (gx, *sides):
                    hail({"gx": side, "gy": gy + step, "ma": peer})

    below, above = jnp.minimum(gy, 1), jnp.minimum(gyn - 1 - gy, 1)
    return lambda: pl.semaphore_wait(barrier, 3 * count - 1 + (below + above) * 3 * count)


def core_kernel(
    widths, lat_i, lat_w, lon_i, lon_w, alpha, perts, innov, weight,
    increment, residual, a_tile, p_tile, p_north, p_south, p_west, p_east, lon_taps, lat_back,
    fine_tile, pick, edge_taps, lat_fore, v_strip, v_side, p_right, p_left,
    f_low, f_high, f_right, f_left, f_west, f_east, fine_wide,
    lat_i_low, lat_i_high, lat_w_low, lat_w_high, lon_i_west, lon_i_east, lon_w_west, lon_w_east,
    up_lon, up_lat, down_lat, down_lon, ext, other, ends_in, flank, tip, flanks, tips,
    send, recv, local,
):
    members, levels, rows, cols = alpha.shape
    steps, half, slots = members // GROUP, rows // 2, GROUP * HB
    frows, fcols = innov.shape[1:]
    ma, count = lax.axis_index("ma"), lax.axis_size("ma")
    gx, gxn = lax.axis_index("gx"), lax.axis_size("gx")
    met = greet()
    f_loads = [
        pltpu.make_async_copy(src.at[ma], fine_tile.at[i], local.at[i])
        for i, src in enumerate((innov, weight))
    ]

    def group_load(src, dst, g, first):
        span = pl.ds(g * GROUP, GROUP)
        return pltpu.make_async_copy(src.at[span], dst.at[span], local.at[first + g])

    p_loads = [group_load(perts, p_tile, g, 2) for g in range(steps)]
    for load in p_loads + f_loads:
        load.start()
    counter = iter(range(96))
    pending = []

    def link(axis, step, src, dst, also=None):
        one = Link(axis, step, src, dst, send, recv, next(counter), also)
        pending.append(one)
        return one

    r, c = iota((cols, 2 * cols), 0), iota((cols, 2 * cols), 1)
    base = jnp.where(
        ((c < cols) & (r - (cols - HB) == c % HB)) | ((c >= cols) & (r == c % HB)), 1.0, 0.0
    )
    turned = (c % cols) // slots
    slot = jnp.where(c < cols, turned, 1 - turned) * GROUP + c % slots // HB
    for l in range(levels):
        for k in range(GROUP):
            at = slice(k % 2 * cols, (k % 2 + 1) * cols)
            n = l * GROUP + k
            pick[n // 2, at] = jnp.where(slot == n, base, 0.0).astype(BF16)
    f_rows = [
        link("gy", 1, innov.at[ma, pl.ds(frows - FR, FR)], f_low.at[0]),
        link("gy", -1, innov.at[ma, pl.ds(0, FR)], f_high.at[0]),
        link("gy", 1, weight.at[ma, pl.ds(frows - FR, FR)], f_low.at[1]),
        link("gy", -1, weight.at[ma, pl.ds(0, FR)], f_high.at[1]),
    ]
    p_rows = [
        link("gy", 1, perts.at[:, :, pl.ds(rows - HB, HB), :], p_north),
        link("gy", -1, perts.at[:, :, pl.ds(0, HB), :], p_south),
    ]
    small = [
        link("gy", 1, lat_i, lat_i_low),
        link("gy", -1, lat_i, lat_i_high),
        link("gy", 1, lat_w, lat_w_low),
        link("gy", -1, lat_w, lat_w_high),
        link("gx", 1, lon_i, lon_i_west),
        link("gx", -1, lon_i, lon_i_east),
        link("gx", 1, lon_w, lon_w_west),
        link("gx", -1, lon_w, lon_w_east),
    ]
    def tilted(src, dst, side, top, bottom, first):
        pairs = []
        for step, at, to in ((1, bottom, first), (-1, top, first + HB)):
            span, there = pl.ds(at, HB), pl.ds(to, HB)
            index = (slice(None),) * (src.ndim - 2)
            pairs.append(
                link(
                    "gy",
                    step,
                    src.at[(*index, span)],
                    dst.at[(*index, there)],
                    {"gx": lax.rem(gx + side, gxn)},
                )
            )
        return pairs

    def packed(piece):
        total = None
        for l in range(levels):
            for k in range(0, GROUP, 2):
                n = (l * GROUP + k) // 2
                part = dot(lanes_of(piece(l, k), piece(l, k + 1)), pick[n])
                total = part if total is None else total + part
        return total.astype(BF16)

    a_loads = [group_load(alpha, a_tile, g, 2 + steps) for g in range(steps)]
    p_arrive = []
    def p_sides(g):
        span = pl.ds(0, rows)
        pair = [
            link("gx", 1, p_right.at[g], p_west.at[g, span]),
            link("gx", -1, p_left.at[g], p_east.at[g, span]),
        ]
        for one in pair:
            one.start()
        p_arrive.append(pair)

    for g in range(steps):
        p_loads[g].wait()
        a_loads[g].start()
        both = packed(lambda l, k: p_tile[g * GROUP + k, l])
        p_right[g] = both[:, :cols]
        p_left[g] = both[:, cols:]
        if g == 0:
            met()
            for one in small + p_rows:
                one.start()
            p_sides(g)
    corners = tilted(p_right, p_west, 1, 0, rows - HB, rows)
    corners += tilted(p_left, p_east, gxn - 1, 0, rows - HB, rows)
    for one in corners:
        one.start()
    for g in range(1, steps):
        p_sides(g)
    for one in f_rows:
        one.start()

    f_main = f_west.shape[0] - 2 * HB

    def f_fold(first, count, start):
        deep = -(-count // (FOLD * HB)) * HB
        parts = []
        for b in range(FOLD):
            stop = min(first + (b + 1) * deep, first + count)
            for i in range(2):
                part = fine_tile[i, first + b * deep : stop, start : start + FC]
                short = deep - part.shape[0]
                parts.append(rows_of(part, jnp.zeros((short, FC), F32)) if short else part)
        return lanes_of(*parts, jnp.zeros((deep, cols - 2 * FOLD * FC), F32))

    for load in f_loads:
        load.wait()
    f_arrive = []
    for step, side, src, dst, start in (
        (1, 1, f_right, f_west, fcols - FC),
        (-1, gxn - 1, f_left, f_east, 0),
    ):
        src[:f_main] = f_fold(0, frows, start)
        src[f_main : f_main + HB] = f_fold(0, FR, start)
        src[f_main + HB :] = f_fold(frows - FR, FR, start)
        span = pl.ds(0, f_main)
        f_arrive.append(link("gx", step, src.at[span], dst.at[span]))
        f_arrive += tilted(src, dst, side, f_main, f_main + HB, f_main)
    for one in f_arrive:
        one.start()

    lane = iota((cols, cols), 1)
    deep = half + 2 * HB
    wide_k = lat_fore.shape[3]
    for l in range(levels):
        spread = widths[l].astype(F32)
        scale = tap_scale(spread)
        cell, at = iota((cols, cols), 0), lane
        lon_taps[l, 0], lon_taps[l, 1] = split(tap_value(cell - at, spread, scale))
        shift = at % (2 * HB)
        gap = side_cell(cell, l, cols) - jnp.where(shift < HB, cols - HB + shift, shift - HB)
        own = cell % slots // HB == at // (2 * HB)
        lon_taps[l, 2], lon_taps[l, 3] = split(jnp.where(own, tap_value(gap, spread, scale), 0.0))
        edge_taps[l, 0], edge_taps[l, 1] = split(tap_value(side_cell(at, l, cols) - cell, spread, scale))
        lat_back[l] = lat_taps(spread, scale, half, deep, -HB, wide_k)
        lat_fore[l, 0] = lat_taps(spread, scale, deep, deep, HB, wide_k)
        lat_fore[l, 1] = lat_taps(spread, scale, deep, deep, -2 * HB, wide_k)

    def tall(u, l):
        h, lo = split(u)
        out = []
        for b in range(2):
            at = slice(b * (rows - deep), b * (rows - deep) + deep)
            stack = rows_of(h[at], h[at], lo[at])
            out.append(dot(lat_fore[l, b, :, : 3 * deep], stack)[: half + HB])
        return out

    for l in range(levels):
        ext[l, HB : HB + rows, :cols] = jnp.zeros((rows, cols), F32)

    @pl.loop(0, steps)
    def _(g):
        group_load(alpha, a_tile, g, 2 + steps).wait()
        for l in range(levels):
            taps = rows_of(
                lanes_of(lon_taps[l, 0], edge_taps[l, 0]), lanes_of(lon_taps[l, 1], edge_taps[l, 1])
            )
            fields = [a_tile[g * GROUP + m, l] for m in range(GROUP)]
            u = dot(rows_of(*[lanes_of(a, a) for a in fields]), taps)
            side = u[:rows, cols:]
            for m in range(1, GROUP):
                mine = lane % slots // HB == m
                side = jnp.where(mine, u[m * rows : (m + 1) * rows, cols:], side)
            total = None
            for k in range(0, GROUP, 2):
                pair = [u[m * rows : (m + 1) * rows, :cols] for m in (k, k + 1)]
                top, bottom = tall(lanes_of(*pair), l)
                for i, m in enumerate((k, k + 1)):
                    at = slice(i * cols, (i + 1) * cols)
                    v = rows_of(top[HB:, at], bottom[:half, at])
                    part = p_tile[g * GROUP + m, l].astype(F32) * v
                    total = part if total is None else total + part
                    v_strip[g * GROUP + m, l] = rows_of(top[:HB, at], bottom[half:, at])
            ext[l, HB : HB + rows, :cols] += total
            v_side[g, l] = rows_of(*tall(side, l))

    for one in p_rows:
        one.arrive()

    for one in f_rows:
        one.arrive()
    for one in small:
        one.arrive()
    lat_at = lanes_of(lat_i[...], lat_i_low[:, frows - FR :], lat_i_high[:, :FR]).astype(F32)
    lat_by = lanes_of(lat_w[...], lat_w_low[:, frows - FR :], lat_w_high[:, :FR])
    lat_at = lat_at - (lax.axis_index("gy") * rows).astype(F32)
    lon_at = lanes_of(lon_i[...], lon_i_west[:, fcols - FC :], lon_i_east[:, :FC]).astype(F32)
    lon_by = lanes_of(lon_w[...], lon_w_west[:, fcols - FC :], lon_w_east[:, :FC])
    lon_total = float(cols * lax.axis_size("gx"))
    lon_at = lon_at - (lax.axis_index("gx") * cols).astype(F32)
    lon_at = jnp.where(
        lon_at < -64.0, lon_at + lon_total, jnp.where(lon_at >= lon_total - 64.0, lon_at - lon_total, lon_at)
    )
    f_tall, f_wide = frows + 2 * FR, fcols + 2 * FC

    def upright(at, by):
        size = at.shape[1]
        space = jnp.zeros((1, -size % 128), F32)
        at, by = lanes_of(at, space), lanes_of(by, space)
        shape = (8, at.shape[1])
        both = jnp.where(iota(shape, 0) == 0, jnp.broadcast_to(at, shape), jnp.broadcast_to(by, shape))
        both = both.T[:size]
        return both[:, 0:1], both[:, 1:2]

    lat_at_up, lat_by_up = upright(lat_at, lat_by)
    lon_at_up, lon_by_up = upright(lon_at, lon_by)
    t_rows, e_rows = rows + 2 * CR, rows + 2 * HB
    up_lat[0], up_lat[1] = split(weigh(iota((f_tall, t_rows), 1) - CR, lat_at_up, lat_by_up))
    down_lat[0], down_lat[1] = split(weigh(iota((e_rows, f_tall), 0) - HB, lat_at, lat_by))
    order = iota((2 * cols, f_wide), 0)
    w = order - cols
    wing = jnp.where(
        w < REACH,
        w - (REACH - HB),
        jnp.where(
            (w >= slots - HB) & (w < slots),
            w - slots,
            jnp.where(
                (w >= slots) & (w < slots + REACH),
                w - slots + cols - HB,
                jnp.where(w >= cols - HB, w + HB, -1000),
            ),
        ),
    )
    up_lon[0], up_lon[1] = split(weigh(jnp.where(w < 0, order, wing), lon_at, lon_by))
    order = iota((f_wide, 2 * cols), 1)
    cell = jnp.where(order < cols, order, side_cell(order - cols, ma, cols))
    down_lon[0], down_lon[1] = split(weigh(cell, lon_at_up, lon_by_up))

    for l in range(levels):

        def strips(g, sums):
            north, south = sums
            for k in range(GROUP):
                m = g * GROUP + k
                north = north + p_north[m, l].astype(F32) * v_strip[m, l, :HB]
                south = south + p_south[m, l].astype(F32) * v_strip[m, l, HB:]
            return north, south

        zero = jnp.zeros((HB, cols), F32)
        north, south = lax.fori_loop(0, steps, strips, (zero, zero))
        ext[l, :HB, :cols] = north
        ext[l, HB + rows :, :cols] = south

    for one in f_arrive:
        one.arrive()
    for i in range(2):

        def wing_of(part):
            def opened(first, last):
                lanes = range(FC * i, 2 * FOLD * FC, 2 * FC)
                return [part[first:last, x : x + FC] for x in lanes]

            low, high = f_main, f_main + HB
            return rows_of(
                rows_of(*opened(0, low))[:frows], *opened(low, high), *opened(high, high + HB)
            )

        fine_wide[i] = lanes_of(
            rows_of(fine_tile[i], f_low[i], f_high[i]), wing_of(f_west), wing_of(f_east)
        )

    thick = iota((rows, cols), 1) // slots
    thin = iota((2 * HB, cols), 1) // slots
    side_sums = [None] * levels
    for g in range(steps):
        for one in p_arrive[g]:
            one.arrive()
        for l in range(levels):
            west, east = p_west[g, :rows].astype(F32), p_east[g, :rows].astype(F32)
            part = jnp.where(thick == l, west, east) * v_side[g, l, HB : HB + rows]
            side_sums[l] = part if g == 0 else side_sums[l] + part
    for one in corners:
        one.arrive()
    t_lane, e_lane = iota((t_rows, cols), 1), iota((e_rows, cols), 1)

    def fold(x, first, deep):
        total = None
        lane_at = iota((deep, cols), 1)
        for b in range(x.shape[0] // deep):
            part = pltpu.roll(x[b * deep : (b + 1) * deep], (b * REACH - first) % cols, 1)
            total = part if total is None else jnp.where(lane_at >= b * REACH, part, total)
        return total

    def unfold(x, first, start, blocks):
        parts = [pltpu.roll(x, (first - b * REACH) % cols, 1) for b in range(start, start + blocks)]
        return rows_of(*parts)

    for l in range(levels):
        ends = None
        for g in range(steps):
            west, east = p_west[g, rows:].astype(F32), p_east[g, rows:].astype(F32)
            v = rows_of(v_side[g, l, :HB], v_side[g, l, HB + rows :])
            part = jnp.where(thin == l, west, east) * v
            ends = part if ends is None else ends + part
        side = rows_of(ends[:HB], side_sums[l], ends[HB:])
        if l:
            side = pltpu.roll(side, slots, 1)
        for shift in (HB, 2 * HB, 4 * HB):
            side = side + pltpu.roll(side, shift, 1)
        ext[l, :, cols:] = side
        core = ext[l, :, :cols]
        eastward = jnp.where(e_lane >= cols - HB, side, pltpu.roll(core, cols - HB, 1))
        westward = jnp.where(e_lane < slots, side, pltpu.roll(core, slots, 1))
        for i, (x, first) in enumerate(((eastward, cols - REACH), (westward, slots - HB))):
            flank[l, i] = fold(x, first, STRIP)
            tip[l, i] = fold(rows_of(x[e_rows - STRIP :], x[:STRIP]), first, HB)

    sent = []
    for s in range(count):
        peer = lax.rem(ma + s, count)
        for i, step in enumerate((1, -1)):
            side = lax.rem(gx + step + gxn, gxn)
            sent.append(link("gx", step, flank.at[peer, i], flanks.at[s, i], {"ma": peer}))
            for j, turn in enumerate((1, -1)):
                at = {"gx": side, "ma": peer}
                sent.append(link("gy", turn, tip.at[peer, i], tips.at[s, i, j], at))
        sent.append(link("gy", 1, ext.at[peer, pl.ds(e_rows - STRIP, STRIP)], ends_in.at[s, 0], {"ma": peer}))
        sent.append(link("gy", -1, ext.at[peer, pl.ds(0, STRIP)], ends_in.at[s, 1], {"ma": peer}))
        if s:
            sent.append(link("ma", peer - ma, ext.at[peer], other.at[s - 1]))
    for one in sent:
        one.start()
    for one in sent:
        one.arrive()
    mine, strips_in, flank_in, tip_in = ext[ma], ends_in[0], flanks[0], tips[0]
    for s in range(1, count):
        mine = mine + other[s - 1]
        strips_in, flank_in, tip_in = strips_in + ends_in[s], flank_in + flanks[s], tip_in + tips[s]
    lap = CR - HB
    edge = STRIP - lap

    def merge(above, middle, below):
        return rows_of(
            above[:lap],
            middle[:edge] + above[lap:],
            middle[edge : e_rows - edge],
            middle[e_rows - edge :] + below[:edge],
            below[edge:],
        )

    mine = merge(strips_in[0], mine, strips_in[1])
    core, side = mine[:, :cols], mine[:, cols:]
    third = STRIP // HB

    def wing_from(i, first):
        return merge(
            unfold(tip_in[i, 0], first, 0, third),
            unfold(flank_in[i], first, 0, e_rows // STRIP),
            unfold(tip_in[i, 1], first, third, third),
        )

    wings = jnp.where(
        t_lane < REACH,
        wing_from(0, 0),
        jnp.where((t_lane >= slots) & (t_lane < slots + REACH), wing_from(1, slots), side),
    )
    across = dot3(split(lanes_of(core, wings)), (up_lon[0], up_lon[1]))
    fine = dot3((up_lat[0], up_lat[1]), split(across))
    increment[ma] = fine[:frows, :fcols]
    final = []

    def share(whole):
        for s in range(1, count):
            peer = lax.rem(ma + s, count)
            final.append(link("ma", peer - ma, whole.at[ma], whole.at[ma]))
            final[-1].start()

    share(increment)
    misfit = fine_wide[1] * (fine - fine_wide[0])
    across = dot3((down_lat[0], down_lat[1]), split(misfit))
    residual[ma] = dot3(split(across), (down_lon[0], down_lon[1]))
    share(residual)
    for one in final:
        one.arrive()
    for one in pending:
        one.sent()


def cost(flops, nbytes):
    return pl.CostEstimate(flops=flops, bytes_accessed=nbytes, transcendentals=0)


def core_step(widths, lat_i, lat_w, lon_i, lon_w, alpha, perts, innov, weight):
    members, levels, rows, cols = alpha.shape
    steps = members // GROUP
    frows, fcols = innov.shape[1:]
    count = lax.axis_size("ma")
    assert levels == 2 and count == levels
    assert (rows + 2 * HB) % STRIP == 0
    half = rows // 2
    deep = half + 2 * HB
    wide_k = -(-3 * deep // 128) * 128
    e_rows, t_rows = rows + 2 * HB, rows + 2 * CR
    f_tall, f_wide = frows + 2 * FR, fcols + 2 * FC
    strip = ((members, levels, HB, cols), BF16)
    side = ((steps, e_rows, cols), BF16)
    outs = [
        (innov.shape, F32),
        ((levels, e_rows, 2 * cols), F32),
        (alpha.shape, BF16),
        (alpha.shape, BF16),
        strip,
        strip,
        side,
        side,
        ((levels, 4, cols, cols), BF16),
        ((levels, half, wide_k), BF16),
    ]
    kept = sum(math.prod(shape) * jnp.dtype(kind).itemsize for shape, kind in outs)
    fine_edge = ((2, FR, fcols), F32)
    fine_side = ((-(-frows // (FOLD * HB)) * HB + 2 * HB, cols), F32)
    packed = ((steps, rows, cols), BF16)
    scratch = [
        ((2, frows, fcols), F32),
        ((levels * GROUP // 2, 2 * cols, 2 * cols), BF16),
        ((levels, 2, cols, cols), BF16),
        ((levels, 2, deep, wide_k), BF16),
        ((members, levels, 2 * HB, cols), F32),
        ((steps, levels, e_rows, cols), F32),
        packed,
        packed,
        fine_edge,
        fine_edge,
        fine_side,
        fine_side,
        fine_side,
        fine_side,
        ((2, f_tall, f_wide), F32),
        (lat_i.shape, jnp.int32),
        (lat_i.shape, jnp.int32),
        (lat_w.shape, F32),
        (lat_w.shape, F32),
        (lon_i.shape, jnp.int32),
        (lon_i.shape, jnp.int32),
        (lon_w.shape, F32),
        (lon_w.shape, F32),
        ((2, 2 * cols, f_wide), BF16),
        ((2, f_tall, t_rows), BF16),
        ((2, e_rows, f_tall), BF16),
        ((2, f_wide, 2 * cols), BF16),
        ((levels, e_rows, 2 * cols), F32),
        ((count - 1, e_rows, 2 * cols), F32),
        ((count, 2, STRIP, 2 * cols), F32),
        ((levels, 2, STRIP, cols), F32),
        ((levels, 2, HB, cols), F32),
        ((count, 2, STRIP, cols), F32),
        ((count, 2, 2, HB, cols), F32),
    ]
    vmem = pl.BlockSpec(memory_space=pltpu.VMEM)
    anywhere = pl.BlockSpec(memory_space=pltpu.HBM)
    return pl.pallas_call(
        core_kernel,
        in_specs=[pl.BlockSpec(memory_space=pltpu.SMEM)] + [vmem] * 4 + [anywhere] * 4,
        out_specs=[vmem] * len(outs),
        out_shape=[pltpu.VMEM(shape, kind) for shape, kind in outs],
        scratch_shapes=[pltpu.VMEM(shape, kind) for shape, kind in scratch]
        + [
            pltpu.SemaphoreType.DMA((96,)),
            pltpu.SemaphoreType.DMA((96,)),
            pltpu.SemaphoreType.DMA((2 + 2 * steps,)),
        ],
        compiler_params=pltpu.CompilerParams(
            collective_id=0, has_side_effects=True, vmem_limit_bytes=VMEM_BYTES - VMEM_SLACK - kept
        ),
        cost_estimate=cost(2**30, 2**24),
    )(widths, lat_i, lat_w, lon_i, lon_w, alpha, perts, innov, weight)


def band(high, low, taps):
    half = taps.shape[0]
    deep = half + 2 * HB
    out = []
    for first in range(0, high.shape[0] - 2 * HB, half):
        h, lo = high[first : first + deep], low[first : first + deep]
        out.append(dot(taps, rows_of(h, h, lo)))
    return rows_of(*out)


def adjoint_kernel(
    alpha, perts, north, south, west, east, residual, lon, lat, fine, out, fine_out, sem
):
    rows, cols = alpha.shape[2:]
    slots = GROUP * HB
    g = pl.program_id(0)
    give = pltpu.make_async_copy(fine, fine_out, sem.at[0])

    @pl.when(g == 0)
    def _():
        give.start()

    @pl.when(g == pl.num_programs(0) - 1)
    def _():
        give.wait()

    zero = jnp.zeros((cols, cols), BF16)

    def stack(high, low):
        return rows_of(lanes_of(high, low), lanes_of(high, zero))

    def halves(x):
        return x[:, :cols] + x[:, cols:]

    lane = iota((rows, cols), 1)
    inner = (lane >= HB) & (lane < cols - HB)
    wide = iota((rows + 2 * HB, cols), 1)
    for l in range(alpha.shape[1]):
        res = residual[l]
        taps = lat[l, :, : 3 * (rows // 2 + 2 * HB)]
        side = jnp.where(wide // slots == l, west[g].astype(F32), east[g].astype(F32))
        edge = band(*split(natural(side, rows) * res[:, cols:]), taps)
        edge = halves(dot(lanes_of(*split(edge)), stack(lon[l, 2], lon[l, 3])))
        cores = []
        for k in range(0, GROUP, 2):
            pairs = []
            for m in (k, k + 1):
                n = g * GROUP + m
                tall = rows_of(
                    north[n, l].astype(F32), perts[n, l].astype(F32), south[n, l].astype(F32)
                )
                pairs.append(split(tall * res[:, :cols]))
            both = band(lanes_of(pairs[0][0], pairs[1][0]), lanes_of(pairs[0][1], pairs[1][1]), taps)
            for i in range(2):
                cores.append(lanes_of(*split(both[:, i * cols : (i + 1) * cols])))
        total = dot(rows_of(*cores), stack(lon[l, 0], lon[l, 1]))
        for m in range(GROUP):
            turned = pltpu.roll(edge, (cols - HB - 2 * HB * m) % cols, 1)
            value = halves(total[m * rows : (m + 1) * rows]) + jnp.where(inner, 0.0, turned)
            out[m, l] = alpha[g * GROUP + m, l].astype(F32) + value


def adjoint(alpha, perts, north, south, west, east, residual, lon, lat, fine):
    members, levels, rows, cols = alpha.shape
    return pl.pallas_call(
        adjoint_kernel,
        grid=(members // GROUP,),
        in_specs=[pl.BlockSpec(memory_space=pltpu.VMEM)] * 10,
        out_specs=[
            pl.BlockSpec((GROUP, levels, rows, cols), lambda g: (g, 0, 0, 0)),
            pl.BlockSpec(memory_space=pltpu.HBM),
        ],
        out_shape=[
            jax.ShapeDtypeStruct(alpha.shape, F32),
            jax.ShapeDtypeStruct(fine.shape, F32),
        ],
        scratch_shapes=[pltpu.SemaphoreType.DMA((1,))],
        compiler_params=pltpu.CompilerParams(vmem_limit_bytes=BACK_LIMIT),
        cost_estimate=cost(members * levels * 2**25, alpha.size * 8),
    )(alpha, perts, north, south, west, east, residual, lon, lat, fine)


def body(
    alpha_fields,
    member_perts,
    band_widths,
    lat_index,
    lat_weight,
    lon_index,
    lon_weight,
    innovation,
    obs_weight,
):
    tables = [x.reshape(1, -1) for x in (lat_index, lat_weight, lon_index, lon_weight)]
    increment, residual, alpha, perts, *rest = core_step(
        band_widths, *tables, alpha_fields, member_perts, innovation, obs_weight
    )
    north, south, west, east, lon, lat = rest
    gradient, increment = adjoint(
        alpha, perts, north, south, west, east, residual, lon, lat, increment
    )
    return (increment, gradient)


def solution(mesh):
    placed = (
        P("ma", None, "gy", "gx"),
        P("ma", None, "gy", "gx"),
        P(),
        P("gy"),
        P("gy"),
        P("gx"),
        P("gx"),
        P(None, "gy", "gx"),
        P(None, "gy", "gx"),
    )
    return jax.shard_map(
        body,
        mesh=mesh,
        in_specs=placed,
        out_specs=(P(None, "gy", "gx"), P("ma", None, "gy", "gx")),
        check_vma=False,
    )
```

```python
import math

import jax
import jax.numpy as jnp
from jax import lax
from jax.experimental import pallas as pl
from jax.experimental.pallas import tpu as pltpu
from jax.sharding import PartitionSpec as P

HB = 8
GROUP = 8
FR = 24
FC = 20
FOLD = 3
CR = 16
STRIP = 24
REACH = HB + 10
MESH = pl.DeviceIdType.MESH
VMEM_BYTES = 67043328
VMEM_SLACK = 2**17
BACK_LIMIT = 32 * 2**20
F32 = jnp.float32
BF16 = jnp.bfloat16


def iota(shape, dim):
    return lax.broadcasted_iota(jnp.int32, shape, dim)


def dot(a, b):
    return jnp.dot(a, b, preferred_element_type=F32)


def split(value):
    high = value.astype(BF16)
    return high, (value - high.astype(F32)).astype(BF16)


def dot3(a, b):
    return dot(a[0], b[0]) + dot(a[1], b[0]) + dot(a[0], b[1])


def rows_of(*parts):
    return jnp.concatenate(parts, axis=0)


def lanes_of(*parts):
    return jnp.concatenate(parts, axis=1)


def natural(x, rows):
    return rows_of(x[rows : rows + HB], x[:rows], x[rows + HB :])


def place(order, size, width):
    return jnp.where(order < size, order, jnp.where(order < size + width, order - size - width, order - width))


def tap_value(distance, spread, scale):
    d = distance.astype(F32)
    value = jnp.exp(-(d * d) / (2.0 * spread * spread)) * scale
    return jnp.where(jnp.abs(distance) <= HB, value, 0.0)


def tap_scale(spread):
    lane = iota((8, 128), 1)
    d = (lane - HB).astype(F32)
    shape = jnp.where(lane <= 2 * HB, jnp.exp(-(d * d) / (2.0 * spread * spread)), 0.0)
    return (1.0 / jnp.sqrt(jnp.sum(shape * shape, axis=1, keepdims=True)))[:1]


def lat_taps(spread, scale, height, deep, offset, width):
    i, c = iota((height, width), 0), iota((height, width), 1)
    r = jnp.where(c >= 2 * deep, c - 2 * deep, jnp.where(c >= deep, c - deep, c))
    value = tap_value(r - i + offset, spread, scale)
    high = value.astype(BF16).astype(F32)
    return jnp.where((c >= deep) & (c < 2 * deep), value - high, high).astype(BF16)


def side_cell(lane, level, cols):
    west = lane // (GROUP * HB) == level
    return jnp.where(west, lane % HB - HB, cols + lane % HB)


def weigh(cell, index, weight):
    cell = cell.astype(F32)
    return jnp.where(cell == index, 1.0 - weight, 0.0) + jnp.where(cell == index + 1.0, weight, 0.0)


class Link:
    def __init__(self, axis, step, src, dst, send, recv, slot, also=None):
        me, count = lax.axis_index(axis), lax.axis_size(axis)
        target = me + step
        self.sends = self.gets = None
        if axis == "gx":
            target = lax.rem(target + count, count)
        elif axis == "gy":
            self.sends = (target >= 0) & (target < count)
            self.gets = (me - step >= 0) & (me - step < count)
        self.dst = dst
        device = {axis: target, **(also or {})}
        self.copy = pltpu.make_async_remote_copy(
            src_ref=src,
            dst_ref=dst,
            send_sem=send.at[slot],
            recv_sem=recv.at[slot],
            device_id=device,
            device_id_type=MESH,
        )

    def start(self):
        if self.sends is None:
            self.copy.start()
        else:
            pl.when(self.sends)(self.copy.start)

    def arrive(self):
        if self.gets is None:
            self.copy.wait_recv()
        else:
            pl.when(self.gets)(self.copy.wait_recv)

            @pl.when(jnp.logical_not(self.gets))
            def _():
                self.dst[...] = jnp.zeros_like(self.dst)

    def sent(self):
        if self.sends is None:
            self.copy.wait_send()
        else:
            pl.when(self.sends)(self.copy.wait_send)


def greet():
    barrier = pltpu.get_barrier_semaphore()
    gx, gxn = lax.axis_index("gx"), lax.axis_size("gx")
    gy, gyn = lax.axis_index("gy"), lax.axis_size("gy")
    ma, count = lax.axis_index("ma"), lax.axis_size("ma")

    def hail(device):
        pl.semaphore_signal(barrier, inc=1, device_id=device, device_id_type=MESH)

    for s in range(count):
        peer = lax.rem(ma + s, count)
        if s:
            hail({"ma": peer})
        sides = [lax.rem(gx + step, gxn) for step in (1, gxn - 1)]
        for side in sides:
            hail({"gx": side, "ma": peer})
        for step, there in ((-1, gy > 0), (1, gy < gyn - 1)):

            @pl.when(there)
            def _(step=step, peer=peer, sides=sides):
                for side in (gx, *sides):
                    hail({"gx": side, "gy": gy + step, "ma": peer})

    below, above = jnp.minimum(gy, 1), jnp.minimum(gyn - 1 - gy, 1)
    return lambda: pl.semaphore_wait(barrier, 3 * count - 1 + (below + above) * 3 * count)


def core_kernel(
    widths, lat_i, lat_w, lon_i, lon_w, alpha, perts, innov, weight,
    increment, residual, a_tile, p_tile, p_north, p_south, p_west, p_east, lon_taps, lat_back,
    fine_tile, pick, edge_taps, lat_fore, v_strip, v_side, p_right, p_left,
    f_low, f_high, f_right, f_left, f_west, f_east, fine_wide,
    lat_i_low, lat_i_high, lat_w_low, lat_w_high, lon_i_west, lon_i_east, lon_w_west, lon_w_east,
    up_lon, up_lat, down_lat, down_lon, ext, other, ends_in, flank, tip, flanks, tips,
    send, recv, local,
):
    members, levels, rows, cols = alpha.shape
    steps, half, slots = members // GROUP, rows // 2, GROUP * HB
    frows, fcols = innov.shape[1:]
    ma, count = lax.axis_index("ma"), lax.axis_size("ma")
    gx, gxn = lax.axis_index("gx"), lax.axis_size("gx")
    met = greet()
    f_loads = [
        pltpu.make_async_copy(src.at[ma], fine_tile.at[i], local.at[i])
        for i, src in enumerate((innov, weight))
    ]

    def group_load(src, dst, g, first):
        span = pl.ds(g * GROUP, GROUP)
        return pltpu.make_async_copy(src.at[span], dst.at[span], local.at[first + g])

    p_loads = [group_load(perts, p_tile, g, 2) for g in range(steps)]
    for load in p_loads + f_loads:
        load.start()
    counter = iter(range(96))
    pending = []

    def link(axis, step, src, dst, also=None):
        one = Link(axis, step, src, dst, send, recv, next(counter), also)
        pending.append(one)
        return one

    r, c = iota((cols, 2 * cols), 0), iota((cols, 2 * cols), 1)
    base = jnp.where(
        ((c < cols) & (r - (cols - HB) == c % HB)) | ((c >= cols) & (r == c % HB)), 1.0, 0.0
    )
    turned = (c % cols) // slots
    slot = jnp.where(c < cols, turned, 1 - turned) * GROUP + c % slots // HB
    for l in range(levels):
        for k in range(GROUP):
            at = slice(k % 2 * cols, (k % 2 + 1) * cols)
            n = l * GROUP + k
            pick[n // 2, at] = jnp.where(slot == n, base, 0.0).astype(BF16)
    f_rows = [
        link("gy", 1, innov.at[ma, pl.ds(frows - FR, FR)], f_low.at[0]),
        link("gy", -1, innov.at[ma, pl.ds(0, FR)], f_high.at[0]),
        link("gy", 1, weight.at[ma, pl.ds(frows - FR, FR)], f_low.at[1]),
        link("gy", -1, weight.at[ma, pl.ds(0, FR)], f_high.at[1]),
    ]
    p_rows = [
        link("gy", 1, perts.at[:, :, pl.ds(rows - HB, HB), :], p_north),
        link("gy", -1, perts.at[:, :, pl.ds(0, HB), :], p_south),
    ]
    small = [
        link("gy", 1, lat_i, lat_i_low),
        link("gy", -1, lat_i, lat_i_high),
        link("gy", 1, lat_w, lat_w_low),
        link("gy", -1, lat_w, lat_w_high),
        link("gx", 1, lon_i, lon_i_west),
        link("gx", -1, lon_i, lon_i_east),
        link("gx", 1, lon_w, lon_w_west),
        link("gx", -1, lon_w, lon_w_east),
    ]
    def tilted(src, dst, side, top, bottom, first):
        pairs = []
        for step, at, to in ((1, bottom, first), (-1, top, first + HB)):
            span, there = pl.ds(at, HB), pl.ds(to, HB)
            index = (slice(None),) * (src.ndim - 2)
            pairs.append(
                link(
                    "gy",
                    step,
                    src.at[(*index, span)],
                    dst.at[(*index, there)],
                    {"gx": lax.rem(gx + side, gxn)},
                )
            )
        return pairs

    def packed(piece):
        total = None
        for l in range(levels):
            for k in range(0, GROUP, 2):
                n = (l * GROUP + k) // 2
                part = dot(lanes_of(piece(l, k), piece(l, k + 1)), pick[n])
                total = part if total is None else total + part
        return total.astype(BF16)

    a_loads = [group_load(alpha, a_tile, g, 2 + steps) for g in range(steps)]
    p_arrive = []
    def p_sides(g):
        span = pl.ds(0, rows)
        pair = [
            link("gx", 1, p_right.at[g], p_west.at[g, span]),
            link("gx", -1, p_left.at[g], p_east.at[g, span]),
        ]
        for one in pair:
            one.start()
        p_arrive.append(pair)

    for g in range(steps):
        p_loads[g].wait()
        a_loads[g].start()
        both = packed(lambda l, k: p_tile[g * GROUP + k, l])
        p_right[g] = both[:, :cols]
        p_left[g] = both[:, cols:]
        if g == 0:
            met()
            for one in small + p_rows:
                one.start()
            p_sides(g)
    corners = tilted(p_right, p_west, 1, 0, rows - HB, rows)
    corners += tilted(p_left, p_east, gxn - 1, 0, rows - HB, rows)
    for one in corners:
        one.start()
    for g in range(1, steps):
        p_sides(g)
    for one in f_rows:
        one.start()

    f_main = f_west.shape[0] - 2 * HB

    def f_fold(first, count, start):
        deep = -(-count // (FOLD * HB)) * HB
        parts = []
        for b in range(FOLD):
            stop = min(first + (b + 1) * deep, first + count)
            for i in range(2):
                part = fine_tile[i, first + b * deep : stop, start : start + FC]
                short = deep - part.shape[0]
                parts.append(rows_of(part, jnp.zeros((short, FC), F32)) if short else part)
        return lanes_of(*parts, jnp.zeros((deep, cols - 2 * FOLD * FC), F32))

    for load in f_loads:
        load.wait()
    f_arrive = []
    for step, side, src, dst, start in (
        (1, 1, f_right, f_west, fcols - FC),
        (-1, gxn - 1, f_left, f_east, 0),
    ):
        src[:f_main] = f_fold(0, frows, start)
        src[f_main : f_main + HB] = f_fold(0, FR, start)
        src[f_main + HB :] = f_fold(frows - FR, FR, start)
        span = pl.ds(0, f_main)
        f_arrive.append(link("gx", step, src.at[span], dst.at[span]))
        f_arrive += tilted(src, dst, side, f_main, f_main + HB, f_main)

    lane = iota((cols, cols), 1)
    deep = half + 2 * HB
    wide_k = lat_fore.shape[3]
    for l in range(levels):
        spread = widths[l].astype(F32)
        scale = tap_scale(spread)
        cell, at = iota((cols, cols), 0), lane
        lon_taps[l, 0], lon_taps[l, 1] = split(tap_value(cell - at, spread, scale))
        shift = at % (2 * HB)
        gap = side_cell(cell, l, cols) - jnp.where(shift < HB, cols - HB + shift, shift - HB)
        own = cell % slots // HB == at // (2 * HB)
        lon_taps[l, 2], lon_taps[l, 3] = split(jnp.where(own, tap_value(gap, spread, scale), 0.0))
        edge_taps[l, 0], edge_taps[l, 1] = split(tap_value(side_cell(at, l, cols) - cell, spread, scale))
        lat_back[l] = lat_taps(spread, scale, half, deep, -HB, wide_k)
        lat_fore[l, 0] = lat_taps(spread, scale, deep, deep, HB, wide_k)
        lat_fore[l, 1] = lat_taps(spread, scale, deep, deep, -2 * HB, wide_k)

    def tall(u, l):
        h, lo = split(u)
        out = []
        for b in range(2):
            at = slice(b * (rows - deep), b * (rows - deep) + deep)
            stack = rows_of(h[at], h[at], lo[at])
            out.append(dot(lat_fore[l, b, :, : 3 * deep], stack)[: half + HB])
        return out

    for l in range(levels):
        ext[l, HB : HB + rows, :cols] = jnp.zeros((rows, cols), F32)

    @pl.loop(0, steps)
    def _(g):
        group_load(alpha, a_tile, g, 2 + steps).wait()
        for l in range(levels):
            taps = rows_of(
                lanes_of(lon_taps[l, 0], edge_taps[l, 0]), lanes_of(lon_taps[l, 1], edge_taps[l, 1])
            )
            fields = [a_tile[g * GROUP + m, l] for m in range(GROUP)]
            u = dot(rows_of(*[lanes_of(a, a) for a in fields]), taps)
            side = u[:rows, cols:]
            for m in range(1, GROUP):
                mine = lane % slots // HB == m
                side = jnp.where(mine, u[m * rows : (m + 1) * rows, cols:], side)
            total = None
            for k in range(0, GROUP, 2):
                pair = [u[m * rows : (m + 1) * rows, :cols] for m in (k, k + 1)]
                top, bottom = tall(lanes_of(*pair), l)
                for i, m in enumerate((k, k + 1)):
                    at = slice(i * cols, (i + 1) * cols)
                    v = rows_of(top[HB:, at], bottom[:half, at])
                    part = p_tile[g * GROUP + m, l].astype(F32) * v
                    total = part if total is None else total + part
                    v_strip[g * GROUP + m, l] = rows_of(top[:HB, at], bottom[half:, at])
            ext[l, HB : HB + rows, :cols] += total
            v_side[g, l] = rows_of(*tall(side, l))

    for one in p_rows:
        one.arrive()

    for one in f_rows:
        one.arrive()
    for one in small:
        one.arrive()
    lat_at = lanes_of(lat_i[...], lat_i_low[:, frows - FR :], lat_i_high[:, :FR]).astype(F32)
    lat_by = lanes_of(lat_w[...], lat_w_low[:, frows - FR :], lat_w_high[:, :FR])
    lat_at = lat_at - (lax.axis_index("gy") * rows).astype(F32)
    lon_at = lanes_of(lon_i[...], lon_i_west[:, fcols - FC :], lon_i_east[:, :FC]).astype(F32)
    lon_by = lanes_of(lon_w[...], lon_w_west[:, fcols - FC :], lon_w_east[:, :FC])
    lon_total = float(cols * lax.axis_size("gx"))
    lon_at = lon_at - (lax.axis_index("gx") * cols).astype(F32)
    lon_at = jnp.where(
        lon_at < -64.0, lon_at + lon_total, jnp.where(lon_at >= lon_total - 64.0, lon_at - lon_total, lon_at)
    )
    f_tall, f_wide = frows + 2 * FR, fcols + 2 * FC

    def upright(at, by):
        size = at.shape[1]
        space = jnp.zeros((1, -size % 128), F32)
        at, by = lanes_of(at, space), lanes_of(by, space)
        shape = (8, at.shape[1])
        both = jnp.where(iota(shape, 0) == 0, jnp.broadcast_to(at, shape), jnp.broadcast_to(by, shape))
        both = both.T[:size]
        return both[:, 0:1], both[:, 1:2]

    lat_at_up, lat_by_up = upright(lat_at, lat_by)
    lon_at_up, lon_by_up = upright(lon_at, lon_by)
    t_rows, e_rows = rows + 2 * CR, rows + 2 * HB
    up_lat[0], up_lat[1] = split(weigh(iota((f_tall, t_rows), 1) - CR, lat_at_up, lat_by_up))
    down_lat[0], down_lat[1] = split(weigh(iota((e_rows, f_tall), 0) - HB, lat_at, lat_by))
    order = iota((2 * cols, f_wide), 0)
    w = order - cols
    wing = jnp.where(
        w < REACH,
        w - (REACH - HB),
        jnp.where(
            (w >= slots - HB) & (w < slots),
            w - slots,
            jnp.where(
                (w >= slots) & (w < slots + REACH),
                w - slots + cols - HB,
                jnp.where(w >= cols - HB, w + HB, -1000),
            ),
        ),
    )
    up_lon[0], up_lon[1] = split(weigh(jnp.where(w < 0, order, wing), lon_at, lon_by))
    order = iota((f_wide, 2 * cols), 1)
    cell = jnp.where(order < cols, order, side_cell(order - cols, ma, cols))
    down_lon[0], down_lon[1] = split(weigh(cell, lon_at_up, lon_by_up))

    for l in range(levels):

        def strips(g, sums):
            north, south = sums
            for k in range(GROUP):
                m = g * GROUP + k
                north = north + p_north[m, l].astype(F32) * v_strip[m, l, :HB]
                south = south + p_south[m, l].astype(F32) * v_strip[m, l, HB:]
            return north, south

        zero = jnp.zeros((HB, cols), F32)
        north, south = lax.fori_loop(0, steps, strips, (zero, zero))
        ext[l, :HB, :cols] = north
        ext[l, HB + rows :, :cols] = south

    for i in range(2):
        fine_wide[i, :, :fcols] = rows_of(fine_tile[i], f_low[i], f_high[i])

    thick = iota((rows, cols), 1) // slots
    thin = iota((2 * HB, cols), 1) // slots
    side_sums = [None] * levels
    for g in range(steps):
        for one in p_arrive[g]:
            one.arrive()
        for l in range(levels):
            west, east = p_west[g, :rows].astype(F32), p_east[g, :rows].astype(F32)
            part = jnp.where(thick == l, west, east) * v_side[g, l, HB : HB + rows]
            side_sums[l] = part if g == 0 else side_sums[l] + part
    for one in corners:
        one.arrive()
    t_lane, e_lane = iota((t_rows, cols), 1), iota((e_rows, cols), 1)

    def fold(x, first, deep):
        total = None
        lane_at = iota((deep, cols), 1)
        for b in range(x.shape[0] // deep):
            part = pltpu.roll(x[b * deep : (b + 1) * deep], (b * REACH - first) % cols, 1)
            total = part if total is None else jnp.where(lane_at >= b * REACH, part, total)
        return total

    def unfold(x, first, start, blocks):
        parts = [pltpu.roll(x, (first - b * REACH) % cols, 1) for b in range(start, start + blocks)]
        return rows_of(*parts)

    for l in range(levels):
        ends = None
        for g in range(steps):
            west, east = p_west[g, rows:].astype(F32), p_east[g, rows:].astype(F32)
            v = rows_of(v_side[g, l, :HB], v_side[g, l, HB + rows :])
            part = jnp.where(thin == l, west, east) * v
            ends = part if ends is None else ends + part
        side = rows_of(ends[:HB], side_sums[l], ends[HB:])
        if l:
            side = pltpu.roll(side, slots, 1)
        for shift in (HB, 2 * HB, 4 * HB):
            side = side + pltpu.roll(side, shift, 1)
        ext[l, :, cols:] = side
        core = ext[l, :, :cols]
        eastward = jnp.where(e_lane >= cols - HB, side, pltpu.roll(core, cols - HB, 1))
        westward = jnp.where(e_lane < slots, side, pltpu.roll(core, slots, 1))
        for i, (x, first) in enumerate(((eastward, cols - REACH), (westward, slots - HB))):
            flank[l, i] = fold(x, first, STRIP)
            tip[l, i] = fold(rows_of(x[e_rows - STRIP :], x[:STRIP]), first, HB)

    corner_links, side_links, end_links, swaps = [], [], [], []
    for s in range(count):
        peer = lax.rem(ma + s, count)
        for i, step in enumerate((1, -1)):
            at = {"ma": peer}
            side_links.append(link("gx", step, flank.at[peer, i], flanks.at[s, i], at))
            strip = ext.at[peer, pl.ds((e_rows - STRIP) * (1 - i), STRIP)]
            end_links.append(link("gy", step, strip, ends_in.at[s, i], at))
            at = {"gx": lax.rem(gx + step + gxn, gxn), "ma": peer}
            for j, turn in enumerate((1, -1)):
                corner_links.append(link("gy", turn, tip.at[peer, i], tips.at[s, i, j], at))
        if s:
            swaps.append(link("ma", peer - ma, ext.at[peer], other.at[s - 1]))
    sent = corner_links + side_links + end_links + swaps
    for one in sent + f_arrive:
        one.start()
    for one in sent:
        one.arrive()
    mine, strips_in, flank_in, tip_in = ext[ma], ends_in[0], flanks[0], tips[0]
    for s in range(1, count):
        mine = mine + other[s - 1]
        strips_in, flank_in, tip_in = strips_in + ends_in[s], flank_in + flanks[s], tip_in + tips[s]
    lap = CR - HB
    edge = STRIP - lap

    def merge(above, middle, below):
        return rows_of(
            above[:lap],
            middle[:edge] + above[lap:],
            middle[edge : e_rows - edge],
            middle[e_rows - edge :] + below[:edge],
            below[edge:],
        )

    mine = merge(strips_in[0], mine, strips_in[1])
    core, side = mine[:, :cols], mine[:, cols:]
    third = STRIP // HB

    def wing_from(i, first):
        return merge(
            unfold(tip_in[i, 0], first, 0, third),
            unfold(flank_in[i], first, 0, e_rows // STRIP),
            unfold(tip_in[i, 1], first, third, third),
        )

    wings = jnp.where(
        t_lane < REACH,
        wing_from(0, 0),
        jnp.where((t_lane >= slots) & (t_lane < slots + REACH), wing_from(1, slots), side),
    )
    across = dot3(split(lanes_of(core, wings)), (up_lon[0], up_lon[1]))
    fine = dot3((up_lat[0], up_lat[1]), split(across))
    increment[ma] = fine[:frows, :fcols]
    final = []

    def share(whole):
        for s in range(1, count):
            peer = lax.rem(ma + s, count)
            final.append(link("ma", peer - ma, whole.at[ma], whole.at[ma]))
            final[-1].start()

    share(increment)
    for one in f_arrive:
        one.arrive()
    for i in range(2):

        def wing_of(part):
            def opened(first, last):
                lanes = range(FC * i, 2 * FOLD * FC, 2 * FC)
                return [part[first:last, x : x + FC] for x in lanes]

            low, high = f_main, f_main + HB
            return rows_of(
                rows_of(*opened(0, low))[:frows], *opened(low, high), *opened(high, high + HB)
            )

        fine_wide[i, :, fcols:] = lanes_of(wing_of(f_west), wing_of(f_east))
    misfit = fine_wide[1] * (fine - fine_wide[0])
    across = dot3((down_lat[0], down_lat[1]), split(misfit))
    residual[ma] = dot3(split(across), (down_lon[0], down_lon[1]))
    share(residual)
    for one in final:
        one.arrive()
    for one in pending:
        one.sent()


def cost(flops, nbytes):
    return pl.CostEstimate(flops=flops, bytes_accessed=nbytes, transcendentals=0)


def core_step(widths, lat_i, lat_w, lon_i, lon_w, alpha, perts, innov, weight):
    members, levels, rows, cols = alpha.shape
    steps = members // GROUP
    frows, fcols = innov.shape[1:]
    count = lax.axis_size("ma")
    assert levels == 2 and count == levels
    assert (rows + 2 * HB) % STRIP == 0
    half = rows // 2
    deep = half + 2 * HB
    wide_k = -(-3 * deep // 128) * 128
    e_rows, t_rows = rows + 2 * HB, rows + 2 * CR
    f_tall, f_wide = frows + 2 * FR, fcols + 2 * FC
    strip = ((members, levels, HB, cols), BF16)
    side = ((steps, e_rows, cols), BF16)
    outs = [
        (innov.shape, F32),
        ((levels, e_rows, 2 * cols), F32),
        (alpha.shape, BF16),
        (alpha.shape, BF16),
        strip,
        strip,
        side,
        side,
        ((levels, 4, cols, cols), BF16),
        ((levels, half, wide_k), BF16),
    ]
    kept = sum(math.prod(shape) * jnp.dtype(kind).itemsize for shape, kind in outs)
    fine_edge = ((2, FR, fcols), F32)
    fine_side = ((-(-frows // (FOLD * HB)) * HB + 2 * HB, cols), F32)
    packed = ((steps, rows, cols), BF16)
    scratch = [
        ((2, frows, fcols), F32),
        ((levels * GROUP // 2, 2 * cols, 2 * cols), BF16),
        ((levels, 2, cols, cols), BF16),
        ((levels, 2, deep, wide_k), BF16),
        ((members, levels, 2 * HB, cols), F32),
        ((steps, levels, e_rows, cols), F32),
        packed,
        packed,
        fine_edge,
        fine_edge,
        fine_side,
        fine_side,
        fine_side,
        fine_side,
        ((2, f_tall, f_wide), F32),
        (lat_i.shape, jnp.int32),
        (lat_i.shape, jnp.int32),
        (lat_w.shape, F32),
        (lat_w.shape, F32),
        (lon_i.shape, jnp.int32),
        (lon_i.shape, jnp.int32),
        (lon_w.shape, F32),
        (lon_w.shape, F32),
        ((2, 2 * cols, f_wide), BF16),
        ((2, f_tall, t_rows), BF16),
        ((2, e_rows, f_tall), BF16),
        ((2, f_wide, 2 * cols), BF16),
        ((levels, e_rows, 2 * cols), F32),
        ((count - 1, e_rows, 2 * cols), F32),
        ((count, 2, STRIP, 2 * cols), F32),
        ((levels, 2, STRIP, cols), F32),
        ((levels, 2, HB, cols), F32),
        ((count, 2, STRIP, cols), F32),
        ((count, 2, 2, HB, cols), F32),
    ]
    vmem = pl.BlockSpec(memory_space=pltpu.VMEM)
    anywhere = pl.BlockSpec(memory_space=pltpu.HBM)
    return pl.pallas_call(
        core_kernel,
        in_specs=[pl.BlockSpec(memory_space=pltpu.SMEM)] + [vmem] * 4 + [anywhere] * 4,
        out_specs=[vmem] * len(outs),
        out_shape=[pltpu.VMEM(shape, kind) for shape, kind in outs],
        scratch_shapes=[pltpu.VMEM(shape, kind) for shape, kind in scratch]
        + [
            pltpu.SemaphoreType.DMA((96,)),
            pltpu.SemaphoreType.DMA((96,)),
            pltpu.SemaphoreType.DMA((2 + 2 * steps,)),
        ],
        compiler_params=pltpu.CompilerParams(
            collective_id=0, has_side_effects=True, vmem_limit_bytes=VMEM_BYTES - VMEM_SLACK - kept
        ),
        cost_estimate=cost(2**30, 2**24),
    )(widths, lat_i, lat_w, lon_i, lon_w, alpha, perts, innov, weight)


def band(high, low, taps):
    half = taps.shape[0]
    deep = half + 2 * HB
    out = []
    for first in range(0, high.shape[0] - 2 * HB, half):
        h, lo = high[first : first + deep], low[first : first + deep]
        out.append(dot(taps, rows_of(h, h, lo)))
    return rows_of(*out)


def adjoint_kernel(
    alpha, perts, north, south, west, east, residual, lon, lat, fine, out, fine_out, held, sem, fine_sem
):
    levels, rows, cols = alpha.shape[1:]
    slots = GROUP * HB
    g, steps = pl.program_id(0), pl.num_programs(0)
    give = pltpu.make_async_copy(fine, fine_out, fine_sem)
    slot = lax.rem(g, 2)

    def store(step, l):
        at = lax.rem(step, 2)
        target = out.at[pl.ds(step * GROUP, GROUP), l]
        return pltpu.make_async_copy(held.at[at, l], target, sem.at[at, l])

    @pl.when(g == 0)
    def _():
        give.start()

    zero = jnp.zeros((cols, cols), BF16)

    def stack(high, low):
        return rows_of(lanes_of(high, low), lanes_of(high, zero))

    def halves(x):
        return x[:, :cols] + x[:, cols:]

    lane = iota((rows, cols), 1)
    inner = (lane >= HB) & (lane < cols - HB)
    wide = iota((rows + 2 * HB, cols), 1)
    for l in range(levels):

        @pl.when(g >= 2)
        def _(l=l):
            store(g - 2, l).wait()

        res = residual[l]
        taps = lat[l, :, : 3 * (rows // 2 + 2 * HB)]
        side = jnp.where(wide // slots == l, west[g].astype(F32), east[g].astype(F32))
        edge = band(*split(natural(side, rows) * res[:, cols:]), taps)
        edge = halves(dot(lanes_of(*split(edge)), stack(lon[l, 2], lon[l, 3])))
        cores = []
        for k in range(0, GROUP, 2):
            pairs = []
            for m in (k, k + 1):
                n = g * GROUP + m
                tall = rows_of(
                    north[n, l].astype(F32), perts[n, l].astype(F32), south[n, l].astype(F32)
                )
                pairs.append(split(tall * res[:, :cols]))
            both = band(lanes_of(pairs[0][0], pairs[1][0]), lanes_of(pairs[0][1], pairs[1][1]), taps)
            for i in range(2):
                cores.append(lanes_of(*split(both[:, i * cols : (i + 1) * cols])))
        total = dot(rows_of(*cores), stack(lon[l, 0], lon[l, 1]))
        for m in range(GROUP):
            turned = pltpu.roll(edge, (cols - HB - 2 * HB * m) % cols, 1)
            value = halves(total[m * rows : (m + 1) * rows]) + jnp.where(inner, 0.0, turned)
            held[slot, l, m] = alpha[g * GROUP + m, l].astype(F32) + value
        store(g, l).start()

    @pl.when(g == steps - 1)
    def _():
        give.wait()
        for l in range(levels):
            store(g - 1, l).wait()
        for l in range(levels):
            store(g, l).wait()


def adjoint(alpha, perts, north, south, west, east, residual, lon, lat, fine):
    members, levels, rows, cols = alpha.shape
    return pl.pallas_call(
        adjoint_kernel,
        grid=(members // GROUP,),
        in_specs=[pl.BlockSpec(memory_space=pltpu.VMEM)] * 10,
        out_specs=[pl.BlockSpec(memory_space=pltpu.HBM)] * 2,
        out_shape=[
            jax.ShapeDtypeStruct(alpha.shape, F32),
            jax.ShapeDtypeStruct(fine.shape, F32),
        ],
        scratch_shapes=[
            pltpu.VMEM((2, levels, GROUP, rows, cols), F32),
            pltpu.SemaphoreType.DMA((2, levels)),
            pltpu.SemaphoreType.DMA,
        ],
        compiler_params=pltpu.CompilerParams(vmem_limit_bytes=BACK_LIMIT),
        cost_estimate=cost(members * levels * 2**25, alpha.size * 8),
    )(alpha, perts, north, south, west, east, residual, lon, lat, fine)


def body(
    alpha_fields,
    member_perts,
    band_widths,
    lat_index,
    lat_weight,
    lon_index,
    lon_weight,
    innovation,
    obs_weight,
):
    tables = [x.reshape(1, -1) for x in (lat_index, lat_weight, lon_index, lon_weight)]
    increment, residual, alpha, perts, *rest = core_step(
        band_widths, *tables, alpha_fields, member_perts, innovation, obs_weight
    )
    north, south, west, east, lon, lat = rest
    gradient, increment = adjoint(
        alpha, perts, north, south, west, east, residual, lon, lat, increment
    )
    return (increment, gradient)


def solution(mesh):
    placed = (
        P("ma", None, "gy", "gx"),
        P("ma", None, "gy", "gx"),
        P(),
        P("gy"),
        P("gy"),
        P("gx"),
        P("gx"),
        P(None, "gy", "gx"),
        P(None, "gy", "gx"),
    )
    return jax.shard_map(
        body,
        mesh=mesh,
        in_specs=placed,
        out_specs=(P(None, "gy", "gx"), P("ma", None, "gy", "gx")),
        check_vma=False,
    )
```

```python
import math

import jax
import jax.numpy as jnp
from jax import lax
from jax.experimental import pallas as pl
from jax.experimental.pallas import tpu as pltpu
from jax.sharding import PartitionSpec as P

HB = 8
GROUP = 8
FR = 24
FC = 20
FOLD = 3
CR = 16
STRIP = 24
REACH = HB + 10
MESH = pl.DeviceIdType.MESH
VMEM_BYTES = 67043328
VMEM_SLACK = 2**17
BACK_LIMIT = 32 * 2**20
F32 = jnp.float32
BF16 = jnp.bfloat16


def iota(shape, dim):
    return lax.broadcasted_iota(jnp.int32, shape, dim)


def dot(a, b):
    return jnp.dot(a, b, preferred_element_type=F32)


def split(value):
    high = value.astype(BF16)
    return high, (value - high.astype(F32)).astype(BF16)


def dot3(a, b):
    return dot(a[0], b[0]) + dot(a[1], b[0]) + dot(a[0], b[1])


def rows_of(*parts):
    return jnp.concatenate(parts, axis=0)


def lanes_of(*parts):
    return jnp.concatenate(parts, axis=1)


def natural(x, rows):
    return rows_of(x[rows : rows + HB], x[:rows], x[rows + HB :])


def place(order, size, width):
    return jnp.where(order < size, order, jnp.where(order < size + width, order - size - width, order - width))


def tap_value(distance, spread, scale):
    d = distance.astype(F32)
    value = jnp.exp(-(d * d) / (2.0 * spread * spread)) * scale
    return jnp.where(jnp.abs(distance) <= HB, value, 0.0)


def tap_scale(spread):
    lane = iota((8, 128), 1)
    d = (lane - HB).astype(F32)
    shape = jnp.where(lane <= 2 * HB, jnp.exp(-(d * d) / (2.0 * spread * spread)), 0.0)
    return (1.0 / jnp.sqrt(jnp.sum(shape * shape, axis=1, keepdims=True)))[:1]


def lat_taps(spread, scale, height, deep, offset, width):
    i, c = iota((height, width), 0), iota((height, width), 1)
    r = jnp.where(c >= 2 * deep, c - 2 * deep, jnp.where(c >= deep, c - deep, c))
    value = tap_value(r - i + offset, spread, scale)
    high = value.astype(BF16).astype(F32)
    return jnp.where((c >= deep) & (c < 2 * deep), value - high, high).astype(BF16)


def side_cell(lane, level, cols):
    west = lane // (GROUP * HB) == level
    return jnp.where(west, lane % HB - HB, cols + lane % HB)


def weigh(cell, index, weight):
    cell = cell.astype(F32)
    return jnp.where(cell == index, 1.0 - weight, 0.0) + jnp.where(cell == index + 1.0, weight, 0.0)


class Link:
    def __init__(self, axis, step, src, dst, send, recv, slot, also=None):
        me, count = lax.axis_index(axis), lax.axis_size(axis)
        target = me + step
        self.sends = self.gets = None
        if axis == "gx":
            target = lax.rem(target + count, count)
        elif axis == "gy":
            self.sends = (target >= 0) & (target < count)
            self.gets = (me - step >= 0) & (me - step < count)
        self.dst = dst
        device = {axis: target, **(also or {})}
        self.copy = pltpu.make_async_remote_copy(
            src_ref=src,
            dst_ref=dst,
            send_sem=send.at[slot],
            recv_sem=recv.at[slot],
            device_id=device,
            device_id_type=MESH,
        )

    def start(self):
        if self.sends is None:
            self.copy.start()
        else:
            pl.when(self.sends)(self.copy.start)

    def arrive(self):
        if self.gets is None:
            self.copy.wait_recv()
        else:
            pl.when(self.gets)(self.copy.wait_recv)

            @pl.when(jnp.logical_not(self.gets))
            def _():
                self.dst[...] = jnp.zeros_like(self.dst)

    def sent(self):
        if self.sends is None:
            self.copy.wait_send()
        else:
            pl.when(self.sends)(self.copy.wait_send)


def greet():
    barrier = pltpu.get_barrier_semaphore()
    gx, gxn = lax.axis_index("gx"), lax.axis_size("gx")
    gy, gyn = lax.axis_index("gy"), lax.axis_size("gy")
    ma, count = lax.axis_index("ma"), lax.axis_size("ma")

    def hail(device):
        pl.semaphore_signal(barrier, inc=1, device_id=device, device_id_type=MESH)

    for s in range(count):
        peer = lax.rem(ma + s, count)
        if s:
            hail({"ma": peer})
        sides = [lax.rem(gx + step, gxn) for step in (1, gxn - 1)]
        for side in sides:
            hail({"gx": side, "ma": peer})
        for step, there in ((-1, gy > 0), (1, gy < gyn - 1)):

            @pl.when(there)
            def _(step=step, peer=peer, sides=sides):
                for side in (gx, *sides):
                    hail({"gx": side, "gy": gy + step, "ma": peer})

    below, above = jnp.minimum(gy, 1), jnp.minimum(gyn - 1 - gy, 1)
    return lambda: pl.semaphore_wait(barrier, 3 * count - 1 + (below + above) * 3 * count)


def core_kernel(
    widths, lat_i, lat_w, lon_i, lon_w, alpha, perts, innov, weight,
    increment, residual, a_tile, p_tile, p_north, p_south, p_west, p_east, lon_taps, lat_back,
    fine_tile, pick, edge_taps, lat_fore, v_strip, v_side, p_right, p_left,
    f_low, f_high, f_right, f_left, f_west, f_east, fine_wide,
    lat_i_low, lat_i_high, lat_w_low, lat_w_high, lon_i_west, lon_i_east, lon_w_west, lon_w_east,
    up_lon, up_lat, down_lat, down_lon, ext, other, ends_in, flank, tip, flanks, tips,
    send, recv, local,
):
    members, levels, rows, cols = alpha.shape
    steps, half, slots = members // GROUP, rows // 2, GROUP * HB
    frows, fcols = innov.shape[1:]
    ma, count = lax.axis_index("ma"), lax.axis_size("ma")
    gx, gxn = lax.axis_index("gx"), lax.axis_size("gx")
    met = greet()
    f_loads = [
        pltpu.make_async_copy(src.at[ma], fine_tile.at[i], local.at[i])
        for i, src in enumerate((innov, weight))
    ]

    def group_load(src, dst, g, first):
        span = pl.ds(g * GROUP, GROUP)
        return pltpu.make_async_copy(src.at[span], dst.at[span], local.at[first + g])

    p_loads = [group_load(perts, p_tile, g, 2) for g in range(steps)]
    for load in p_loads + f_loads:
        load.start()
    counter = iter(range(96))
    pending = []

    def link(axis, step, src, dst, also=None):
        one = Link(axis, step, src, dst, send, recv, next(counter), also)
        pending.append(one)
        return one

    r, c = iota((cols, 2 * cols), 0), iota((cols, 2 * cols), 1)
    base = jnp.where(
        ((c < cols) & (r - (cols - HB) == c % HB)) | ((c >= cols) & (r == c % HB)), 1.0, 0.0
    )
    turned = (c % cols) // slots
    slot = jnp.where(c < cols, turned, 1 - turned) * GROUP + c % slots // HB
    for l in range(levels):
        for k in range(GROUP):
            at = slice(k % 2 * cols, (k % 2 + 1) * cols)
            n = l * GROUP + k
            pick[n // 2, at] = jnp.where(slot == n, base, 0.0).astype(BF16)
    f_rows = [
        link("gy", 1, innov.at[ma, pl.ds(frows - FR, FR)], f_low.at[0]),
        link("gy", -1, innov.at[ma, pl.ds(0, FR)], f_high.at[0]),
        link("gy", 1, weight.at[ma, pl.ds(frows - FR, FR)], f_low.at[1]),
        link("gy", -1, weight.at[ma, pl.ds(0, FR)], f_high.at[1]),
    ]
    p_rows = [
        link("gy", 1, perts.at[:, :, pl.ds(rows - HB, HB), :], p_north),
        link("gy", -1, perts.at[:, :, pl.ds(0, HB), :], p_south),
    ]
    small = [
        link("gy", 1, lat_i, lat_i_low),
        link("gy", -1, lat_i, lat_i_high),
        link("gy", 1, lat_w, lat_w_low),
        link("gy", -1, lat_w, lat_w_high),
        link("gx", 1, lon_i, lon_i_west),
        link("gx", -1, lon_i, lon_i_east),
        link("gx", 1, lon_w, lon_w_west),
        link("gx", -1, lon_w, lon_w_east),
    ]
    def tilted(src, dst, side, top, bottom, first):
        pairs = []
        for step, at, to in ((1, bottom, first), (-1, top, first + HB)):
            span, there = pl.ds(at, HB), pl.ds(to, HB)
            index = (slice(None),) * (src.ndim - 2)
            pairs.append(
                link(
                    "gy",
                    step,
                    src.at[(*index, span)],
                    dst.at[(*index, there)],
                    {"gx": lax.rem(gx + side, gxn)},
                )
            )
        return pairs

    def packed(piece):
        total = None
        for l in range(levels):
            for k in range(0, GROUP, 2):
                n = (l * GROUP + k) // 2
                part = dot(lanes_of(piece(l, k), piece(l, k + 1)), pick[n])
                total = part if total is None else total + part
        return total.astype(BF16)

    a_loads = [group_load(alpha, a_tile, g, 2 + steps) for g in range(steps)]
    p_arrive = []
    def p_sides(g):
        span = pl.ds(0, rows)
        pair = [
            link("gx", 1, p_right.at[g], p_west.at[g, span]),
            link("gx", -1, p_left.at[g], p_east.at[g, span]),
        ]
        for one in pair:
            one.start()
        p_arrive.append(pair)

    for g in range(steps):
        p_loads[g].wait()
        a_loads[g].start()
        both = packed(lambda l, k: p_tile[g * GROUP + k, l])
        p_right[g] = both[:, :cols]
        p_left[g] = both[:, cols:]
        if g == 0:
            met()
            for one in small + p_rows:
                one.start()
            p_sides(g)
    corners = tilted(p_right, p_west, 1, 0, rows - HB, rows)
    corners += tilted(p_left, p_east, gxn - 1, 0, rows - HB, rows)
    for one in corners:
        one.start()
    for g in range(1, steps):
        p_sides(g)
    for one in f_rows:
        one.start()

    f_main = f_west.shape[0] - 2 * HB

    def f_fold(first, count, start):
        deep = -(-count // (FOLD * HB)) * HB
        parts = []
        for b in range(FOLD):
            stop = min(first + (b + 1) * deep, first + count)
            for i in range(2):
                part = fine_tile[i, first + b * deep : stop, start : start + FC]
                short = deep - part.shape[0]
                parts.append(rows_of(part, jnp.zeros((short, FC), F32)) if short else part)
        return lanes_of(*parts, jnp.zeros((deep, cols - 2 * FOLD * FC), F32))

    for load in f_loads:
        load.wait()
    f_arrive = []
    for step, side, src, dst, start in (
        (1, 1, f_right, f_west, fcols - FC),
        (-1, gxn - 1, f_left, f_east, 0),
    ):
        src[:f_main] = f_fold(0, frows, start)
        src[f_main : f_main + HB] = f_fold(0, FR, start)
        src[f_main + HB :] = f_fold(frows - FR, FR, start)
        span = pl.ds(0, f_main)
        f_arrive.append(link("gx", step, src.at[span], dst.at[span]))
        f_arrive += tilted(src, dst, side, f_main, f_main + HB, f_main)

    lane = iota((cols, cols), 1)
    deep = half + 2 * HB
    wide_k = lat_fore.shape[3]
    for l in range(levels):
        spread = widths[l].astype(F32)
        scale = tap_scale(spread)
        cell, at = iota((cols, cols), 0), lane
        lon_taps[l, 0], lon_taps[l, 1] = split(tap_value(cell - at, spread, scale))
        shift = at % (2 * HB)
        gap = side_cell(cell, l, cols) - jnp.where(shift < HB, cols - HB + shift, shift - HB)
        own = cell % slots // HB == at // (2 * HB)
        lon_taps[l, 2], lon_taps[l, 3] = split(jnp.where(own, tap_value(gap, spread, scale), 0.0))
        edge_taps[l, 0], edge_taps[l, 1] = split(tap_value(side_cell(at, l, cols) - cell, spread, scale))
        lat_back[l] = lat_taps(spread, scale, half, deep, -HB, wide_k)
        lat_fore[l, 0] = lat_taps(spread, scale, deep, deep, HB, wide_k)
        lat_fore[l, 1] = lat_taps(spread, scale, deep, deep, -2 * HB, wide_k)

    def tall(u, l):
        h, lo = split(u)
        out = []
        for b in range(2):
            at = slice(b * (rows - deep), b * (rows - deep) + deep)
            stack = rows_of(h[at], h[at], lo[at])
            out.append(dot(lat_fore[l, b, :, : 3 * deep], stack)[: half + HB])
        return out

    for l in range(levels):
        ext[l, HB : HB + rows, :cols] = jnp.zeros((rows, cols), F32)

    @pl.loop(0, steps)
    def _(g):
        group_load(alpha, a_tile, g, 2 + steps).wait()
        for l in range(levels):
            taps = rows_of(
                lanes_of(lon_taps[l, 0], edge_taps[l, 0]), lanes_of(lon_taps[l, 1], edge_taps[l, 1])
            )
            fields = [a_tile[g * GROUP + m, l] for m in range(GROUP)]
            u = dot(rows_of(*[lanes_of(a, a) for a in fields]), taps)
            side = u[:rows, cols:]
            for m in range(1, GROUP):
                mine = lane % slots // HB == m
                side = jnp.where(mine, u[m * rows : (m + 1) * rows, cols:], side)
            total = None
            for k in range(0, GROUP, 2):
                pair = [u[m * rows : (m + 1) * rows, :cols] for m in (k, k + 1)]
                top, bottom = tall(lanes_of(*pair), l)
                for i, m in enumerate((k, k + 1)):
                    at = slice(i * cols, (i + 1) * cols)
                    v = rows_of(top[HB:, at], bottom[:half, at])
                    part = p_tile[g * GROUP + m, l].astype(F32) * v
                    total = part if total is None else total + part
                    v_strip[g * GROUP + m, l] = rows_of(top[:HB, at], bottom[half:, at])
            ext[l, HB : HB + rows, :cols] += total
            v_side[g, l] = rows_of(*tall(side, l))

    for one in p_rows:
        one.arrive()

    for one in f_rows:
        one.arrive()
    for one in small:
        one.arrive()
    lat_at = lanes_of(lat_i[...], lat_i_low[:, frows - FR :], lat_i_high[:, :FR]).astype(F32)
    lat_by = lanes_of(lat_w[...], lat_w_low[:, frows - FR :], lat_w_high[:, :FR])
    lat_at = lat_at - (lax.axis_index("gy") * rows).astype(F32)
    lon_at = lanes_of(lon_i[...], lon_i_west[:, fcols - FC :], lon_i_east[:, :FC]).astype(F32)
    lon_by = lanes_of(lon_w[...], lon_w_west[:, fcols - FC :], lon_w_east[:, :FC])
    lon_total = float(cols * lax.axis_size("gx"))
    lon_at = lon_at - (lax.axis_index("gx") * cols).astype(F32)
    lon_at = jnp.where(
        lon_at < -64.0, lon_at + lon_total, jnp.where(lon_at >= lon_total - 64.0, lon_at - lon_total, lon_at)
    )
    f_tall, f_wide = frows + 2 * FR, fcols + 2 * FC

    def upright(at, by):
        size = at.shape[1]
        space = jnp.zeros((1, -size % 128), F32)
        at, by = lanes_of(at, space), lanes_of(by, space)
        shape = (8, at.shape[1])
        both = jnp.where(iota(shape, 0) == 0, jnp.broadcast_to(at, shape), jnp.broadcast_to(by, shape))
        both = both.T[:size]
        return both[:, 0:1], both[:, 1:2]

    lat_at_up, lat_by_up = upright(lat_at, lat_by)
    lon_at_up, lon_by_up = upright(lon_at, lon_by)
    t_rows, e_rows = rows + 2 * CR, rows + 2 * HB
    up_lat[0], up_lat[1] = split(weigh(iota((f_tall, t_rows), 1) - CR, lat_at_up, lat_by_up))
    down_lat[0], down_lat[1] = split(weigh(iota((e_rows, f_tall), 0) - HB, lat_at, lat_by))
    order = iota((2 * cols, f_wide), 0)
    w = order - cols
    wing = jnp.where(
        w < REACH,
        w - (REACH - HB),
        jnp.where(
            (w >= slots - HB) & (w < slots),
            w - slots,
            jnp.where(
                (w >= slots) & (w < slots + REACH),
                w - slots + cols - HB,
                jnp.where(w >= cols - HB, w + HB, -1000),
            ),
        ),
    )
    up_lon[0], up_lon[1] = split(weigh(jnp.where(w < 0, order, wing), lon_at, lon_by))
    order = iota((f_wide, 2 * cols), 1)
    cell = jnp.where(order < cols, order, side_cell(order - cols, ma, cols))
    down_lon[0], down_lon[1] = split(weigh(cell, lon_at_up, lon_by_up))

    for l in range(levels):

        def strips(g, sums):
            north, south = sums
            for k in range(GROUP):
                m = g * GROUP + k
                north = north + p_north[m, l].astype(F32) * v_strip[m, l, :HB]
                south = south + p_south[m, l].astype(F32) * v_strip[m, l, HB:]
            return north, south

        zero = jnp.zeros((HB, cols), F32)
        north, south = lax.fori_loop(0, steps, strips, (zero, zero))
        ext[l, :HB, :cols] = north
        ext[l, HB + rows :, :cols] = south

    for i in range(2):
        fine_wide[i, :, :fcols] = rows_of(fine_tile[i], f_low[i], f_high[i])

    thick = iota((rows, cols), 1) // slots
    thin = iota((2 * HB, cols), 1) // slots
    side_sums = [None] * levels
    for g in range(steps):
        for one in p_arrive[g]:
            one.arrive()
        for l in range(levels):
            west, east = p_west[g, :rows].astype(F32), p_east[g, :rows].astype(F32)
            part = jnp.where(thick == l, west, east) * v_side[g, l, HB : HB + rows]
            side_sums[l] = part if g == 0 else side_sums[l] + part
    for one in corners:
        one.arrive()
    t_lane, e_lane = iota((t_rows, cols), 1), iota((e_rows, cols), 1)

    def fold(x, first, deep):
        total = None
        lane_at = iota((deep, cols), 1)
        for b in range(x.shape[0] // deep):
            part = pltpu.roll(x[b * deep : (b + 1) * deep], (b * REACH - first) % cols, 1)
            total = part if total is None else jnp.where(lane_at >= b * REACH, part, total)
        return total

    def unfold(x, first, start, blocks):
        parts = [pltpu.roll(x, (first - b * REACH) % cols, 1) for b in range(start, start + blocks)]
        return rows_of(*parts)

    for l in range(levels):
        ends = None
        for g in range(steps):
            west, east = p_west[g, rows:].astype(F32), p_east[g, rows:].astype(F32)
            v = rows_of(v_side[g, l, :HB], v_side[g, l, HB + rows :])
            part = jnp.where(thin == l, west, east) * v
            ends = part if ends is None else ends + part
        side = rows_of(ends[:HB], side_sums[l], ends[HB:])
        if l:
            side = pltpu.roll(side, slots, 1)
        for shift in (HB, 2 * HB, 4 * HB):
            side = side + pltpu.roll(side, shift, 1)
        ext[l, :, cols:] = side
        core = ext[l, :, :cols]
        eastward = jnp.where(e_lane >= cols - HB, side, pltpu.roll(core, cols - HB, 1))
        westward = jnp.where(e_lane < slots, side, pltpu.roll(core, slots, 1))
        for i, (x, first) in enumerate(((eastward, cols - REACH), (westward, slots - HB))):
            flank[l, i] = fold(x, first, STRIP)
            tip[l, i] = fold(rows_of(x[e_rows - STRIP :], x[:STRIP]), first, HB)

    corner_links, side_links, end_links, swaps = [], [], [], []
    for s in range(count):
        peer = lax.rem(ma + s, count)
        for i, step in enumerate((1, -1)):
            at = {"ma": peer}
            side_links.append(link("gx", step, flank.at[peer, i], flanks.at[s, i], at))
            strip = ext.at[peer, pl.ds((e_rows - STRIP) * (1 - i), STRIP)]
            end_links.append(link("gy", step, strip, ends_in.at[s, i], at))
            at = {"gx": lax.rem(gx + step + gxn, gxn), "ma": peer}
            for j, turn in enumerate((1, -1)):
                corner_links.append(link("gy", turn, tip.at[peer, i], tips.at[s, i, j], at))
        if s:
            swaps.append(link("ma", peer - ma, ext.at[peer], other.at[s - 1]))
    sent = corner_links + side_links + end_links + swaps
    for one in sent + f_arrive:
        one.start()
    for one in sent:
        one.arrive()
    mine, strips_in, flank_in, tip_in = ext[ma], ends_in[0], flanks[0], tips[0]
    for s in range(1, count):
        mine = mine + other[s - 1]
        strips_in, flank_in, tip_in = strips_in + ends_in[s], flank_in + flanks[s], tip_in + tips[s]
    lap = CR - HB
    edge = STRIP - lap

    def merge(above, middle, below):
        return rows_of(
            above[:lap],
            middle[:edge] + above[lap:],
            middle[edge : e_rows - edge],
            middle[e_rows - edge :] + below[:edge],
            below[edge:],
        )

    mine = merge(strips_in[0], mine, strips_in[1])
    core, side = mine[:, :cols], mine[:, cols:]
    third = STRIP // HB

    def wing_from(i, first):
        return merge(
            unfold(tip_in[i, 0], first, 0, third),
            unfold(flank_in[i], first, 0, e_rows // STRIP),
            unfold(tip_in[i, 1], first, third, third),
        )

    wings = jnp.where(
        t_lane < REACH,
        wing_from(0, 0),
        jnp.where((t_lane >= slots) & (t_lane < slots + REACH), wing_from(1, slots), side),
    )
    across = dot3(split(lanes_of(core, wings)), (up_lon[0], up_lon[1]))
    fine = dot3((up_lat[0], up_lat[1]), split(across))
    increment[ma] = fine[:frows, :fcols]
    final = []

    def share(whole):
        for s in range(1, count):
            peer = lax.rem(ma + s, count)
            final.append(link("ma", peer - ma, whole.at[ma], whole.at[ma]))
            final[-1].start()

    share(increment)
    for one in f_arrive:
        one.arrive()
    for i in range(2):

        def wing_of(part):
            def opened(first, last):
                lanes = range(FC * i, 2 * FOLD * FC, 2 * FC)
                return [part[first:last, x : x + FC] for x in lanes]

            low, high = f_main, f_main + HB
            return rows_of(
                rows_of(*opened(0, low))[:frows], *opened(low, high), *opened(high, high + HB)
            )

        fine_wide[i, :, fcols:] = lanes_of(wing_of(f_west), wing_of(f_east))
    misfit = fine_wide[1] * (fine - fine_wide[0])
    across = dot3((down_lat[0], down_lat[1]), split(misfit))
    residual[ma] = dot3(split(across), (down_lon[0], down_lon[1]))
    share(residual)
    for one in final:
        one.arrive()
    for one in pending:
        one.sent()


def cost(flops, nbytes):
    return pl.CostEstimate(flops=flops, bytes_accessed=nbytes, transcendentals=0)


def core_step(widths, lat_i, lat_w, lon_i, lon_w, alpha, perts, innov, weight):
    members, levels, rows, cols = alpha.shape
    steps = members // GROUP
    frows, fcols = innov.shape[1:]
    count = lax.axis_size("ma")
    assert levels == 2 and count == levels
    assert (rows + 2 * HB) % STRIP == 0
    half = rows // 2
    deep = half + 2 * HB
    wide_k = -(-3 * deep // 128) * 128
    e_rows, t_rows = rows + 2 * HB, rows + 2 * CR
    f_tall, f_wide = frows + 2 * FR, fcols + 2 * FC
    strip = ((members, levels, HB, cols), BF16)
    side = ((steps, e_rows, cols), BF16)
    outs = [
        (innov.shape, F32),
        ((levels, e_rows, 2 * cols), F32),
        (alpha.shape, BF16),
        (alpha.shape, BF16),
        strip,
        strip,
        side,
        side,
        ((levels, 4, cols, cols), BF16),
        ((levels, half, wide_k), BF16),
    ]
    kept = sum(math.prod(shape) * jnp.dtype(kind).itemsize for shape, kind in outs)
    fine_edge = ((2, FR, fcols), F32)
    fine_side = ((-(-frows // (FOLD * HB)) * HB + 2 * HB, cols), F32)
    packed = ((steps, rows, cols), BF16)
    scratch = [
        ((2, frows, fcols), F32),
        ((levels * GROUP // 2, 2 * cols, 2 * cols), BF16),
        ((levels, 2, cols, cols), BF16),
        ((levels, 2, deep, wide_k), BF16),
        ((members, levels, 2 * HB, cols), F32),
        ((steps, levels, e_rows, cols), F32),
        packed,
        packed,
        fine_edge,
        fine_edge,
        fine_side,
        fine_side,
        fine_side,
        fine_side,
        ((2, f_tall, f_wide), F32),
        (lat_i.shape, jnp.int32),
        (lat_i.shape, jnp.int32),
        (lat_w.shape, F32),
        (lat_w.shape, F32),
        (lon_i.shape, jnp.int32),
        (lon_i.shape, jnp.int32),
        (lon_w.shape, F32),
        (lon_w.shape, F32),
        ((2, 2 * cols, f_wide), BF16),
        ((2, f_tall, t_rows), BF16),
        ((2, e_rows, f_tall), BF16),
        ((2, f_wide, 2 * cols), BF16),
        ((levels, e_rows, 2 * cols), F32),
        ((count - 1, e_rows, 2 * cols), F32),
        ((count, 2, STRIP, 2 * cols), F32),
        ((levels, 2, STRIP, cols), F32),
        ((levels, 2, HB, cols), F32),
        ((count, 2, STRIP, cols), F32),
        ((count, 2, 2, HB, cols), F32),
    ]
    vmem = pl.BlockSpec(memory_space=pltpu.VMEM)
    anywhere = pl.BlockSpec(memory_space=pltpu.HBM)
    return pl.pallas_call(
        core_kernel,
        in_specs=[pl.BlockSpec(memory_space=pltpu.SMEM)] + [vmem] * 4 + [anywhere] * 4,
        out_specs=[vmem] * len(outs),
        out_shape=[pltpu.VMEM(shape, kind) for shape, kind in outs],
        scratch_shapes=[pltpu.VMEM(shape, kind) for shape, kind in scratch]
        + [
            pltpu.SemaphoreType.DMA((96,)),
            pltpu.SemaphoreType.DMA((96,)),
            pltpu.SemaphoreType.DMA((2 + 2 * steps,)),
        ],
        compiler_params=pltpu.CompilerParams(
            collective_id=0, has_side_effects=True, vmem_limit_bytes=VMEM_BYTES - VMEM_SLACK - kept
        ),
        cost_estimate=cost(2**30, 2**24),
    )(widths, lat_i, lat_w, lon_i, lon_w, alpha, perts, innov, weight)


def band(high, low, taps):
    half = taps.shape[0]
    deep = half + 2 * HB
    out = []
    for first in range(0, high.shape[0] - 2 * HB, half):
        h, lo = high[first : first + deep], low[first : first + deep]
        out.append(dot(taps, rows_of(h, h, lo)))
    return rows_of(*out)


def adjoint_kernel(
    alpha, perts, north, south, west, east, residual, lon, lat, fine, out, fine_out, sem
):
    rows, cols = alpha.shape[2:]
    slots = GROUP * HB
    g = pl.program_id(0)
    give = pltpu.make_async_copy(fine, fine_out, sem.at[0])

    @pl.when(g == 0)
    def _():
        give.start()

    @pl.when(g == pl.num_programs(0) - 1)
    def _():
        give.wait()

    zero = jnp.zeros((cols, cols), BF16)

    def stack(high, low):
        return rows_of(lanes_of(high, low), lanes_of(high, zero))

    def halves(x):
        return x[:, :cols] + x[:, cols:]

    lane = iota((rows, cols), 1)
    inner = (lane >= HB) & (lane < cols - HB)
    wide = iota((rows + 2 * HB, cols), 1)
    for l in range(alpha.shape[1]):
        res = residual[l]
        taps = lat[l, :, : 3 * (rows // 2 + 2 * HB)]
        side = jnp.where(wide // slots == l, west[g].astype(F32), east[g].astype(F32))
        edge = band(*split(natural(side, rows) * res[:, cols:]), taps)
        edge = halves(dot(lanes_of(*split(edge)), stack(lon[l, 2], lon[l, 3])))
        cores = []
        for k in range(0, GROUP, 2):
            pairs = []
            for m in (k, k + 1):
                n = g * GROUP + m
                tall = rows_of(
                    north[n, l].astype(F32), perts[n, l].astype(F32), south[n, l].astype(F32)
                )
                pairs.append(split(tall * res[:, :cols]))
            both = band(lanes_of(pairs[0][0], pairs[1][0]), lanes_of(pairs[0][1], pairs[1][1]), taps)
            for i in range(2):
                cores.append(lanes_of(*split(both[:, i * cols : (i + 1) * cols])))
        total = dot(rows_of(*cores), stack(lon[l, 0], lon[l, 1]))
        for m in range(GROUP):
            turned = pltpu.roll(edge, (cols - HB - 2 * HB * m) % cols, 1)
            value = halves(total[m * rows : (m + 1) * rows]) + jnp.where(inner, 0.0, turned)
            out[m, l] = alpha[g * GROUP + m, l].astype(F32) + value


def adjoint(alpha, perts, north, south, west, east, residual, lon, lat, fine):
    members, levels, rows, cols = alpha.shape
    return pl.pallas_call(
        adjoint_kernel,
        grid=(members // GROUP,),
        in_specs=[pl.BlockSpec(memory_space=pltpu.VMEM)] * 10,
        out_specs=[
            pl.BlockSpec((GROUP, levels, rows, cols), lambda g: (g, 0, 0, 0)),
            pl.BlockSpec(memory_space=pltpu.HBM),
        ],
        out_shape=[
            jax.ShapeDtypeStruct(alpha.shape, F32),
            jax.ShapeDtypeStruct(fine.shape, F32),
        ],
        scratch_shapes=[pltpu.SemaphoreType.DMA((1,))],
        compiler_params=pltpu.CompilerParams(vmem_limit_bytes=BACK_LIMIT),
        cost_estimate=cost(members * levels * 2**25, alpha.size * 8),
    )(alpha, perts, north, south, west, east, residual, lon, lat, fine)


def body(
    alpha_fields,
    member_perts,
    band_widths,
    lat_index,
    lat_weight,
    lon_index,
    lon_weight,
    innovation,
    obs_weight,
):
    tables = [x.reshape(1, -1) for x in (lat_index, lat_weight, lon_index, lon_weight)]
    increment, residual, alpha, perts, *rest = core_step(
        band_widths, *tables, alpha_fields, member_perts, innovation, obs_weight
    )
    north, south, west, east, lon, lat = rest
    gradient, increment = adjoint(
        alpha, perts, north, south, west, east, residual, lon, lat, increment
    )
    return (increment, gradient)


def solution(mesh):
    placed = (
        P("ma", None, "gy", "gx"),
        P("ma", None, "gy", "gx"),
        P(),
        P("gy"),
        P("gy"),
        P("gx"),
        P("gx"),
        P(None, "gy", "gx"),
        P(None, "gy", "gx"),
    )
    return jax.shard_map(
        body,
        mesh=mesh,
        in_specs=placed,
        out_specs=(P(None, "gy", "gx"), P("ma", None, "gy", "gx")),
        check_vma=False,
    )
```

```python
import math

import jax
import jax.numpy as jnp
from jax import lax
from jax.experimental import pallas as pl
from jax.experimental.pallas import tpu as pltpu
from jax.sharding import PartitionSpec as P

HB = 8
GROUP = 8
FR = 24
FC = 20
FOLD = 3
CR = 16
STRIP = 24
REACH = HB + 10
MESH = pl.DeviceIdType.MESH
VMEM_BYTES = 67043328
VMEM_SLACK = 2**17
BACK_LIMIT = 32 * 2**20
F32 = jnp.float32
BF16 = jnp.bfloat16


def iota(shape, dim):
    return lax.broadcasted_iota(jnp.int32, shape, dim)


def dot(a, b):
    return jnp.dot(a, b, preferred_element_type=F32)


def split(value):
    high = value.astype(BF16)
    return high, (value - high.astype(F32)).astype(BF16)


def dot3(a, b):
    return dot(a[0], b[0]) + dot(a[1], b[0]) + dot(a[0], b[1])


def rows_of(*parts):
    return jnp.concatenate(parts, axis=0)


def lanes_of(*parts):
    return jnp.concatenate(parts, axis=1)


def natural(x, rows):
    return rows_of(x[rows : rows + HB], x[:rows], x[rows + HB :])


def place(order, size, width):
    return jnp.where(order < size, order, jnp.where(order < size + width, order - size - width, order - width))


def tap_value(distance, spread, scale):
    d = distance.astype(F32)
    value = jnp.exp(-(d * d) / (2.0 * spread * spread)) * scale
    return jnp.where(jnp.abs(distance) <= HB, value, 0.0)


def tap_scale(spread):
    lane = iota((8, 128), 1)
    d = (lane - HB).astype(F32)
    shape = jnp.where(lane <= 2 * HB, jnp.exp(-(d * d) / (2.0 * spread * spread)), 0.0)
    return (1.0 / jnp.sqrt(jnp.sum(shape * shape, axis=1, keepdims=True)))[:1]


def lat_taps(spread, scale, height, deep, offset, width):
    i, c = iota((height, width), 0), iota((height, width), 1)
    r = jnp.where(c >= 2 * deep, c - 2 * deep, jnp.where(c >= deep, c - deep, c))
    value = tap_value(r - i + offset, spread, scale)
    high = value.astype(BF16).astype(F32)
    return jnp.where((c >= deep) & (c < 2 * deep), value - high, high).astype(BF16)


def side_cell(lane, level, cols):
    west = lane // (GROUP * HB) == level
    return jnp.where(west, lane % HB - HB, cols + lane % HB)


def weigh(cell, index, weight):
    cell = cell.astype(F32)
    return jnp.where(cell == index, 1.0 - weight, 0.0) + jnp.where(cell == index + 1.0, weight, 0.0)


class Link:
    def __init__(self, axis, step, src, dst, send, recv, slot, also=None):
        me, count = lax.axis_index(axis), lax.axis_size(axis)
        target = me + step
        self.sends = self.gets = None
        if axis == "gx":
            target = lax.rem(target + count, count)
        elif axis == "gy":
            self.sends = (target >= 0) & (target < count)
            self.gets = (me - step >= 0) & (me - step < count)
        self.dst = dst
        device = {axis: target, **(also or {})}
        self.copy = pltpu.make_async_remote_copy(
            src_ref=src,
            dst_ref=dst,
            send_sem=send.at[slot],
            recv_sem=recv.at[slot],
            device_id=device,
            device_id_type=MESH,
        )

    def start(self):
        if self.sends is None:
            self.copy.start()
        else:
            pl.when(self.sends)(self.copy.start)

    def arrive(self):
        if self.gets is None:
            self.copy.wait_recv()
        else:
            pl.when(self.gets)(self.copy.wait_recv)

            @pl.when(jnp.logical_not(self.gets))
            def _():
                self.dst[...] = jnp.zeros_like(self.dst)

    def sent(self):
        if self.sends is None:
            self.copy.wait_send()
        else:
            pl.when(self.sends)(self.copy.wait_send)


def greet():
    barrier = pltpu.get_barrier_semaphore()
    gx, gxn = lax.axis_index("gx"), lax.axis_size("gx")
    gy, gyn = lax.axis_index("gy"), lax.axis_size("gy")
    ma, count = lax.axis_index("ma"), lax.axis_size("ma")

    def hail(device):
        pl.semaphore_signal(barrier, inc=1, device_id=device, device_id_type=MESH)

    for s in range(count):
        peer = lax.rem(ma + s, count)
        if s:
            hail({"ma": peer})
        sides = [lax.rem(gx + step, gxn) for step in (1, gxn - 1)]
        for side in sides:
            hail({"gx": side, "ma": peer})
        for step, there in ((-1, gy > 0), (1, gy < gyn - 1)):

            @pl.when(there)
            def _(step=step, peer=peer, sides=sides):
                for side in (gx, *sides):
                    hail({"gx": side, "gy": gy + step, "ma": peer})

    below, above = jnp.minimum(gy, 1), jnp.minimum(gyn - 1 - gy, 1)
    return lambda: pl.semaphore_wait(barrier, 3 * count - 1 + (below + above) * 3 * count)


def core_kernel(
    widths, lat_i, lat_w, lon_i, lon_w, alpha, perts, innov, weight,
    increment, residual, a_tile, p_tile, p_north, p_south, p_west, p_east, lon_taps, lat_back,
    fine_tile, pick, edge_taps, lat_fore, v_strip, v_side, p_right, p_left,
    f_low, f_high, f_right, f_left, f_west, f_east, fine_wide,
    lat_i_low, lat_i_high, lat_w_low, lat_w_high, lon_i_west, lon_i_east, lon_w_west, lon_w_east,
    up_lon, up_lat, down_lat, down_lon, ext, other, ends_in, flank, tip, flanks, tips,
    send, recv, local,
):
    members, levels, rows, cols = alpha.shape
    steps, half, slots = members // GROUP, rows // 2, GROUP * HB
    frows, fcols = innov.shape[1:]
    ma, count = lax.axis_index("ma"), lax.axis_size("ma")
    gx, gxn = lax.axis_index("gx"), lax.axis_size("gx")
    met = greet()
    f_loads = [
        pltpu.make_async_copy(src.at[ma], fine_tile.at[i], local.at[i])
        for i, src in enumerate((innov, weight))
    ]

    def group_load(src, dst, g, first):
        span = pl.ds(g * GROUP, GROUP)
        return pltpu.make_async_copy(src.at[span], dst.at[span], local.at[first + g])

    p_loads = [group_load(perts, p_tile, g, 2) for g in range(steps)]
    for load in p_loads + f_loads:
        load.start()
    counter = iter(range(96))
    pending = []

    def link(axis, step, src, dst, also=None):
        one = Link(axis, step, src, dst, send, recv, next(counter), also)
        pending.append(one)
        return one

    r, c = iota((cols, 2 * cols), 0), iota((cols, 2 * cols), 1)
    base = jnp.where(
        ((c < cols) & (r - (cols - HB) == c % HB)) | ((c >= cols) & (r == c % HB)), 1.0, 0.0
    )
    turned = (c % cols) // slots
    slot = jnp.where(c < cols, turned, 1 - turned) * GROUP + c % slots // HB
    for l in range(levels):
        for k in range(GROUP):
            at = slice(k % 2 * cols, (k % 2 + 1) * cols)
            n = l * GROUP + k
            pick[n // 2, at] = jnp.where(slot == n, base, 0.0).astype(BF16)
    f_rows = [
        link("gy", 1, innov.at[ma, pl.ds(frows - FR, FR)], f_low.at[0]),
        link("gy", -1, innov.at[ma, pl.ds(0, FR)], f_high.at[0]),
        link("gy", 1, weight.at[ma, pl.ds(frows - FR, FR)], f_low.at[1]),
        link("gy", -1, weight.at[ma, pl.ds(0, FR)], f_high.at[1]),
    ]
    p_rows = [
        link("gy", 1, perts.at[:, :, pl.ds(rows - HB, HB), :], p_north),
        link("gy", -1, perts.at[:, :, pl.ds(0, HB), :], p_south),
    ]
    small = [
        link("gy", 1, lat_i, lat_i_low),
        link("gy", -1, lat_i, lat_i_high),
        link("gy", 1, lat_w, lat_w_low),
        link("gy", -1, lat_w, lat_w_high),
        link("gx", 1, lon_i, lon_i_west),
        link("gx", -1, lon_i, lon_i_east),
        link("gx", 1, lon_w, lon_w_west),
        link("gx", -1, lon_w, lon_w_east),
    ]
    def tilted(src, dst, side, top, bottom, first):
        pairs = []
        for step, at, to in ((1, bottom, first), (-1, top, first + HB)):
            span, there = pl.ds(at, HB), pl.ds(to, HB)
            index = (slice(None),) * (src.ndim - 2)
            pairs.append(
                link(
                    "gy",
                    step,
                    src.at[(*index, span)],
                    dst.at[(*index, there)],
                    {"gx": lax.rem(gx + side, gxn)},
                )
            )
        return pairs

    def packed(piece):
        total = None
        for l in range(levels):
            for k in range(0, GROUP, 2):
                n = (l * GROUP + k) // 2
                part = dot(lanes_of(piece(l, k), piece(l, k + 1)), pick[n])
                total = part if total is None else total + part
        return total.astype(BF16)

    a_loads = [group_load(alpha, a_tile, g, 2 + steps) for g in range(steps)]
    p_arrive = []
    rim = STRIP - HB

    def p_sides(groups, first, deep):
        part, span = pl.ds(groups.start, groups.stop - groups.start), pl.ds(first, deep)
        pair = [
            link("gx", 1, p_right.at[part, span], p_west.at[part, span]),
            link("gx", -1, p_left.at[part, span], p_east.at[part, span]),
        ]
        for one in pair:
            one.start()
        return pair

    for g in range(steps):
        p_loads[g].wait()
        a_loads[g].start()
        both = packed(lambda l, k: p_tile[g * GROUP + k, l])
        p_right[g] = both[:, :cols]
        p_left[g] = both[:, cols:]
        if g == 0:
            met()
            for one in small + p_rows:
                one.start()
            rims = p_sides(range(1), 0, rows)
    corners = tilted(p_right, p_west, 1, 0, rows - HB, rows)
    corners += tilted(p_left, p_east, gxn - 1, 0, rows - HB, rows)
    for first in (0, rows - rim):
        rims += p_sides(range(1, steps), first, rim)
    for one in corners:
        one.start()
    rims += corners
    for g in range(1, steps):
        p_arrive.append(p_sides(range(g, g + 1), rim, rows - 2 * rim))
    for one in f_rows:
        one.start()

    f_main = f_west.shape[0] - 2 * HB

    def f_fold(first, count, start):
        deep = -(-count // (FOLD * HB)) * HB
        parts = []
        for b in range(FOLD):
            stop = min(first + (b + 1) * deep, first + count)
            for i in range(2):
                part = fine_tile[i, first + b * deep : stop, start : start + FC]
                short = deep - part.shape[0]
                parts.append(rows_of(part, jnp.zeros((short, FC), F32)) if short else part)
        return lanes_of(*parts, jnp.zeros((deep, cols - 2 * FOLD * FC), F32))

    for load in f_loads:
        load.wait()
    f_arrive = []
    for step, side, src, dst, start in (
        (1, 1, f_right, f_west, fcols - FC),
        (-1, gxn - 1, f_left, f_east, 0),
    ):
        src[:f_main] = f_fold(0, frows, start)
        src[f_main : f_main + HB] = f_fold(0, FR, start)
        src[f_main + HB :] = f_fold(frows - FR, FR, start)
        span = pl.ds(0, f_main)
        f_arrive.append(link("gx", step, src.at[span], dst.at[span]))
        f_arrive += tilted(src, dst, side, f_main, f_main + HB, f_main)

    lane = iota((cols, cols), 1)
    deep = half + 2 * HB
    wide_k = lat_fore.shape[3]
    for l in range(levels):
        spread = widths[l].astype(F32)
        scale = tap_scale(spread)
        cell, at = iota((cols, cols), 0), lane
        lon_taps[l, 0], lon_taps[l, 1] = split(tap_value(cell - at, spread, scale))
        shift = at % (2 * HB)
        gap = side_cell(cell, l, cols) - jnp.where(shift < HB, cols - HB + shift, shift - HB)
        own = cell % slots // HB == at // (2 * HB)
        lon_taps[l, 2], lon_taps[l, 3] = split(jnp.where(own, tap_value(gap, spread, scale), 0.0))
        edge_taps[l, 0], edge_taps[l, 1] = split(tap_value(side_cell(at, l, cols) - cell, spread, scale))
        lat_back[l] = lat_taps(spread, scale, half, deep, -HB, wide_k)
        lat_fore[l, 0] = lat_taps(spread, scale, deep, deep, HB, wide_k)
        lat_fore[l, 1] = lat_taps(spread, scale, deep, deep, -2 * HB, wide_k)

    def tall(u, l):
        h, lo = split(u)
        out = []
        for b in range(2):
            at = slice(b * (rows - deep), b * (rows - deep) + deep)
            stack = rows_of(h[at], h[at], lo[at])
            out.append(dot(lat_fore[l, b, :, : 3 * deep], stack)[: half + HB])
        return out

    for l in range(levels):
        ext[l, HB : HB + rows, :cols] = jnp.zeros((rows, cols), F32)

    @pl.loop(0, steps)
    def _(g):
        group_load(alpha, a_tile, g, 2 + steps).wait()
        for l in range(levels):
            taps = rows_of(
                lanes_of(lon_taps[l, 0], edge_taps[l, 0]), lanes_of(lon_taps[l, 1], edge_taps[l, 1])
            )
            fields = [a_tile[g * GROUP + m, l] for m in range(GROUP)]
            u = dot(rows_of(*[lanes_of(a, a) for a in fields]), taps)
            side = u[:rows, cols:]
            for m in range(1, GROUP):
                mine = lane % slots // HB == m
                side = jnp.where(mine, u[m * rows : (m + 1) * rows, cols:], side)
            total = None
            for k in range(0, GROUP, 2):
                pair = [u[m * rows : (m + 1) * rows, :cols] for m in (k, k + 1)]
                top, bottom = tall(lanes_of(*pair), l)
                for i, m in enumerate((k, k + 1)):
                    at = slice(i * cols, (i + 1) * cols)
                    v = rows_of(top[HB:, at], bottom[:half, at])
                    part = p_tile[g * GROUP + m, l].astype(F32) * v
                    total = part if total is None else total + part
                    v_strip[g * GROUP + m, l] = rows_of(top[:HB, at], bottom[half:, at])
            ext[l, HB : HB + rows, :cols] += total
            v_side[g, l] = rows_of(*tall(side, l))

    for one in p_rows:
        one.arrive()

    for one in f_rows:
        one.arrive()
    for one in small:
        one.arrive()
    lat_at = lanes_of(lat_i[...], lat_i_low[:, frows - FR :], lat_i_high[:, :FR]).astype(F32)
    lat_by = lanes_of(lat_w[...], lat_w_low[:, frows - FR :], lat_w_high[:, :FR])
    lat_at = lat_at - (lax.axis_index("gy") * rows).astype(F32)
    lon_at = lanes_of(lon_i[...], lon_i_west[:, fcols - FC :], lon_i_east[:, :FC]).astype(F32)
    lon_by = lanes_of(lon_w[...], lon_w_west[:, fcols - FC :], lon_w_east[:, :FC])
    lon_total = float(cols * lax.axis_size("gx"))
    lon_at = lon_at - (lax.axis_index("gx") * cols).astype(F32)
    lon_at = jnp.where(
        lon_at < -64.0, lon_at + lon_total, jnp.where(lon_at >= lon_total - 64.0, lon_at - lon_total, lon_at)
    )
    f_tall, f_wide = frows + 2 * FR, fcols + 2 * FC

    def upright(at, by):
        size = at.shape[1]
        space = jnp.zeros((1, -size % 128), F32)
        at, by = lanes_of(at, space), lanes_of(by, space)
        shape = (8, at.shape[1])
        both = jnp.where(iota(shape, 0) == 0, jnp.broadcast_to(at, shape), jnp.broadcast_to(by, shape))
        both = both.T[:size]
        return both[:, 0:1], both[:, 1:2]

    lat_at_up, lat_by_up = upright(lat_at, lat_by)
    lon_at_up, lon_by_up = upright(lon_at, lon_by)
    t_rows, e_rows = rows + 2 * CR, rows + 2 * HB
    up_lat[0], up_lat[1] = split(weigh(iota((f_tall, t_rows), 1) - CR, lat_at_up, lat_by_up))
    down_lat[0], down_lat[1] = split(weigh(iota((e_rows, f_tall), 0) - HB, lat_at, lat_by))
    order = iota((2 * cols, f_wide), 0)
    w = order - cols
    wing = jnp.where(
        w < REACH,
        w - (REACH - HB),
        jnp.where(
            (w >= slots - HB) & (w < slots),
            w - slots,
            jnp.where(
                (w >= slots) & (w < slots + REACH),
                w - slots + cols - HB,
                jnp.where(w >= cols - HB, w + HB, -1000),
            ),
        ),
    )
    up_lon[0], up_lon[1] = split(weigh(jnp.where(w < 0, order, wing), lon_at, lon_by))
    order = iota((f_wide, 2 * cols), 1)
    cell = jnp.where(order < cols, order, side_cell(order - cols, ma, cols))
    down_lon[0], down_lon[1] = split(weigh(cell, lon_at_up, lon_by_up))

    for l in range(levels):

        def strips(g, sums):
            north, south = sums
            for k in range(GROUP):
                m = g * GROUP + k
                north = north + p_north[m, l].astype(F32) * v_strip[m, l, :HB]
                south = south + p_south[m, l].astype(F32) * v_strip[m, l, HB:]
            return north, south

        zero = jnp.zeros((HB, cols), F32)
        north, south = lax.fori_loop(0, steps, strips, (zero, zero))
        ext[l, :HB, :cols] = north
        ext[l, HB + rows :, :cols] = south

    for i in range(2):
        fine_wide[i, :, :fcols] = rows_of(fine_tile[i], f_low[i], f_high[i])

    t_lane = iota((t_rows, cols), 1)

    def fold(x, first, deep):
        total = None
        lane_at = iota((deep, cols), 1)
        for b in range(x.shape[0] // deep):
            part = pltpu.roll(x[b * deep : (b + 1) * deep], (b * REACH - first) % cols, 1)
            total = part if total is None else jnp.where(lane_at >= b * REACH, part, total)
        return total

    def unfold(x, first, start, blocks):
        parts = [pltpu.roll(x, (first - b * REACH) % cols, 1) for b in range(start, start + blocks)]
        return rows_of(*parts)

    def side_sum(total, l):
        if l:
            total = pltpu.roll(total, slots, 1)
        for shift in (HB, 2 * HB, 4 * HB):
            total = total + pltpu.roll(total, shift, 1)
        return total

    def products(l, g, take, v):
        west, east = take(p_west.at[g]).astype(F32), take(p_east.at[g]).astype(F32)
        return jnp.where(iota(west.shape, 1) // slots == l, west, east) * v

    def outward(core, side):
        lane_at = iota(side.shape, 1)
        eastward = jnp.where(lane_at >= cols - HB, side, pltpu.roll(core, cols - HB, 1))
        westward = jnp.where(lane_at < slots, side, pltpu.roll(core, slots, 1))
        return (eastward, cols - REACH), (westward, slots - HB)

    def rim_of(part):
        far = part[rows:].astype(F32)
        near = [part[:rim].astype(F32), part[rows - rim : rows].astype(F32)]
        return rows_of(far[:HB], *near, far[HB:])

    for one in rims:
        one.arrive()
    for l in range(levels):
        total = None
        for g in range(steps):
            v = rows_of(v_side[g, l, :STRIP], v_side[g, l, e_rows - STRIP :])
            part = products(l, g, rim_of, v)
            total = part if total is None else total + part
        total = side_sum(total, l)
        ext[l, :STRIP, cols:] = total[:STRIP]
        ext[l, e_rows - STRIP :, cols:] = total[STRIP:]
        core = rows_of(ext[l, :STRIP, :cols], ext[l, e_rows - STRIP :, :cols])
        for i, (x, first) in enumerate(outward(core, total)):
            tip[l, i] = fold(rows_of(x[STRIP:], x[:STRIP]), first, HB)

    corner_links, side_links, end_links, swaps = [], [], [], []
    for s in range(count):
        peer = lax.rem(ma + s, count)
        for i, step in enumerate((1, -1)):
            at = {"ma": peer}
            side_links.append(link("gx", step, flank.at[peer, i], flanks.at[s, i], at))
            strip = ext.at[peer, pl.ds((e_rows - STRIP) * (1 - i), STRIP)]
            end_links.append(link("gy", step, strip, ends_in.at[s, i], at))
            at = {"gx": lax.rem(gx + step + gxn, gxn), "ma": peer}
            for j, turn in enumerate((1, -1)):
                corner_links.append(link("gy", turn, tip.at[peer, i], tips.at[s, i, j], at))
        if s:
            swaps.append(link("ma", peer - ma, ext.at[peer], other.at[s - 1]))
    for one in corner_links + end_links:
        one.start()
    inside = slice(STRIP, e_rows - STRIP)
    side_sums = [None] * levels
    for g in range(steps):
        if g:
            for one in p_arrive[g - 1]:
                one.arrive()
        for l in range(levels):
            part = products(l, g, lambda x: x[rim : rows - rim], v_side[g, l, inside])
            side_sums[l] = part if g == 0 else side_sums[l] + part
    for l in range(levels):
        ext[l, inside, cols:] = side_sum(side_sums[l], l)
        for i, (x, first) in enumerate(outward(ext[l, :, :cols], ext[l, :, cols:])):
            flank[l, i] = fold(x, first, STRIP)
    sent = corner_links + end_links + side_links + swaps
    late = side_links + swaps + f_arrive
    for one in late:
        one.start()
    for one in pending:
        if one not in late:
            one.sent()
    for one in sent:
        one.arrive()
    mine, strips_in, flank_in, tip_in = ext[ma], ends_in[0], flanks[0], tips[0]
    for s in range(1, count):
        mine = mine + other[s - 1]
        strips_in, flank_in, tip_in = strips_in + ends_in[s], flank_in + flanks[s], tip_in + tips[s]
    lap = CR - HB
    edge = STRIP - lap

    def merge(above, middle, below):
        return rows_of(
            above[:lap],
            middle[:edge] + above[lap:],
            middle[edge : e_rows - edge],
            middle[e_rows - edge :] + below[:edge],
            below[edge:],
        )

    mine = merge(strips_in[0], mine, strips_in[1])
    core, side = mine[:, :cols], mine[:, cols:]
    third = STRIP // HB

    def wing_from(i, first):
        return merge(
            unfold(tip_in[i, 0], first, 0, third),
            unfold(flank_in[i], first, 0, e_rows // STRIP),
            unfold(tip_in[i, 1], first, third, third),
        )

    wings = jnp.where(
        t_lane < REACH,
        wing_from(0, 0),
        jnp.where((t_lane >= slots) & (t_lane < slots + REACH), wing_from(1, slots), side),
    )
    across = dot3(split(lanes_of(core, wings)), (up_lon[0], up_lon[1]))
    fine = dot3((up_lat[0], up_lat[1]), split(across))
    increment[ma] = fine[:frows, :fcols]
    final = []

    def share(whole):
        for s in range(1, count):
            peer = lax.rem(ma + s, count)
            final.append(link("ma", peer - ma, whole.at[ma], whole.at[ma]))
            final[-1].start()

    share(increment)
    for one in f_arrive:
        one.arrive()
    for i in range(2):

        def wing_of(part):
            def opened(first, last):
                lanes = range(FC * i, 2 * FOLD * FC, 2 * FC)
                return [part[first:last, x : x + FC] for x in lanes]

            low, high = f_main, f_main + HB
            return rows_of(
                rows_of(*opened(0, low))[:frows], *opened(low, high), *opened(high, high + HB)
            )

        fine_wide[i, :, fcols:] = lanes_of(wing_of(f_west), wing_of(f_east))
    misfit = fine_wide[1] * (fine - fine_wide[0])
    across = dot3((down_lat[0], down_lat[1]), split(misfit))
    residual[ma] = dot3(split(across), (down_lon[0], down_lon[1]))
    share(residual)
    for one in late:
        one.sent()
    for one in final:
        one.arrive()
    for one in final:
        one.sent()


def cost(flops, nbytes):
    return pl.CostEstimate(flops=flops, bytes_accessed=nbytes, transcendentals=0)


def core_step(widths, lat_i, lat_w, lon_i, lon_w, alpha, perts, innov, weight):
    members, levels, rows, cols = alpha.shape
    steps = members // GROUP
    frows, fcols = innov.shape[1:]
    count = lax.axis_size("ma")
    assert levels == 2 and count == levels
    assert (rows + 2 * HB) % STRIP == 0
    half = rows // 2
    deep = half + 2 * HB
    wide_k = -(-3 * deep // 128) * 128
    e_rows, t_rows = rows + 2 * HB, rows + 2 * CR
    f_tall, f_wide = frows + 2 * FR, fcols + 2 * FC
    strip = ((members, levels, HB, cols), BF16)
    side = ((steps, e_rows, cols), BF16)
    outs = [
        (innov.shape, F32),
        ((levels, e_rows, 2 * cols), F32),
        (alpha.shape, BF16),
        (alpha.shape, BF16),
        strip,
        strip,
        side,
        side,
        ((levels, 4, cols, cols), BF16),
        ((levels, half, wide_k), BF16),
    ]
    kept = sum(math.prod(shape) * jnp.dtype(kind).itemsize for shape, kind in outs)
    fine_edge = ((2, FR, fcols), F32)
    fine_side = ((-(-frows // (FOLD * HB)) * HB + 2 * HB, cols), F32)
    packed = ((steps, rows, cols), BF16)
    scratch = [
        ((2, frows, fcols), F32),
        ((levels * GROUP // 2, 2 * cols, 2 * cols), BF16),
        ((levels, 2, cols, cols), BF16),
        ((levels, 2, deep, wide_k), BF16),
        ((members, levels, 2 * HB, cols), F32),
        ((steps, levels, e_rows, cols), F32),
        packed,
        packed,
        fine_edge,
        fine_edge,
        fine_side,
        fine_side,
        fine_side,
        fine_side,
        ((2, f_tall, f_wide), F32),
        (lat_i.shape, jnp.int32),
        (lat_i.shape, jnp.int32),
        (lat_w.shape, F32),
        (lat_w.shape, F32),
        (lon_i.shape, jnp.int32),
        (lon_i.shape, jnp.int32),
        (lon_w.shape, F32),
        (lon_w.shape, F32),
        ((2, 2 * cols, f_wide), BF16),
        ((2, f_tall, t_rows), BF16),
        ((2, e_rows, f_tall), BF16),
        ((2, f_wide, 2 * cols), BF16),
        ((levels, e_rows, 2 * cols), F32),
        ((count - 1, e_rows, 2 * cols), F32),
        ((count, 2, STRIP, 2 * cols), F32),
        ((levels, 2, STRIP, cols), F32),
        ((levels, 2, HB, cols), F32),
        ((count, 2, STRIP, cols), F32),
        ((count, 2, 2, HB, cols), F32),
    ]
    vmem = pl.BlockSpec(memory_space=pltpu.VMEM)
    anywhere = pl.BlockSpec(memory_space=pltpu.HBM)
    return pl.pallas_call(
        core_kernel,
        in_specs=[pl.BlockSpec(memory_space=pltpu.SMEM)] + [vmem] * 4 + [anywhere] * 4,
        out_specs=[vmem] * len(outs),
        out_shape=[pltpu.VMEM(shape, kind) for shape, kind in outs],
        scratch_shapes=[pltpu.VMEM(shape, kind) for shape, kind in scratch]
        + [
            pltpu.SemaphoreType.DMA((96,)),
            pltpu.SemaphoreType.DMA((96,)),
            pltpu.SemaphoreType.DMA((2 + 2 * steps,)),
        ],
        compiler_params=pltpu.CompilerParams(
            collective_id=0, has_side_effects=True, vmem_limit_bytes=VMEM_BYTES - VMEM_SLACK - kept
        ),
        cost_estimate=cost(2**30, 2**24),
    )(widths, lat_i, lat_w, lon_i, lon_w, alpha, perts, innov, weight)


def band(high, low, taps):
    half = taps.shape[0]
    deep = half + 2 * HB
    out = []
    for first in range(0, high.shape[0] - 2 * HB, half):
        h, lo = high[first : first + deep], low[first : first + deep]
        out.append(dot(taps, rows_of(h, h, lo)))
    return rows_of(*out)


def adjoint_kernel(
    alpha, perts, north, south, west, east, residual, lon, lat, fine, out, fine_out, sem
):
    rows, cols = alpha.shape[2:]
    slots = GROUP * HB
    g = pl.program_id(0)
    give = pltpu.make_async_copy(fine, fine_out, sem.at[0])

    @pl.when(g == 0)
    def _():
        give.start()

    @pl.when(g == pl.num_programs(0) - 1)
    def _():
        give.wait()

    zero = jnp.zeros((cols, cols), BF16)

    def stack(high, low):
        return rows_of(lanes_of(high, low), lanes_of(high, zero))

    def halves(x):
        return x[:, :cols] + x[:, cols:]

    lane = iota((rows, cols), 1)
    inner = (lane >= HB) & (lane < cols - HB)
    wide = iota((rows + 2 * HB, cols), 1)
    for l in range(alpha.shape[1]):
        res = residual[l]
        taps = lat[l, :, : 3 * (rows // 2 + 2 * HB)]
        side = jnp.where(wide // slots == l, west[g].astype(F32), east[g].astype(F32))
        edge = band(*split(natural(side, rows) * res[:, cols:]), taps)
        edge = halves(dot(lanes_of(*split(edge)), stack(lon[l, 2], lon[l, 3])))
        cores = []
        for k in range(0, GROUP, 2):
            pairs = []
            for m in (k, k + 1):
                n = g * GROUP + m
                tall = rows_of(
                    north[n, l].astype(F32), perts[n, l].astype(F32), south[n, l].astype(F32)
                )
                pairs.append(split(tall * res[:, :cols]))
            both = band(lanes_of(pairs[0][0], pairs[1][0]), lanes_of(pairs[0][1], pairs[1][1]), taps)
            for i in range(2):
                cores.append(lanes_of(*split(both[:, i * cols : (i + 1) * cols])))
        total = dot(rows_of(*cores), stack(lon[l, 0], lon[l, 1]))
        for m in range(GROUP):
            turned = pltpu.roll(edge, (cols - HB - 2 * HB * m) % cols, 1)
            value = halves(total[m * rows : (m + 1) * rows]) + jnp.where(inner, 0.0, turned)
            out[m, l] = alpha[g * GROUP + m, l].astype(F32) + value


def adjoint(alpha, perts, north, south, west, east, residual, lon, lat, fine):
    members, levels, rows, cols = alpha.shape
    return pl.pallas_call(
        adjoint_kernel,
        grid=(members // GROUP,),
        in_specs=[pl.BlockSpec(memory_space=pltpu.VMEM)] * 10,
        out_specs=[
            pl.BlockSpec((GROUP, levels, rows, cols), lambda g: (g, 0, 0, 0)),
            pl.BlockSpec(memory_space=pltpu.HBM),
        ],
        out_shape=[
            jax.ShapeDtypeStruct(alpha.shape, F32),
            jax.ShapeDtypeStruct(fine.shape, F32),
        ],
        scratch_shapes=[pltpu.SemaphoreType.DMA((1,))],
        compiler_params=pltpu.CompilerParams(vmem_limit_bytes=BACK_LIMIT),
        cost_estimate=cost(members * levels * 2**25, alpha.size * 8),
    )(alpha, perts, north, south, west, east, residual, lon, lat, fine)


def body(
    alpha_fields,
    member_perts,
    band_widths,
    lat_index,
    lat_weight,
    lon_index,
    lon_weight,
    innovation,
    obs_weight,
):
    tables = [x.reshape(1, -1) for x in (lat_index, lat_weight, lon_index, lon_weight)]
    increment, residual, alpha, perts, *rest = core_step(
        band_widths, *tables, alpha_fields, member_perts, innovation, obs_weight
    )
    north, south, west, east, lon, lat = rest
    gradient, increment = adjoint(
        alpha, perts, north, south, west, east, residual, lon, lat, increment
    )
    return (increment, gradient)


def solution(mesh):
    placed = (
        P("ma", None, "gy", "gx"),
        P("ma", None, "gy", "gx"),
        P(),
        P("gy"),
        P("gy"),
        P("gx"),
        P("gx"),
        P(None, "gy", "gx"),
        P(None, "gy", "gx"),
    )
    return jax.shard_map(
        body,
        mesh=mesh,
        in_specs=placed,
        out_specs=(P(None, "gy", "gx"), P("ma", None, "gy", "gx")),
        check_vma=False,
    )
```

```python
import math

import jax
import jax.numpy as jnp
from jax import lax
from jax.experimental import pallas as pl
from jax.experimental.pallas import tpu as pltpu
from jax.sharding import PartitionSpec as P

HB = 8
GROUP = 8
FR = 24
FC = 20
FOLD = 3
CR = 16
STRIP = 24
REACH = HB + 10
MESH = pl.DeviceIdType.MESH
VMEM_BYTES = 67043328
VMEM_SLACK = 2**17
BACK_LIMIT = 32 * 2**20
F32 = jnp.float32
BF16 = jnp.bfloat16


def iota(shape, dim):
    return lax.broadcasted_iota(jnp.int32, shape, dim)


def dot(a, b):
    return jnp.dot(a, b, preferred_element_type=F32)


def split(value):
    high = value.astype(BF16)
    return high, (value - high.astype(F32)).astype(BF16)


def dot3(a, b):
    return dot(a[0], b[0]) + dot(a[1], b[0]) + dot(a[0], b[1])


def rows_of(*parts):
    return jnp.concatenate(parts, axis=0)


def lanes_of(*parts):
    return jnp.concatenate(parts, axis=1)


def natural(x, rows):
    return rows_of(x[rows : rows + HB], x[:rows], x[rows + HB :])


def place(order, size, width):
    return jnp.where(order < size, order, jnp.where(order < size + width, order - size - width, order - width))


def tap_value(distance, spread, scale):
    d = distance.astype(F32)
    value = jnp.exp(-(d * d) / (2.0 * spread * spread)) * scale
    return jnp.where(jnp.abs(distance) <= HB, value, 0.0)


def tap_scale(spread):
    lane = iota((8, 128), 1)
    d = (lane - HB).astype(F32)
    shape = jnp.where(lane <= 2 * HB, jnp.exp(-(d * d) / (2.0 * spread * spread)), 0.0)
    return (1.0 / jnp.sqrt(jnp.sum(shape * shape, axis=1, keepdims=True)))[:1]


def lat_taps(spread, scale, height, deep, offset, width):
    i, c = iota((height, width), 0), iota((height, width), 1)
    r = jnp.where(c >= 2 * deep, c - 2 * deep, jnp.where(c >= deep, c - deep, c))
    value = tap_value(r - i + offset, spread, scale)
    high = value.astype(BF16).astype(F32)
    return jnp.where((c >= deep) & (c < 2 * deep), value - high, high).astype(BF16)


def side_cell(lane, level, cols):
    west = lane // (GROUP * HB) == level
    return jnp.where(west, lane % HB - HB, cols + lane % HB)


def weigh(cell, index, weight):
    cell = cell.astype(F32)
    return jnp.where(cell == index, 1.0 - weight, 0.0) + jnp.where(cell == index + 1.0, weight, 0.0)


class Link:
    def __init__(self, axis, step, src, dst, send, recv, slot, also=None):
        me, count = lax.axis_index(axis), lax.axis_size(axis)
        target = me + step
        self.sends = self.gets = None
        if axis == "gx":
            target = lax.rem(target + count, count)
        elif axis == "gy":
            self.sends = (target >= 0) & (target < count)
            self.gets = (me - step >= 0) & (me - step < count)
        self.dst = dst
        device = {axis: target, **(also or {})}
        self.copy = pltpu.make_async_remote_copy(
            src_ref=src,
            dst_ref=dst,
            send_sem=send.at[slot],
            recv_sem=recv.at[slot],
            device_id=device,
            device_id_type=MESH,
        )

    def start(self):
        if self.sends is None:
            self.copy.start()
        else:
            pl.when(self.sends)(self.copy.start)

    def arrive(self):
        if self.gets is None:
            self.copy.wait_recv()
        else:
            pl.when(self.gets)(self.copy.wait_recv)

            @pl.when(jnp.logical_not(self.gets))
            def _():
                self.dst[...] = jnp.zeros_like(self.dst)

    def sent(self):
        if self.sends is None:
            self.copy.wait_send()
        else:
            pl.when(self.sends)(self.copy.wait_send)


def greet():
    barrier = pltpu.get_barrier_semaphore()
    gx, gxn = lax.axis_index("gx"), lax.axis_size("gx")
    gy, gyn = lax.axis_index("gy"), lax.axis_size("gy")
    ma, count = lax.axis_index("ma"), lax.axis_size("ma")

    def hail(device):
        pl.semaphore_signal(barrier, inc=1, device_id=device, device_id_type=MESH)

    for s in range(count):
        peer = lax.rem(ma + s, count)
        if s:
            hail({"ma": peer})
        sides = [lax.rem(gx + step, gxn) for step in (1, gxn - 1)]
        for side in sides:
            hail({"gx": side, "ma": peer})
        for step, there in ((-1, gy > 0), (1, gy < gyn - 1)):

            @pl.when(there)
            def _(step=step, peer=peer, sides=sides):
                for side in (gx, *sides):
                    hail({"gx": side, "gy": gy + step, "ma": peer})

    below, above = jnp.minimum(gy, 1), jnp.minimum(gyn - 1 - gy, 1)
    return lambda: pl.semaphore_wait(barrier, 3 * count - 1 + (below + above) * 3 * count)


def core_kernel(
    widths_in, lat_i_in, lat_w_in, lon_i_in, lon_w_in, alpha, perts, innov, weight,
    increment, residual, a_tile, p_tile, p_north, p_south, p_west, p_east, lon_taps, lat_back,
    widths, lat_i, lat_w, lon_i, lon_w, fine_tile, pick, edge_taps, lat_fore, v_strip, v_side, p_right, p_left,
    f_low, f_high, f_right, f_left, f_west, f_east, fine_wide,
    lat_i_low, lat_i_high, lat_w_low, lat_w_high, lon_i_west, lon_i_east, lon_w_west, lon_w_east,
    up_lon, up_lat, down_lat, down_lon, ext, other, ends_in, flank, tip, flanks, tips,
    send, recv, local,
):
    members, levels, rows, cols = alpha.shape
    steps, half, slots = members // GROUP, rows // 2, GROUP * HB
    frows, fcols = innov.shape[1:]
    ma, count = lax.axis_index("ma"), lax.axis_size("ma")
    gx, gxn = lax.axis_index("gx"), lax.axis_size("gx")
    met = greet()
    tables = ((widths_in, widths), (lat_i_in, lat_i), (lat_w_in, lat_w), (lon_i_in, lon_i), (lon_w_in, lon_w))
    t_loads = [
        pltpu.make_async_copy(src, dst, local.at[2 + 2 * steps + i])
        for i, (src, dst) in enumerate(tables)
    ]
    for load in t_loads:
        load.start()
    f_loads = [
        pltpu.make_async_copy(src.at[ma], fine_tile.at[i], local.at[i])
        for i, src in enumerate((innov, weight))
    ]

    def group_load(src, dst, g, first):
        span = pl.ds(g * GROUP, GROUP)
        return pltpu.make_async_copy(src.at[span], dst.at[span], local.at[first + g])

    p_loads = [group_load(perts, p_tile, g, 2) for g in range(steps)]
    for load in p_loads + f_loads:
        load.start()
    counter = iter(range(96))
    pending = []

    def link(axis, step, src, dst, also=None):
        one = Link(axis, step, src, dst, send, recv, next(counter), also)
        pending.append(one)
        return one

    r, c = iota((cols, 2 * cols), 0), iota((cols, 2 * cols), 1)
    base = jnp.where(
        ((c < cols) & (r - (cols - HB) == c % HB)) | ((c >= cols) & (r == c % HB)), 1.0, 0.0
    )
    turned = (c % cols) // slots
    slot = jnp.where(c < cols, turned, 1 - turned) * GROUP + c % slots // HB
    for l in range(levels):
        for k in range(GROUP):
            at = slice(k % 2 * cols, (k % 2 + 1) * cols)
            n = l * GROUP + k
            pick[n // 2, at] = jnp.where(slot == n, base, 0.0).astype(BF16)
    f_rows = [
        link("gy", 1, innov.at[ma, pl.ds(frows - FR, FR)], f_low.at[0]),
        link("gy", -1, innov.at[ma, pl.ds(0, FR)], f_high.at[0]),
        link("gy", 1, weight.at[ma, pl.ds(frows - FR, FR)], f_low.at[1]),
        link("gy", -1, weight.at[ma, pl.ds(0, FR)], f_high.at[1]),
    ]
    p_rows = [
        link("gy", 1, perts.at[:, :, pl.ds(rows - HB, HB), :], p_north),
        link("gy", -1, perts.at[:, :, pl.ds(0, HB), :], p_south),
    ]
    small = [
        link("gy", 1, lat_i, lat_i_low),
        link("gy", -1, lat_i, lat_i_high),
        link("gy", 1, lat_w, lat_w_low),
        link("gy", -1, lat_w, lat_w_high),
        link("gx", 1, lon_i, lon_i_west),
        link("gx", -1, lon_i, lon_i_east),
        link("gx", 1, lon_w, lon_w_west),
        link("gx", -1, lon_w, lon_w_east),
    ]
    def tilted(src, dst, side, top, bottom, first):
        pairs = []
        for step, at, to in ((1, bottom, first), (-1, top, first + HB)):
            span, there = pl.ds(at, HB), pl.ds(to, HB)
            index = (slice(None),) * (src.ndim - 2)
            pairs.append(
                link(
                    "gy",
                    step,
                    src.at[(*index, span)],
                    dst.at[(*index, there)],
                    {"gx": lax.rem(gx + side, gxn)},
                )
            )
        return pairs

    def packed(piece):
        total = None
        for l in range(levels):
            for k in range(0, GROUP, 2):
                n = (l * GROUP + k) // 2
                part = dot(lanes_of(piece(l, k), piece(l, k + 1)), pick[n])
                total = part if total is None else total + part
        return total.astype(BF16)

    a_loads = [group_load(alpha, a_tile, g, 2 + steps) for g in range(steps)]
    p_arrive = []
    rim = STRIP - HB

    def p_sides(groups, first, deep):
        part, span = pl.ds(groups.start, groups.stop - groups.start), pl.ds(first, deep)
        pair = [
            link("gx", 1, p_right.at[part, span], p_west.at[part, span]),
            link("gx", -1, p_left.at[part, span], p_east.at[part, span]),
        ]
        for one in pair:
            one.start()
        return pair

    for g in range(steps):
        p_loads[g].wait()
        a_loads[g].start()
        both = packed(lambda l, k: p_tile[g * GROUP + k, l])
        p_right[g] = both[:, :cols]
        p_left[g] = both[:, cols:]
        if g == 0:
            for load in t_loads:
                load.wait()
            met()
            for one in small + p_rows:
                one.start()
            rims = p_sides(range(1), 0, rows)
    corners = tilted(p_right, p_west, 1, 0, rows - HB, rows)
    corners += tilted(p_left, p_east, gxn - 1, 0, rows - HB, rows)
    for first in (0, rows - rim):
        rims += p_sides(range(1, steps), first, rim)
    for one in corners:
        one.start()
    rims += corners
    for g in range(1, steps):
        p_arrive.append(p_sides(range(g, g + 1), rim, rows - 2 * rim))
    for one in f_rows:
        one.start()

    f_main = f_west.shape[0] - 2 * HB

    def f_fold(first, count, start):
        deep = -(-count // (FOLD * HB)) * HB
        parts = []
        for b in range(FOLD):
            stop = min(first + (b + 1) * deep, first + count)
            for i in range(2):
                part = fine_tile[i, first + b * deep : stop, start : start + FC]
                short = deep - part.shape[0]
                parts.append(rows_of(part, jnp.zeros((short, FC), F32)) if short else part)
        return lanes_of(*parts, jnp.zeros((deep, cols - 2 * FOLD * FC), F32))

    for load in f_loads:
        load.wait()
    f_arrive = []
    for step, side, src, dst, start in (
        (1, 1, f_right, f_west, fcols - FC),
        (-1, gxn - 1, f_left, f_east, 0),
    ):
        src[:f_main] = f_fold(0, frows, start)
        src[f_main : f_main + HB] = f_fold(0, FR, start)
        src[f_main + HB :] = f_fold(frows - FR, FR, start)
        span = pl.ds(0, f_main)
        f_arrive.append(link("gx", step, src.at[span], dst.at[span]))
        f_arrive += tilted(src, dst, side, f_main, f_main + HB, f_main)

    lane = iota((cols, cols), 1)
    deep = half + 2 * HB
    wide_k = lat_fore.shape[3]
    for l in range(levels):
        spread = widths[l].astype(F32)
        scale = tap_scale(spread)
        cell, at = iota((cols, cols), 0), lane
        lon_taps[l, 0], lon_taps[l, 1] = split(tap_value(cell - at, spread, scale))
        shift = at % (2 * HB)
        gap = side_cell(cell, l, cols) - jnp.where(shift < HB, cols - HB + shift, shift - HB)
        own = cell % slots // HB == at // (2 * HB)
        lon_taps[l, 2], lon_taps[l, 3] = split(jnp.where(own, tap_value(gap, spread, scale), 0.0))
        edge_taps[l, 0], edge_taps[l, 1] = split(tap_value(side_cell(at, l, cols) - cell, spread, scale))
        lat_back[l] = lat_taps(spread, scale, half, deep, -HB, wide_k)
        lat_fore[l, 0] = lat_taps(spread, scale, deep, deep, HB, wide_k)
        lat_fore[l, 1] = lat_taps(spread, scale, deep, deep, -2 * HB, wide_k)

    def tall(u, l):
        h, lo = split(u)
        out = []
        for b in range(2):
            at = slice(b * (rows - deep), b * (rows - deep) + deep)
            stack = rows_of(h[at], h[at], lo[at])
            out.append(dot(lat_fore[l, b, :, : 3 * deep], stack)[: half + HB])
        return out

    for l in range(levels):
        ext[l, HB : HB + rows, :cols] = jnp.zeros((rows, cols), F32)

    @pl.loop(0, steps)
    def _(g):
        group_load(alpha, a_tile, g, 2 + steps).wait()
        for l in range(levels):
            taps = rows_of(
                lanes_of(lon_taps[l, 0], edge_taps[l, 0]), lanes_of(lon_taps[l, 1], edge_taps[l, 1])
            )
            fields = [a_tile[g * GROUP + m, l] for m in range(GROUP)]
            u = dot(rows_of(*[lanes_of(a, a) for a in fields]), taps)
            side = u[:rows, cols:]
            for m in range(1, GROUP):
                mine = lane % slots // HB == m
                side = jnp.where(mine, u[m * rows : (m + 1) * rows, cols:], side)
            total = None
            for k in range(0, GROUP, 2):
                pair = [u[m * rows : (m + 1) * rows, :cols] for m in (k, k + 1)]
                top, bottom = tall(lanes_of(*pair), l)
                for i, m in enumerate((k, k + 1)):
                    at = slice(i * cols, (i + 1) * cols)
                    v = rows_of(top[HB:, at], bottom[:half, at])
                    part = p_tile[g * GROUP + m, l].astype(F32) * v
                    total = part if total is None else total + part
                    v_strip[g * GROUP + m, l] = rows_of(top[:HB, at], bottom[half:, at])
            ext[l, HB : HB + rows, :cols] += total
            v_side[g, l] = rows_of(*tall(side, l))

    for one in p_rows:
        one.arrive()

    for one in f_rows:
        one.arrive()
    for one in small:
        one.arrive()
    lat_at = lanes_of(lat_i[...], lat_i_low[:, frows - FR :], lat_i_high[:, :FR]).astype(F32)
    lat_by = lanes_of(lat_w[...], lat_w_low[:, frows - FR :], lat_w_high[:, :FR])
    lat_at = lat_at - (lax.axis_index("gy") * rows).astype(F32)
    lon_at = lanes_of(lon_i[...], lon_i_west[:, fcols - FC :], lon_i_east[:, :FC]).astype(F32)
    lon_by = lanes_of(lon_w[...], lon_w_west[:, fcols - FC :], lon_w_east[:, :FC])
    lon_total = float(cols * lax.axis_size("gx"))
    lon_at = lon_at - (lax.axis_index("gx") * cols).astype(F32)
    lon_at = jnp.where(
        lon_at < -64.0, lon_at + lon_total, jnp.where(lon_at >= lon_total - 64.0, lon_at - lon_total, lon_at)
    )
    f_tall, f_wide = frows + 2 * FR, fcols + 2 * FC

    def upright(at, by):
        size = at.shape[1]
        space = jnp.zeros((1, -size % 128), F32)
        at, by = lanes_of(at, space), lanes_of(by, space)
        shape = (8, at.shape[1])
        both = jnp.where(iota(shape, 0) == 0, jnp.broadcast_to(at, shape), jnp.broadcast_to(by, shape))
        both = both.T[:size]
        return both[:, 0:1], both[:, 1:2]

    lat_at_up, lat_by_up = upright(lat_at, lat_by)
    lon_at_up, lon_by_up = upright(lon_at, lon_by)
    t_rows, e_rows = rows + 2 * CR, rows + 2 * HB
    up_lat[0], up_lat[1] = split(weigh(iota((f_tall, t_rows), 1) - CR, lat_at_up, lat_by_up))
    down_lat[0], down_lat[1] = split(weigh(iota((e_rows, f_tall), 0) - HB, lat_at, lat_by))
    order = iota((2 * cols, f_wide), 0)
    w = order - cols
    wing = jnp.where(
        w < REACH,
        w - (REACH - HB),
        jnp.where(
            (w >= slots - HB) & (w < slots),
            w - slots,
            jnp.where(
                (w >= slots) & (w < slots + REACH),
                w - slots + cols - HB,
                jnp.where(w >= cols - HB, w + HB, -1000),
            ),
        ),
    )
    up_lon[0], up_lon[1] = split(weigh(jnp.where(w < 0, order, wing), lon_at, lon_by))
    order = iota((f_wide, 2 * cols), 1)
    cell = jnp.where(order < cols, order, side_cell(order - cols, ma, cols))
    down_lon[0], down_lon[1] = split(weigh(cell, lon_at_up, lon_by_up))

    for l in range(levels):

        def strips(g, sums):
            north, south = sums
            for k in range(GROUP):
                m = g * GROUP + k
                north = north + p_north[m, l].astype(F32) * v_strip[m, l, :HB]
                south = south + p_south[m, l].astype(F32) * v_strip[m, l, HB:]
            return north, south

        zero = jnp.zeros((HB, cols), F32)
        north, south = lax.fori_loop(0, steps, strips, (zero, zero))
        ext[l, :HB, :cols] = north
        ext[l, HB + rows :, :cols] = south

    for i in range(2):
        fine_wide[i, :, :fcols] = rows_of(fine_tile[i], f_low[i], f_high[i])

    t_lane = iota((t_rows, cols), 1)

    def fold(x, first, deep):
        total = None
        lane_at = iota((deep, cols), 1)
        for b in range(x.shape[0] // deep):
            part = pltpu.roll(x[b * deep : (b + 1) * deep], (b * REACH - first) % cols, 1)
            total = part if total is None else jnp.where(lane_at >= b * REACH, part, total)
        return total

    def unfold(x, first, start, blocks):
        parts = [pltpu.roll(x, (first - b * REACH) % cols, 1) for b in range(start, start + blocks)]
        return rows_of(*parts)

    def side_sum(total, l):
        if l:
            total = pltpu.roll(total, slots, 1)
        for shift in (HB, 2 * HB, 4 * HB):
            total = total + pltpu.roll(total, shift, 1)
        return total

    def products(l, g, take, v):
        west, east = take(p_west.at[g]).astype(F32), take(p_east.at[g]).astype(F32)
        return jnp.where(iota(west.shape, 1) // slots == l, west, east) * v

    def outward(core, side):
        lane_at = iota(side.shape, 1)
        eastward = jnp.where(lane_at >= cols - HB, side, pltpu.roll(core, cols - HB, 1))
        westward = jnp.where(lane_at < slots, side, pltpu.roll(core, slots, 1))
        return (eastward, cols - REACH), (westward, slots - HB)

    def rim_of(part):
        far = part[rows:].astype(F32)
        near = [part[:rim].astype(F32), part[rows - rim : rows].astype(F32)]
        return rows_of(far[:HB], *near, far[HB:])

    for one in rims:
        one.arrive()
    for l in range(levels):
        total = None
        for g in range(steps):
            v = rows_of(v_side[g, l, :STRIP], v_side[g, l, e_rows - STRIP :])
            part = products(l, g, rim_of, v)
            total = part if total is None else total + part
        total = side_sum(total, l)
        ext[l, :STRIP, cols:] = total[:STRIP]
        ext[l, e_rows - STRIP :, cols:] = total[STRIP:]
        core = rows_of(ext[l, :STRIP, :cols], ext[l, e_rows - STRIP :, :cols])
        for i, (x, first) in enumerate(outward(core, total)):
            tip[l, i] = fold(rows_of(x[STRIP:], x[:STRIP]), first, HB)

    corner_links, side_links, end_links, swaps = [], [], [], []
    for s in range(count):
        peer = lax.rem(ma + s, count)
        for i, step in enumerate((1, -1)):
            at = {"ma": peer}
            side_links.append(link("gx", step, flank.at[peer, i], flanks.at[s, i], at))
            strip = ext.at[peer, pl.ds((e_rows - STRIP) * (1 - i), STRIP)]
            end_links.append(link("gy", step, strip, ends_in.at[s, i], at))
            at = {"gx": lax.rem(gx + step + gxn, gxn), "ma": peer}
            for j, turn in enumerate((1, -1)):
                corner_links.append(link("gy", turn, tip.at[peer, i], tips.at[s, i, j], at))
        if s:
            swaps.append(link("ma", peer - ma, ext.at[peer], other.at[s - 1]))
    for one in corner_links + end_links:
        one.start()
    inside = slice(STRIP, e_rows - STRIP)
    side_sums = [None] * levels
    for g in range(steps):
        if g:
            for one in p_arrive[g - 1]:
                one.arrive()
        for l in range(levels):
            part = products(l, g, lambda x: x[rim : rows - rim], v_side[g, l, inside])
            side_sums[l] = part if g == 0 else side_sums[l] + part
    for l in range(levels):
        ext[l, inside, cols:] = side_sum(side_sums[l], l)
        for i, (x, first) in enumerate(outward(ext[l, :, :cols], ext[l, :, cols:])):
            flank[l, i] = fold(x, first, STRIP)
    sent = corner_links + end_links + side_links + swaps
    late = side_links + swaps + f_arrive
    for one in late:
        one.start()
    for one in pending:
        if one not in late:
            one.sent()
    for one in sent:
        one.arrive()
    mine, strips_in, flank_in, tip_in = ext[ma], ends_in[0], flanks[0], tips[0]
    for s in range(1, count):
        mine = mine + other[s - 1]
        strips_in, flank_in, tip_in = strips_in + ends_in[s], flank_in + flanks[s], tip_in + tips[s]
    lap = CR - HB
    edge = STRIP - lap

    def merge(above, middle, below):
        return rows_of(
            above[:lap],
            middle[:edge] + above[lap:],
            middle[edge : e_rows - edge],
            middle[e_rows - edge :] + below[:edge],
            below[edge:],
        )

    mine = merge(strips_in[0], mine, strips_in[1])
    core, side = mine[:, :cols], mine[:, cols:]
    third = STRIP // HB

    def wing_from(i, first):
        return merge(
            unfold(tip_in[i, 0], first, 0, third),
            unfold(flank_in[i], first, 0, e_rows // STRIP),
            unfold(tip_in[i, 1], first, third, third),
        )

    wings = jnp.where(
        t_lane < REACH,
        wing_from(0, 0),
        jnp.where((t_lane >= slots) & (t_lane < slots + REACH), wing_from(1, slots), side),
    )
    across = dot3(split(lanes_of(core, wings)), (up_lon[0], up_lon[1]))
    fine = dot3((up_lat[0], up_lat[1]), split(across))
    increment[ma] = fine[:frows, :fcols]
    final = []

    def share(whole):
        for s in range(1, count):
            peer = lax.rem(ma + s, count)
            final.append(link("ma", peer - ma, whole.at[ma], whole.at[ma]))
            final[-1].start()

    share(increment)
    for one in f_arrive:
        one.arrive()
    for i in range(2):

        def wing_of(part):
            def opened(first, last):
                lanes = range(FC * i, 2 * FOLD * FC, 2 * FC)
                return [part[first:last, x : x + FC] for x in lanes]

            low, high = f_main, f_main + HB
            return rows_of(
                rows_of(*opened(0, low))[:frows], *opened(low, high), *opened(high, high + HB)
            )

        fine_wide[i, :, fcols:] = lanes_of(wing_of(f_west), wing_of(f_east))
    misfit = fine_wide[1] * (fine - fine_wide[0])
    across = dot3((down_lat[0], down_lat[1]), split(misfit))
    residual[ma] = dot3(split(across), (down_lon[0], down_lon[1]))
    share(residual)
    for one in late:
        one.sent()
    for one in final:
        one.arrive()
    for one in final:
        one.sent()


def cost(flops, nbytes):
    return pl.CostEstimate(flops=flops, bytes_accessed=nbytes, transcendentals=0)


def core_step(widths, lat_i, lat_w, lon_i, lon_w, alpha, perts, innov, weight):
    members, levels, rows, cols = alpha.shape
    steps = members // GROUP
    frows, fcols = innov.shape[1:]
    count = lax.axis_size("ma")
    assert levels == 2 and count == levels
    assert (rows + 2 * HB) % STRIP == 0
    half = rows // 2
    deep = half + 2 * HB
    wide_k = -(-3 * deep // 128) * 128
    e_rows, t_rows = rows + 2 * HB, rows + 2 * CR
    f_tall, f_wide = frows + 2 * FR, fcols + 2 * FC
    strip = ((members, levels, HB, cols), BF16)
    side = ((steps, e_rows, cols), BF16)
    outs = [
        (innov.shape, F32),
        ((levels, e_rows, 2 * cols), F32),
        (alpha.shape, BF16),
        (alpha.shape, BF16),
        strip,
        strip,
        side,
        side,
        ((levels, 4, cols, cols), BF16),
        ((levels, half, wide_k), BF16),
    ]
    kept = sum(math.prod(shape) * jnp.dtype(kind).itemsize for shape, kind in outs)
    fine_edge = ((2, FR, fcols), F32)
    fine_side = ((-(-frows // (FOLD * HB)) * HB + 2 * HB, cols), F32)
    packed = ((steps, rows, cols), BF16)
    scratch = [
        (lat_i.shape, jnp.int32),
        (lat_w.shape, F32),
        (lon_i.shape, jnp.int32),
        (lon_w.shape, F32),
        ((2, frows, fcols), F32),
        ((levels * GROUP // 2, 2 * cols, 2 * cols), BF16),
        ((levels, 2, cols, cols), BF16),
        ((levels, 2, deep, wide_k), BF16),
        ((members, levels, 2 * HB, cols), F32),
        ((steps, levels, e_rows, cols), F32),
        packed,
        packed,
        fine_edge,
        fine_edge,
        fine_side,
        fine_side,
        fine_side,
        fine_side,
        ((2, f_tall, f_wide), F32),
        (lat_i.shape, jnp.int32),
        (lat_i.shape, jnp.int32),
        (lat_w.shape, F32),
        (lat_w.shape, F32),
        (lon_i.shape, jnp.int32),
        (lon_i.shape, jnp.int32),
        (lon_w.shape, F32),
        (lon_w.shape, F32),
        ((2, 2 * cols, f_wide), BF16),
        ((2, f_tall, t_rows), BF16),
        ((2, e_rows, f_tall), BF16),
        ((2, f_wide, 2 * cols), BF16),
        ((levels, e_rows, 2 * cols), F32),
        ((count - 1, e_rows, 2 * cols), F32),
        ((count, 2, STRIP, 2 * cols), F32),
        ((levels, 2, STRIP, cols), F32),
        ((levels, 2, HB, cols), F32),
        ((count, 2, STRIP, cols), F32),
        ((count, 2, 2, HB, cols), F32),
    ]
    vmem = pl.BlockSpec(memory_space=pltpu.VMEM)
    anywhere = pl.BlockSpec(memory_space=pltpu.HBM)
    return pl.pallas_call(
        core_kernel,
        in_specs=[anywhere] * 9,
        out_specs=[vmem] * len(outs),
        out_shape=[pltpu.VMEM(shape, kind) for shape, kind in outs],
        scratch_shapes=[pltpu.SMEM(widths.shape, jnp.int32)]
        + [pltpu.VMEM(shape, kind) for shape, kind in scratch]
        + [
            pltpu.SemaphoreType.DMA((96,)),
            pltpu.SemaphoreType.DMA((96,)),
            pltpu.SemaphoreType.DMA((7 + 2 * steps,)),
        ],
        compiler_params=pltpu.CompilerParams(
            collective_id=0, has_side_effects=True, vmem_limit_bytes=VMEM_BYTES - VMEM_SLACK - kept
        ),
        cost_estimate=cost(2**30, 2**24),
    )(widths, lat_i, lat_w, lon_i, lon_w, alpha, perts, innov, weight)


def band(high, low, taps):
    half = taps.shape[0]
    deep = half + 2 * HB
    out = []
    for first in range(0, high.shape[0] - 2 * HB, half):
        h, lo = high[first : first + deep], low[first : first + deep]
        out.append(dot(taps, rows_of(h, h, lo)))
    return rows_of(*out)


def adjoint_kernel(
    alpha, perts, north, south, west, east, residual, lon, lat, fine, out, fine_out, sem
):
    rows, cols = alpha.shape[2:]
    slots = GROUP * HB
    g = pl.program_id(0)
    give = pltpu.make_async_copy(fine, fine_out, sem.at[0])

    @pl.when(g == 0)
    def _():
        give.start()

    @pl.when(g == pl.num_programs(0) - 1)
    def _():
        give.wait()

    zero = jnp.zeros((cols, cols), BF16)

    def stack(high, low):
        return rows_of(lanes_of(high, low), lanes_of(high, zero))

    def halves(x):
        return x[:, :cols] + x[:, cols:]

    lane = iota((rows, cols), 1)
    inner = (lane >= HB) & (lane < cols - HB)
    wide = iota((rows + 2 * HB, cols), 1)
    for l in range(alpha.shape[1]):
        res = residual[l]
        taps = lat[l, :, : 3 * (rows // 2 + 2 * HB)]
        side = jnp.where(wide // slots == l, west[g].astype(F32), east[g].astype(F32))
        edge = band(*split(natural(side, rows) * res[:, cols:]), taps)
        edge = halves(dot(lanes_of(*split(edge)), stack(lon[l, 2], lon[l, 3])))
        cores = []
        for k in range(0, GROUP, 2):
            pairs = []
            for m in (k, k + 1):
                n = g * GROUP + m
                tall = rows_of(
                    north[n, l].astype(F32), perts[n, l].astype(F32), south[n, l].astype(F32)
                )
                pairs.append(split(tall * res[:, :cols]))
            both = band(lanes_of(pairs[0][0], pairs[1][0]), lanes_of(pairs[0][1], pairs[1][1]), taps)
            for i in range(2):
                cores.append(lanes_of(*split(both[:, i * cols : (i + 1) * cols])))
        total = dot(rows_of(*cores), stack(lon[l, 0], lon[l, 1]))
        for m in range(GROUP):
            turned = pltpu.roll(edge, (cols - HB - 2 * HB * m) % cols, 1)
            value = halves(total[m * rows : (m + 1) * rows]) + jnp.where(inner, 0.0, turned)
            out[m, l] = alpha[g * GROUP + m, l].astype(F32) + value


def adjoint(alpha, perts, north, south, west, east, residual, lon, lat, fine):
    members, levels, rows, cols = alpha.shape
    return pl.pallas_call(
        adjoint_kernel,
        grid=(members // GROUP,),
        in_specs=[pl.BlockSpec(memory_space=pltpu.VMEM)] * 10,
        out_specs=[
            pl.BlockSpec((GROUP, levels, rows, cols), lambda g: (g, 0, 0, 0)),
            pl.BlockSpec(memory_space=pltpu.HBM),
        ],
        out_shape=[
            jax.ShapeDtypeStruct(alpha.shape, F32),
            jax.ShapeDtypeStruct(fine.shape, F32),
        ],
        scratch_shapes=[pltpu.SemaphoreType.DMA((1,))],
        compiler_params=pltpu.CompilerParams(vmem_limit_bytes=BACK_LIMIT),
        cost_estimate=cost(members * levels * 2**25, alpha.size * 8),
    )(alpha, perts, north, south, west, east, residual, lon, lat, fine)


def body(
    alpha_fields,
    member_perts,
    band_widths,
    lat_index,
    lat_weight,
    lon_index,
    lon_weight,
    innovation,
    obs_weight,
):
    tables = [x.reshape(1, -1) for x in (lat_index, lat_weight, lon_index, lon_weight)]
    increment, residual, alpha, perts, *rest = core_step(
        band_widths, *tables, alpha_fields, member_perts, innovation, obs_weight
    )
    north, south, west, east, lon, lat = rest
    gradient, increment = adjoint(
        alpha, perts, north, south, west, east, residual, lon, lat, increment
    )
    return (increment, gradient)


def solution(mesh):
    placed = (
        P("ma", None, "gy", "gx"),
        P("ma", None, "gy", "gx"),
        P(),
        P("gy"),
        P("gy"),
        P("gx"),
        P("gx"),
        P(None, "gy", "gx"),
        P(None, "gy", "gx"),
    )
    return jax.shard_map(
        body,
        mesh=mesh,
        in_specs=placed,
        out_specs=(P(None, "gy", "gx"), P("ma", None, "gy", "gx")),
        check_vma=False,
    )
```

```python
import math

import jax
import jax.numpy as jnp
from jax import lax
from jax.experimental import pallas as pl
from jax.experimental.pallas import tpu as pltpu
from jax.sharding import PartitionSpec as P

HB = 8
GROUP = 8
FR = 24
FC = 20
FOLD = 3
CR = 16
STRIP = 24
REACH = HB + 10
MESH = pl.DeviceIdType.MESH
VMEM_BYTES = 67043328
VMEM_SLACK = 2**17
BACK_LIMIT = 32 * 2**20
F32 = jnp.float32
BF16 = jnp.bfloat16


def iota(shape, dim):
    return lax.broadcasted_iota(jnp.int32, shape, dim)


def dot(a, b):
    return jnp.dot(a, b, preferred_element_type=F32)


def split(value):
    high = value.astype(BF16)
    return high, (value - high.astype(F32)).astype(BF16)


def dot3(a, b):
    return dot(a[0], b[0]) + dot(a[1], b[0]) + dot(a[0], b[1])


def rows_of(*parts):
    return jnp.concatenate(parts, axis=0)


def lanes_of(*parts):
    return jnp.concatenate(parts, axis=1)


def natural(x, rows):
    return rows_of(x[rows : rows + HB], x[:rows], x[rows + HB :])


def place(order, size, width):
    return jnp.where(order < size, order, jnp.where(order < size + width, order - size - width, order - width))


def tap_value(distance, spread, scale):
    d = distance.astype(F32)
    value = jnp.exp(-(d * d) / (2.0 * spread * spread)) * scale
    return jnp.where(jnp.abs(distance) <= HB, value, 0.0)


def tap_scale(spread):
    lane = iota((8, 128), 1)
    d = (lane - HB).astype(F32)
    shape = jnp.where(lane <= 2 * HB, jnp.exp(-(d * d) / (2.0 * spread * spread)), 0.0)
    return (1.0 / jnp.sqrt(jnp.sum(shape * shape, axis=1, keepdims=True)))[:1]


def lat_taps(spread, scale, height, deep, offset, width):
    i, c = iota((height, width), 0), iota((height, width), 1)
    r = jnp.where(c >= 2 * deep, c - 2 * deep, jnp.where(c >= deep, c - deep, c))
    value = tap_value(r - i + offset, spread, scale)
    high = value.astype(BF16).astype(F32)
    return jnp.where((c >= deep) & (c < 2 * deep), value - high, high).astype(BF16)


def side_cell(lane, level, cols):
    west = lane // (GROUP * HB) == level
    return jnp.where(west, lane % HB - HB, cols + lane % HB)


def weigh(cell, index, weight):
    cell = cell.astype(F32)
    return jnp.where(cell == index, 1.0 - weight, 0.0) + jnp.where(cell == index + 1.0, weight, 0.0)


class Link:
    def __init__(self, axis, step, src, dst, send, recv, slot, also=None):
        me, count = lax.axis_index(axis), lax.axis_size(axis)
        target = me + step
        self.sends = self.gets = None
        if axis == "gx":
            target = lax.rem(target + count, count)
        elif axis == "gy":
            self.sends = (target >= 0) & (target < count)
            self.gets = (me - step >= 0) & (me - step < count)
        self.dst = dst
        device = {axis: target, **(also or {})}
        self.copy = pltpu.make_async_remote_copy(
            src_ref=src,
            dst_ref=dst,
            send_sem=send.at[slot],
            recv_sem=recv.at[slot],
            device_id=device,
            device_id_type=MESH,
        )

    def start(self):
        if self.sends is None:
            self.copy.start()
        else:
            pl.when(self.sends)(self.copy.start)

    def arrive(self):
        if self.gets is None:
            self.copy.wait_recv()
        else:
            pl.when(self.gets)(self.copy.wait_recv)

            @pl.when(jnp.logical_not(self.gets))
            def _():
                self.dst[...] = jnp.zeros_like(self.dst)

    def sent(self):
        if self.sends is None:
            self.copy.wait_send()
        else:
            pl.when(self.sends)(self.copy.wait_send)


def greet():
    barrier = pltpu.get_barrier_semaphore()
    gx, gxn = lax.axis_index("gx"), lax.axis_size("gx")
    gy, gyn = lax.axis_index("gy"), lax.axis_size("gy")
    ma, count = lax.axis_index("ma"), lax.axis_size("ma")

    def hail(device):
        pl.semaphore_signal(barrier, inc=1, device_id=device, device_id_type=MESH)

    peers = [lax.rem(ma + s, count) for s in range(count)]
    sides = [lax.rem(gx + step, gxn) for step in (1, gxn - 1)]
    for step, there in ((-1, gy > 0), (1, gy < gyn - 1)):

        @pl.when(there)
        def _(step=step):
            for side in (*sides, gx):
                for peer in peers[::-1]:
                    hail({"gx": side, "gy": gy + step, "ma": peer})

    for side in sides:
        for peer in peers[::-1]:
            hail({"gx": side, "ma": peer})
    for peer in peers[1:]:
        hail({"ma": peer})

    below, above = jnp.minimum(gy, 1), jnp.minimum(gyn - 1 - gy, 1)
    return lambda: pl.semaphore_wait(barrier, 3 * count - 1 + (below + above) * 3 * count)


def core_kernel(
    widths_in, lat_i_in, lat_w_in, lon_i_in, lon_w_in, alpha, perts, innov, weight,
    increment, residual, a_tile, p_tile, p_north, p_south, p_west, p_east, lon_taps, lat_back,
    widths, lat_i, lat_w, lon_i, lon_w, fine_tile, pick, edge_taps, lat_fore, v_strip, v_side, p_right, p_left,
    f_low, f_high, f_right, f_left, f_west, f_east, fine_wide,
    lat_i_low, lat_i_high, lat_w_low, lat_w_high, lon_i_west, lon_i_east, lon_w_west, lon_w_east,
    up_lon, up_lat, down_lat, down_lon, ext, other, ends_in, flank, tip, flanks, tips,
    send, recv, local,
):
    members, levels, rows, cols = alpha.shape
    steps, half, slots = members // GROUP, rows // 2, GROUP * HB
    frows, fcols = innov.shape[1:]
    ma, count = lax.axis_index("ma"), lax.axis_size("ma")
    gx, gxn = lax.axis_index("gx"), lax.axis_size("gx")
    met = greet()
    tables = ((widths_in, widths), (lat_i_in, lat_i), (lat_w_in, lat_w), (lon_i_in, lon_i), (lon_w_in, lon_w))
    t_loads = [
        pltpu.make_async_copy(src, dst, local.at[2 + 2 * steps + i])
        for i, (src, dst) in enumerate(tables)
    ]
    for load in t_loads:
        load.start()
    f_loads = [
        pltpu.make_async_copy(src.at[ma], fine_tile.at[i], local.at[i])
        for i, src in enumerate((innov, weight))
    ]

    def group_load(src, dst, g, first):
        span = pl.ds(g * GROUP, GROUP)
        return pltpu.make_async_copy(src.at[span], dst.at[span], local.at[first + g])

    p_loads = [group_load(perts, p_tile, g, 2) for g in range(steps)]
    for load in p_loads + f_loads:
        load.start()
    counter = iter(range(96))
    pending = []

    def link(axis, step, src, dst, also=None):
        one = Link(axis, step, src, dst, send, recv, next(counter), also)
        pending.append(one)
        return one

    r, c = iota((cols, 2 * cols), 0), iota((cols, 2 * cols), 1)
    base = jnp.where(
        ((c < cols) & (r - (cols - HB) == c % HB)) | ((c >= cols) & (r == c % HB)), 1.0, 0.0
    )
    turned = (c % cols) // slots
    slot = jnp.where(c < cols, turned, 1 - turned) * GROUP + c % slots // HB
    for l in range(levels):
        for k in range(GROUP):
            at = slice(k % 2 * cols, (k % 2 + 1) * cols)
            n = l * GROUP + k
            pick[n // 2, at] = jnp.where(slot == n, base, 0.0).astype(BF16)
    f_rows = [
        link("gy", 1, innov.at[ma, pl.ds(frows - FR, FR)], f_low.at[0]),
        link("gy", -1, innov.at[ma, pl.ds(0, FR)], f_high.at[0]),
        link("gy", 1, weight.at[ma, pl.ds(frows - FR, FR)], f_low.at[1]),
        link("gy", -1, weight.at[ma, pl.ds(0, FR)], f_high.at[1]),
    ]
    p_rows = [
        link("gy", 1, perts.at[:, :, pl.ds(rows - HB, HB), :], p_north),
        link("gy", -1, perts.at[:, :, pl.ds(0, HB), :], p_south),
    ]
    small = [
        link("gy", 1, lat_i, lat_i_low),
        link("gy", -1, lat_i, lat_i_high),
        link("gy", 1, lat_w, lat_w_low),
        link("gy", -1, lat_w, lat_w_high),
        link("gx", 1, lon_i, lon_i_west),
        link("gx", -1, lon_i, lon_i_east),
        link("gx", 1, lon_w, lon_w_west),
        link("gx", -1, lon_w, lon_w_east),
    ]
    def tilted(src, dst, side, top, bottom, first):
        pairs = []
        for step, at, to in ((1, bottom, first), (-1, top, first + HB)):
            span, there = pl.ds(at, HB), pl.ds(to, HB)
            index = (slice(None),) * (src.ndim - 2)
            pairs.append(
                link(
                    "gy",
                    step,
                    src.at[(*index, span)],
                    dst.at[(*index, there)],
                    {"gx": lax.rem(gx + side, gxn)},
                )
            )
        return pairs

    def packed(piece):
        total = None
        for l in range(levels):
            for k in range(0, GROUP, 2):
                n = (l * GROUP + k) // 2
                part = dot(lanes_of(piece(l, k), piece(l, k + 1)), pick[n])
                total = part if total is None else total + part
        return total.astype(BF16)

    a_loads = [group_load(alpha, a_tile, g, 2 + steps) for g in range(steps)]
    p_arrive = []
    rim = STRIP - HB

    def p_sides(groups, first, deep):
        part, span = pl.ds(groups.start, groups.stop - groups.start), pl.ds(first, deep)
        pair = [
            link("gx", 1, p_right.at[part, span], p_west.at[part, span]),
            link("gx", -1, p_left.at[part, span], p_east.at[part, span]),
        ]
        for one in pair:
            one.start()
        return pair

    for g in range(steps):
        p_loads[g].wait()
        a_loads[g].start()
        both = packed(lambda l, k: p_tile[g * GROUP + k, l])
        p_right[g] = both[:, :cols]
        p_left[g] = both[:, cols:]
        if g == 0:
            for load in t_loads:
                load.wait()
            met()
            for one in small + p_rows:
                one.start()
            rims = p_sides(range(1), 0, rows)
    corners = tilted(p_right, p_west, 1, 0, rows - HB, rows)
    corners += tilted(p_left, p_east, gxn - 1, 0, rows - HB, rows)
    for first in (0, rows - rim):
        rims += p_sides(range(1, steps), first, rim)
    for one in corners:
        one.start()
    rims += corners
    for g in range(1, steps):
        p_arrive.append(p_sides(range(g, g + 1), rim, rows - 2 * rim))
    for one in f_rows:
        one.start()

    f_main = f_west.shape[0] - 2 * HB

    def f_fold(first, count, start):
        deep = -(-count // (FOLD * HB)) * HB
        parts = []
        for b in range(FOLD):
            stop = min(first + (b + 1) * deep, first + count)
            for i in range(2):
                part = fine_tile[i, first + b * deep : stop, start : start + FC]
                short = deep - part.shape[0]
                parts.append(rows_of(part, jnp.zeros((short, FC), F32)) if short else part)
        return lanes_of(*parts, jnp.zeros((deep, cols - 2 * FOLD * FC), F32))

    for load in f_loads:
        load.wait()
    f_arrive = []
    for step, side, src, dst, start in (
        (1, 1, f_right, f_west, fcols - FC),
        (-1, gxn - 1, f_left, f_east, 0),
    ):
        src[:f_main] = f_fold(0, frows, start)
        src[f_main : f_main + HB] = f_fold(0, FR, start)
        src[f_main + HB :] = f_fold(frows - FR, FR, start)
        span = pl.ds(0, f_main)
        f_arrive.append(link("gx", step, src.at[span], dst.at[span]))
        f_arrive += tilted(src, dst, side, f_main, f_main + HB, f_main)

    lane = iota((cols, cols), 1)
    deep = half + 2 * HB
    wide_k = lat_fore.shape[3]
    for l in range(levels):
        spread = widths[l].astype(F32)
        scale = tap_scale(spread)
        cell, at = iota((cols, cols), 0), lane
        lon_taps[l, 0], lon_taps[l, 1] = split(tap_value(cell - at, spread, scale))
        shift = at % (2 * HB)
        gap = side_cell(cell, l, cols) - jnp.where(shift < HB, cols - HB + shift, shift - HB)
        own = cell % slots // HB == at // (2 * HB)
        lon_taps[l, 2], lon_taps[l, 3] = split(jnp.where(own, tap_value(gap, spread, scale), 0.0))
        edge_taps[l, 0], edge_taps[l, 1] = split(tap_value(side_cell(at, l, cols) - cell, spread, scale))
        lat_back[l] = lat_taps(spread, scale, half, deep, -HB, wide_k)
        lat_fore[l, 0] = lat_taps(spread, scale, deep, deep, HB, wide_k)
        lat_fore[l, 1] = lat_taps(spread, scale, deep, deep, -2 * HB, wide_k)

    def tall(u, l):
        h, lo = split(u)
        out = []
        for b in range(2):
            at = slice(b * (rows - deep), b * (rows - deep) + deep)
            stack = rows_of(h[at], h[at], lo[at])
            out.append(dot(lat_fore[l, b, :, : 3 * deep], stack)[: half + HB])
        return out

    for l in range(levels):
        ext[l, HB : HB + rows, :cols] = jnp.zeros((rows, cols), F32)

    @pl.loop(0, steps)
    def _(g):
        group_load(alpha, a_tile, g, 2 + steps).wait()
        for l in range(levels):
            taps = rows_of(
                lanes_of(lon_taps[l, 0], edge_taps[l, 0]), lanes_of(lon_taps[l, 1], edge_taps[l, 1])
            )
            fields = [a_tile[g * GROUP + m, l] for m in range(GROUP)]
            u = dot(rows_of(*[lanes_of(a, a) for a in fields]), taps)
            side = u[:rows, cols:]
            for m in range(1, GROUP):
                mine = lane % slots // HB == m
                side = jnp.where(mine, u[m * rows : (m + 1) * rows, cols:], side)
            total = None
            for k in range(0, GROUP, 2):
                pair = [u[m * rows : (m + 1) * rows, :cols] for m in (k, k + 1)]
                top, bottom = tall(lanes_of(*pair), l)
                for i, m in enumerate((k, k + 1)):
                    at = slice(i * cols, (i + 1) * cols)
                    v = rows_of(top[HB:, at], bottom[:half, at])
                    part = p_tile[g * GROUP + m, l].astype(F32) * v
                    total = part if total is None else total + part
                    v_strip[g * GROUP + m, l] = rows_of(top[:HB, at], bottom[half:, at])
            ext[l, HB : HB + rows, :cols] += total
            v_side[g, l] = rows_of(*tall(side, l))

    for one in p_rows:
        one.arrive()

    for one in f_rows:
        one.arrive()
    for one in small:
        one.arrive()
    lat_at = lanes_of(lat_i[...], lat_i_low[:, frows - FR :], lat_i_high[:, :FR]).astype(F32)
    lat_by = lanes_of(lat_w[...], lat_w_low[:, frows - FR :], lat_w_high[:, :FR])
    lat_at = lat_at - (lax.axis_index("gy") * rows).astype(F32)
    lon_at = lanes_of(lon_i[...], lon_i_west[:, fcols - FC :], lon_i_east[:, :FC]).astype(F32)
    lon_by = lanes_of(lon_w[...], lon_w_west[:, fcols - FC :], lon_w_east[:, :FC])
    lon_total = float(cols * lax.axis_size("gx"))
    lon_at = lon_at - (lax.axis_index("gx") * cols).astype(F32)
    lon_at = jnp.where(
        lon_at < -64.0, lon_at + lon_total, jnp.where(lon_at >= lon_total - 64.0, lon_at - lon_total, lon_at)
    )
    f_tall, f_wide = frows + 2 * FR, fcols + 2 * FC

    def upright(at, by):
        size = at.shape[1]
        space = jnp.zeros((1, -size % 128), F32)
        at, by = lanes_of(at, space), lanes_of(by, space)
        shape = (8, at.shape[1])
        both = jnp.where(iota(shape, 0) == 0, jnp.broadcast_to(at, shape), jnp.broadcast_to(by, shape))
        both = both.T[:size]
        return both[:, 0:1], both[:, 1:2]

    lat_at_up, lat_by_up = upright(lat_at, lat_by)
    lon_at_up, lon_by_up = upright(lon_at, lon_by)
    t_rows, e_rows = rows + 2 * CR, rows + 2 * HB
    up_lat[0], up_lat[1] = split(weigh(iota((f_tall, t_rows), 1) - CR, lat_at_up, lat_by_up))
    down_lat[0], down_lat[1] = split(weigh(iota((e_rows, f_tall), 0) - HB, lat_at, lat_by))
    order = iota((2 * cols, f_wide), 0)
    w = order - cols
    wing = jnp.where(
        w < REACH,
        w - (REACH - HB),
        jnp.where(
            (w >= slots - HB) & (w < slots),
            w - slots,
            jnp.where(
                (w >= slots) & (w < slots + REACH),
                w - slots + cols - HB,
                jnp.where(w >= cols - HB, w + HB, -1000),
            ),
        ),
    )
    up_lon[0], up_lon[1] = split(weigh(jnp.where(w < 0, order, wing), lon_at, lon_by))
    order = iota((f_wide, 2 * cols), 1)
    cell = jnp.where(order < cols, order, side_cell(order - cols, ma, cols))
    down_lon[0], down_lon[1] = split(weigh(cell, lon_at_up, lon_by_up))

    for l in range(levels):

        def strips(g, sums):
            north, south = sums
            for k in range(GROUP):
                m = g * GROUP + k
                north = north + p_north[m, l].astype(F32) * v_strip[m, l, :HB]
                south = south + p_south[m, l].astype(F32) * v_strip[m, l, HB:]
            return north, south

        zero = jnp.zeros((HB, cols), F32)
        north, south = lax.fori_loop(0, steps, strips, (zero, zero))
        ext[l, :HB, :cols] = north
        ext[l, HB + rows :, :cols] = south

    for i in range(2):
        fine_wide[i, :, :fcols] = rows_of(fine_tile[i], f_low[i], f_high[i])

    t_lane = iota((t_rows, cols), 1)

    def fold(x, first, deep):
        total = None
        lane_at = iota((deep, cols), 1)
        for b in range(x.shape[0] // deep):
            part = pltpu.roll(x[b * deep : (b + 1) * deep], (b * REACH - first) % cols, 1)
            total = part if total is None else jnp.where(lane_at >= b * REACH, part, total)
        return total

    def unfold(x, first, start, blocks):
        parts = [pltpu.roll(x, (first - b * REACH) % cols, 1) for b in range(start, start + blocks)]
        return rows_of(*parts)

    def side_sum(total, l):
        if l:
            total = pltpu.roll(total, slots, 1)
        for shift in (HB, 2 * HB, 4 * HB):
            total = total + pltpu.roll(total, shift, 1)
        return total

    def products(l, g, take, v):
        west, east = take(p_west.at[g]).astype(F32), take(p_east.at[g]).astype(F32)
        return jnp.where(iota(west.shape, 1) // slots == l, west, east) * v

    def outward(core, side):
        lane_at = iota(side.shape, 1)
        eastward = jnp.where(lane_at >= cols - HB, side, pltpu.roll(core, cols - HB, 1))
        westward = jnp.where(lane_at < slots, side, pltpu.roll(core, slots, 1))
        return (eastward, cols - REACH), (westward, slots - HB)

    def rim_of(part):
        far = part[rows:].astype(F32)
        near = [part[:rim].astype(F32), part[rows - rim : rows].astype(F32)]
        return rows_of(far[:HB], *near, far[HB:])

    for one in rims:
        one.arrive()
    for l in range(levels):
        total = None
        for g in range(steps):
            v = rows_of(v_side[g, l, :STRIP], v_side[g, l, e_rows - STRIP :])
            part = products(l, g, rim_of, v)
            total = part if total is None else total + part
        total = side_sum(total, l)
        ext[l, :STRIP, cols:] = total[:STRIP]
        ext[l, e_rows - STRIP :, cols:] = total[STRIP:]
        core = rows_of(ext[l, :STRIP, :cols], ext[l, e_rows - STRIP :, :cols])
        for i, (x, first) in enumerate(outward(core, total)):
            tip[l, i] = fold(rows_of(x[STRIP:], x[:STRIP]), first, HB)

    corner_links, side_links, end_links, swaps = [], [], [], []
    for s in range(count):
        peer = lax.rem(ma + s, count)
        for i, step in enumerate((1, -1)):
            at = {"ma": peer}
            side_links.append(link("gx", step, flank.at[peer, i], flanks.at[s, i], at))
            strip = ext.at[peer, pl.ds((e_rows - STRIP) * (1 - i), STRIP)]
            end_links.append(link("gy", step, strip, ends_in.at[s, i], at))
            at = {"gx": lax.rem(gx + step + gxn, gxn), "ma": peer}
            for j, turn in enumerate((1, -1)):
                corner_links.append(link("gy", turn, tip.at[peer, i], tips.at[s, i, j], at))
        if s:
            swaps.append(link("ma", peer - ma, ext.at[peer], other.at[s - 1]))
    for one in corner_links + end_links:
        one.start()
    inside = slice(STRIP, e_rows - STRIP)
    side_sums = [None] * levels
    for g in range(steps):
        if g:
            for one in p_arrive[g - 1]:
                one.arrive()
        for l in range(levels):
            part = products(l, g, lambda x: x[rim : rows - rim], v_side[g, l, inside])
            side_sums[l] = part if g == 0 else side_sums[l] + part
    for l in range(levels):
        ext[l, inside, cols:] = side_sum(side_sums[l], l)
        for i, (x, first) in enumerate(outward(ext[l, :, :cols], ext[l, :, cols:])):
            flank[l, i] = fold(x, first, STRIP)
    sent = corner_links + end_links + side_links + swaps
    late = side_links + swaps + f_arrive
    for one in late:
        one.start()
    for one in pending:
        if one not in late:
            one.sent()
    for one in sent:
        one.arrive()
    mine, strips_in, flank_in, tip_in = ext[ma], ends_in[0], flanks[0], tips[0]
    for s in range(1, count):
        mine = mine + other[s - 1]
        strips_in, flank_in, tip_in = strips_in + ends_in[s], flank_in + flanks[s], tip_in + tips[s]
    lap = CR - HB
    edge = STRIP - lap

    def merge(above, middle, below):
        return rows_of(
            above[:lap],
            middle[:edge] + above[lap:],
            middle[edge : e_rows - edge],
            middle[e_rows - edge :] + below[:edge],
            below[edge:],
        )

    mine = merge(strips_in[0], mine, strips_in[1])
    core, side = mine[:, :cols], mine[:, cols:]
    third = STRIP // HB

    def wing_from(i, first):
        return merge(
            unfold(tip_in[i, 0], first, 0, third),
            unfold(flank_in[i], first, 0, e_rows // STRIP),
            unfold(tip_in[i, 1], first, third, third),
        )

    wings = jnp.where(
        t_lane < REACH,
        wing_from(0, 0),
        jnp.where((t_lane >= slots) & (t_lane < slots + REACH), wing_from(1, slots), side),
    )
    across = dot3(split(lanes_of(core, wings)), (up_lon[0], up_lon[1]))
    fine = dot3((up_lat[0], up_lat[1]), split(across))
    increment[ma] = fine[:frows, :fcols]
    final = []

    def share(whole):
        for s in range(1, count):
            peer = lax.rem(ma + s, count)
            final.append(link("ma", peer - ma, whole.at[ma], whole.at[ma]))
            final[-1].start()

    share(increment)
    for one in f_arrive:
        one.arrive()
    for i in range(2):

        def wing_of(part):
            def opened(first, last):
                lanes = range(FC * i, 2 * FOLD * FC, 2 * FC)
                return [part[first:last, x : x + FC] for x in lanes]

            low, high = f_main, f_main + HB
            return rows_of(
                rows_of(*opened(0, low))[:frows], *opened(low, high), *opened(high, high + HB)
            )

        fine_wide[i, :, fcols:] = lanes_of(wing_of(f_west), wing_of(f_east))
    misfit = fine_wide[1] * (fine - fine_wide[0])
    across = dot3((down_lat[0], down_lat[1]), split(misfit))
    residual[ma] = dot3(split(across), (down_lon[0], down_lon[1]))
    share(residual)
    for one in late:
        one.sent()
    for one in final:
        one.arrive()
    for one in final:
        one.sent()


def cost(flops, nbytes):
    return pl.CostEstimate(flops=flops, bytes_accessed=nbytes, transcendentals=0)


def core_step(widths, lat_i, lat_w, lon_i, lon_w, alpha, perts, innov, weight):
    members, levels, rows, cols = alpha.shape
    steps = members // GROUP
    frows, fcols = innov.shape[1:]
    count = lax.axis_size("ma")
    assert levels == 2 and count == levels
    assert (rows + 2 * HB) % STRIP == 0
    half = rows // 2
    deep = half + 2 * HB
    wide_k = -(-3 * deep // 128) * 128
    e_rows, t_rows = rows + 2 * HB, rows + 2 * CR
    f_tall, f_wide = frows + 2 * FR, fcols + 2 * FC
    strip = ((members, levels, HB, cols), BF16)
    side = ((steps, e_rows, cols), BF16)
    outs = [
        (innov.shape, F32),
        ((levels, e_rows, 2 * cols), F32),
        (alpha.shape, BF16),
        (alpha.shape, BF16),
        strip,
        strip,
        side,
        side,
        ((levels, 4, cols, cols), BF16),
        ((levels, half, wide_k), BF16),
    ]
    kept = sum(math.prod(shape) * jnp.dtype(kind).itemsize for shape, kind in outs)
    fine_edge = ((2, FR, fcols), F32)
    fine_side = ((-(-frows // (FOLD * HB)) * HB + 2 * HB, cols), F32)
    packed = ((steps, rows, cols), BF16)
    scratch = [
        (lat_i.shape, jnp.int32),
        (lat_w.shape, F32),
        (lon_i.shape, jnp.int32),
        (lon_w.shape, F32),
        ((2, frows, fcols), F32),
        ((levels * GROUP // 2, 2 * cols, 2 * cols), BF16),
        ((levels, 2, cols, cols), BF16),
        ((levels, 2, deep, wide_k), BF16),
        ((members, levels, 2 * HB, cols), F32),
        ((steps, levels, e_rows, cols), F32),
        packed,
        packed,
        fine_edge,
        fine_edge,
        fine_side,
        fine_side,
        fine_side,
        fine_side,
        ((2, f_tall, f_wide), F32),
        (lat_i.shape, jnp.int32),
        (lat_i.shape, jnp.int32),
        (lat_w.shape, F32),
        (lat_w.shape, F32),
        (lon_i.shape, jnp.int32),
        (lon_i.shape, jnp.int32),
        (lon_w.shape, F32),
        (lon_w.shape, F32),
        ((2, 2 * cols, f_wide), BF16),
        ((2, f_tall, t_rows), BF16),
        ((2, e_rows, f_tall), BF16),
        ((2, f_wide, 2 * cols), BF16),
        ((levels, e_rows, 2 * cols), F32),
        ((count - 1, e_rows, 2 * cols), F32),
        ((count, 2, STRIP, 2 * cols), F32),
        ((levels, 2, STRIP, cols), F32),
        ((levels, 2, HB, cols), F32),
        ((count, 2, STRIP, cols), F32),
        ((count, 2, 2, HB, cols), F32),
    ]
    vmem = pl.BlockSpec(memory_space=pltpu.VMEM)
    anywhere = pl.BlockSpec(memory_space=pltpu.HBM)
    return pl.pallas_call(
        core_kernel,
        in_specs=[anywhere] * 9,
        out_specs=[vmem] * len(outs),
        out_shape=[pltpu.VMEM(shape, kind) for shape, kind in outs],
        scratch_shapes=[pltpu.SMEM(widths.shape, jnp.int32)]
        + [pltpu.VMEM(shape, kind) for shape, kind in scratch]
        + [
            pltpu.SemaphoreType.DMA((96,)),
            pltpu.SemaphoreType.DMA((96,)),
            pltpu.SemaphoreType.DMA((7 + 2 * steps,)),
        ],
        compiler_params=pltpu.CompilerParams(
            collective_id=0, has_side_effects=True, vmem_limit_bytes=VMEM_BYTES - VMEM_SLACK - kept
        ),
        cost_estimate=cost(2**30, 2**24),
    )(widths, lat_i, lat_w, lon_i, lon_w, alpha, perts, innov, weight)


def band(high, low, taps):
    half = taps.shape[0]
    deep = half + 2 * HB
    out = []
    for first in range(0, high.shape[0] - 2 * HB, half):
        h, lo = high[first : first + deep], low[first : first + deep]
        out.append(dot(taps, rows_of(h, h, lo)))
    return rows_of(*out)


def adjoint_kernel(
    alpha, perts, north, south, west, east, residual, lon, lat, fine, out, fine_out, sem
):
    rows, cols = alpha.shape[2:]
    slots = GROUP * HB
    g = pl.program_id(0)
    give = pltpu.make_async_copy(fine, fine_out, sem.at[0])

    @pl.when(g == 0)
    def _():
        give.start()

    @pl.when(g == pl.num_programs(0) - 1)
    def _():
        give.wait()

    zero = jnp.zeros((cols, cols), BF16)

    def stack(high, low):
        return rows_of(lanes_of(high, low), lanes_of(high, zero))

    def halves(x):
        return x[:, :cols] + x[:, cols:]

    lane = iota((rows, cols), 1)
    inner = (lane >= HB) & (lane < cols - HB)
    wide = iota((rows + 2 * HB, cols), 1)
    for l in range(alpha.shape[1]):
        res = residual[l]
        taps = lat[l, :, : 3 * (rows // 2 + 2 * HB)]
        side = jnp.where(wide // slots == l, west[g].astype(F32), east[g].astype(F32))
        edge = band(*split(natural(side, rows) * res[:, cols:]), taps)
        edge = halves(dot(lanes_of(*split(edge)), stack(lon[l, 2], lon[l, 3])))
        cores = []
        for k in range(0, GROUP, 2):
            pairs = []
            for m in (k, k + 1):
                n = g * GROUP + m
                tall = rows_of(
                    north[n, l].astype(F32), perts[n, l].astype(F32), south[n, l].astype(F32)
                )
                pairs.append(split(tall * res[:, :cols]))
            both = band(lanes_of(pairs[0][0], pairs[1][0]), lanes_of(pairs[0][1], pairs[1][1]), taps)
            for i in range(2):
                cores.append(lanes_of(*split(both[:, i * cols : (i + 1) * cols])))
        total = dot(rows_of(*cores), stack(lon[l, 0], lon[l, 1]))
        for m in range(GROUP):
            turned = pltpu.roll(edge, (cols - HB - 2 * HB * m) % cols, 1)
            value = halves(total[m * rows : (m + 1) * rows]) + jnp.where(inner, 0.0, turned)
            out[m, l] = alpha[g * GROUP + m, l].astype(F32) + value


def adjoint(alpha, perts, north, south, west, east, residual, lon, lat, fine):
    members, levels, rows, cols = alpha.shape
    return pl.pallas_call(
        adjoint_kernel,
        grid=(members // GROUP,),
        in_specs=[pl.BlockSpec(memory_space=pltpu.VMEM)] * 10,
        out_specs=[
            pl.BlockSpec((GROUP, levels, rows, cols), lambda g: (g, 0, 0, 0)),
            pl.BlockSpec(memory_space=pltpu.HBM),
        ],
        out_shape=[
            jax.ShapeDtypeStruct(alpha.shape, F32),
            jax.ShapeDtypeStruct(fine.shape, F32),
        ],
        scratch_shapes=[pltpu.SemaphoreType.DMA((1,))],
        compiler_params=pltpu.CompilerParams(vmem_limit_bytes=BACK_LIMIT),
        cost_estimate=cost(members * levels * 2**25, alpha.size * 8),
    )(alpha, perts, north, south, west, east, residual, lon, lat, fine)


def body(
    alpha_fields,
    member_perts,
    band_widths,
    lat_index,
    lat_weight,
    lon_index,
    lon_weight,
    innovation,
    obs_weight,
):
    tables = [x.reshape(1, -1) for x in (lat_index, lat_weight, lon_index, lon_weight)]
    increment, residual, alpha, perts, *rest = core_step(
        band_widths, *tables, alpha_fields, member_perts, innovation, obs_weight
    )
    north, south, west, east, lon, lat = rest
    gradient, increment = adjoint(
        alpha, perts, north, south, west, east, residual, lon, lat, increment
    )
    return (increment, gradient)


def solution(mesh):
    placed = (
        P("ma", None, "gy", "gx"),
        P("ma", None, "gy", "gx"),
        P(),
        P("gy"),
        P("gy"),
        P("gx"),
        P("gx"),
        P(None, "gy", "gx"),
        P(None, "gy", "gx"),
    )
    return jax.shard_map(
        body,
        mesh=mesh,
        in_specs=placed,
        out_specs=(P(None, "gy", "gx"), P("ma", None, "gy", "gx")),
        check_vma=False,
    )
```
